32 devices in a mesh: model: 32 (over z, y, x, core).
Axes of the slice: x: 2, y: 2, z: 4, core: 2. Of those that a mesh axis runs over, the one named last changes fastest.
Arguments:
- act_in: bfloat16 [4096, 8192], P('model')
- ln_gain: float32 [8192], replicated
- w_q: bfloat16 [8192, 8192], P(None, 'model')
- w_kv: bfloat16 [8192, 256], replicated
- w_o: bfloat16 [8192, 8192], P('model')
- positions: int32 [4096], replicated
Outputs:
- output 1: bfloat16 [4096, 8192], P('model')
- output 2: bfloat16 [4096, 128], replicated
- output 3: bfloat16 [4096, 128], replicated
All inputs are finite; a program needn't handle non-finite values.
Results may differ from the reference program's by a relative error of at most 0.02.
Values are sent between devices in bfloat16 or wider.
A program may use at most 1 GiB of HBM per device.

```python
import jax
import jax.numpy as jnp
from jax import lax

TOKENS = 4096
SEQ = 4096
D = 8192
HEADS = 64
HEAD = 128
NORM_EPS = 1e-6


def setup_inputs(seed: int = 0) -> dict:
    rng_keys = jax.random.split(jax.random.key(seed), 6)
    act_in = jax.random.normal(rng_keys[0], (TOKENS, D), jnp.float32).astype(jnp.bfloat16)
    ln_gain = jax.random.uniform(rng_keys[1], (D,), jnp.float32, 0.6, 1.4)
    w_q = (jax.random.normal(rng_keys[2], (D, HEADS * HEAD), jnp.float32) * D ** -0.5).astype(jnp.bfloat16)
    w_kv = (jax.random.normal(rng_keys[3], (D, 2 * HEAD), jnp.float32) * D ** -0.5).astype(jnp.bfloat16)
    out_scale = (SEQ / (HEADS * HEAD)) ** 0.5 / 8.0
    w_o = (jax.random.normal(rng_keys[4], (HEADS * HEAD, D), jnp.float32) * out_scale).astype(jnp.bfloat16)
    positions = jax.random.permutation(rng_keys[5], SEQ).astype(jnp.int32)
    return dict(act_in=act_in, ln_gain=ln_gain, w_q=w_q, w_kv=w_kv, w_o=w_o, positions=positions)


def layer_norm(act_rows, gain_vec):
    rows_f32 = act_rows.astype(jnp.float32)
    row_mean = jnp.mean(rows_f32, axis=-1, keepdims=True)
    centered = rows_f32 - row_mean
    variance = jnp.mean(centered * centered, axis=-1, keepdims=True)
    return (centered * lax.rsqrt(variance + NORM_EPS) * gain_vec).astype(jnp.bfloat16)


def reference(act_in, ln_gain, w_q, w_kv, w_o, positions):
    normed = layer_norm(act_in, ln_gain)
    queries = jnp.dot(normed, w_q, preferred_element_type=jnp.float32).astype(jnp.bfloat16)
    kv_proj = jnp.dot(normed, w_kv, preferred_element_type=jnp.float32).astype(jnp.bfloat16)
    k_cache = kv_proj[:, :HEAD]
    v_cache = kv_proj[:, HEAD:]
    n_seq = TOKENS // SEQ
    visible = positions[None, :] <= positions[:, None]
    q_seqs = queries.reshape(n_seq, SEQ, HEADS, HEAD).transpose(0, 2, 1, 3)
    k_seqs = k_cache.reshape(n_seq, SEQ, HEAD)
    v_seqs = v_cache.reshape(n_seq, SEQ, HEAD)

    def one_seq(operands):
        q_blk, k_blk, v_blk = operands

        def one_head(q_head):
            scores = jnp.dot(q_head, k_blk.T, preferred_element_type=jnp.float32) * HEAD ** -0.5
            scores = jnp.where(visible, scores, -1e30)
            attn_prob = jax.nn.softmax(scores, axis=-1).astype(jnp.bfloat16)
            return jnp.dot(attn_prob, v_blk, preferred_element_type=jnp.float32).astype(jnp.bfloat16)

        return lax.map(one_head, q_blk)

    attended = lax.map(one_seq, (q_seqs, k_seqs, v_seqs))
    attended = attended.transpose(0, 2, 1, 3).reshape(TOKENS, HEADS * HEAD)
    y_out = jnp.dot(attended, w_o, preferred_element_type=jnp.float32).astype(jnp.bfloat16)
    return y_out, k_cache, v_cache
```

```python
import jax
import jax.numpy as jnp
from jax import lax
from jax.experimental import pallas as pl
from jax.experimental.pallas import tpu as pltpu
from jax.sharding import PartitionSpec as P

NORM_EPS = 1e-6
LOG2E = 1.4426950408889634
MESH = pl.DeviceIdType.MESH
BF16, F32, I32 = jnp.bfloat16, jnp.float32, jnp.int32
HD = 128
PAIR = 2 * HD
KEYS = 8 * HD
QUADS = 4
CHUNKS = 16
AHEAD = 2
MASKED = -1e30
BOTH, THREE = range(2), range(3)
HANDED_ON = (3, 4)

TILES = ((0, 0, 0), (0, 1, 0), (1, 0, 0), (1, 1, 0), (0, 2, 0), (1, 2, 0), (2, 0, 0), (2, 1, 0), (2, 2, 0), (3, 0, 1),
         (1, 3, 0), (2, 3, 0), (0, 3, 0), (3, 2, 1), (3, 0, 2), (3, 2, 2))
LATE = (1, 2, 4, 6, 9, 10, 14)
TICKS = (11, 12, 13, 15)
EARLY = (12, 13, 14)
LAST = TILES[-1]
NEXT = [TILES[0] if i in LATE else t for i, t in enumerate(TILES)][1:]


def digits(values):
    return sum((v % 4) << (2 * i) for i, v in enumerate(values))


TABLES = [digits(t[c] - LAST[c] for t in TILES) for c in range(3)] + [digits(t[c] for t in NEXT) for c in range(3)]

COPIES = dict(kvz=3, kvp=3, kvd=1, h=10, hd=10, wx=5, wy=5, pre=6, wod=1, wox=3 * CHUNKS, woy=3 * CHUNKS, ox=8, yd=CHUNKS)
START = {}
for _name, _n in COPIES.items():
    START[_name] = sum(COPIES[k] for k in START)
TOTAL = sum(COPIES.values())
SENDS, RECVS = 3, 5


def kernel(x_in, gain, wq_in, wkv_in, wo_in, pos, y_out, k_out, v_out, wo_land,
           hbuf, wq, kv, v_t, posk, obuf, wbuf, acc, early, sc0, sc1, pr0, pr1, out_t, qacc, qbuf,
           loc, snd, rcv, hf_r, hb_r, ld, ys_s, yr_r, yl, ready):
    me = lax.axis_index("model")
    core = lax.rem(me, 2)
    quad = lax.rem(me // 2, QUADS)
    z = me // 8
    width = hbuf.shape[3]
    half = width // 2
    cw = half // CHUNKS
    upper = z // 2
    away = 1 - 2 * upper

    def zof(d):
        return d + upper * (3 - 2 * d)

    e = zof(z)
    end, mid = e == 0, e == 1
    base = me - 8 * z
    dx = 2 - 4 * lax.rem(quad, 2)
    dy = 4 - 8 * (quad // 2)
    sib, xn, yn, dg = me + 1 - 2 * core, me + dx, me + dy, me + dx + dy
    fwd = base + 8 * (z + away)
    bwd = base + 8 * (z - away * e)
    side = base + 8 * (z + away * (1 - 2 * e))
    zpeers = [base + 8 * lax.rem(z + i, QUADS) for i in (1, 2, 3)]
    bufs = ((sc0, pr0), (sc1, pr1))

    def put(src, dst, ssem, rsem, dev):
        return pltpu.make_async_remote_copy(src, dst, ssem, rsem, device_id=(dev,), device_id_type=MESH)

    def send(kind, i, src, dst, dev):
        n = START[kind] + i
        return put(src, dst, snd.at[n], rcv.at[n], dev)

    def kv_z(i):
        blk = kv.at[z, :, core]
        return send("kvz", i, blk, blk, zpeers[i])

    def kv_p(i):
        blk = kv.at[z, quad, core]
        return send("kvp", i, blk, blk, (xn, yn, dg)[i])

    def kv_d():
        blk = kv.at[:, :, core]
        return send("kvd", 0, blk, blk, sib)

    hh = HD // 2

    def hrows(zz, cc, i):
        return hbuf.at[zz, cc, pl.ds(hh * i, hh), :]

    def h_put(n, zz, i, rsem, dev):
        return put(hrows(zz, 0, i), hrows(zz, 0, i), snd.at[START["h"] + n], rsem, dev)

    def h_own(i, rsems):
        return h_put(i, z, i, rsems.at[i], fwd)

    def h_own_b(i):
        return h_put(2 + i, z, i, hf_r.at[i], bwd)

    def h_f2b(i):
        return h_put(4 + i, zof(e + 1 + i // 2), i % 2, hf_r.at[2 + i], bwd)

    def h_b2f(i):
        return h_put(8 + i, zof(e - 1), i, hf_r.at[2 + i], fwd)

    def h_d(i):
        zz = z if i < 2 else (zof(e + i // 2) if i < 8 else zof(e - 1))
        return send("hd", i, hrows(zz, 0, i % 2), hrows(zz, 1, i % 2), sib)

    def f_half(i):
        zz = zof(e + 1 + i // 2)
        h_put(0, zz, i % 2, hf_r.at[i], fwd).wait_recv()
        h_d(2 + i).start()
        if i < 4:
            @pl.when(mid)
            def _():
                h_f2b(i).start()

    def b_half(i):
        @pl.when(mid)
        def _():
            h_put(0, zof(e - 1), i, hb_r.at[i], bwd).wait_recv()
            h_d(8 + i).start()
            h_b2f(i).start()

    def h_d_wait(*idx):
        for i in idx:
            h_d(i).wait_recv()

    nb = wq.shape[1]
    hb = nb // 2

    def w_piece(i, x):
        if i < 3:
            rows = (pl.ds(0, nb), pl.ds(0, hb), pl.ds(hb, hb))[i]
            h = min(i, 1)
            src = wq_in.at[rows, :, pl.ds(HD * h, HD)]
            dst = wq.at[1 + h, rows, :, pl.ds(0 if x else HD, HD)]
        else:
            h = i - 3
            rows = pl.ds(0 if x else hb, hb)
            src = wq.at[1 + h, rows, :, pl.ds(HD if x else 0, HD)]
            dst = wq.at[3, rows, :, pl.ds(HD * h, HD)]
        return send("wx" if x else "wy", i, src, dst, xn if x else yn)

    def w_x(i):
        return w_piece(i, x=True)

    def w_y(i):
        return w_piece(i, x=False)

    def wo_sib():
        src = wo_in.at[:, pl.ds(pl.multiple_of((1 - core) * half, half), half)]
        return send("wod", 0, src, wo_land.at[1, 0], sib)

    def cols(ch):
        return pl.ds(pl.multiple_of(ch * cw, cw), cw)

    def own_cols(ch):
        return pl.ds(pl.multiple_of(core * half + ch * cw, cw), cw)

    def wo_piece(i, ch, x):
        src = (wo_in.at[:, own_cols(ch)], wo_land.at[1, 0, :, cols(ch)], wo_land.at[0 if x else 1, 2 if x else 1, :, cols(ch)])[i]
        part = (0, 1, 0 if x else 1)[i]
        dst = wo_land.at[part, 3 if i == 2 else 1 if x else 2, :, cols(ch)]
        return send("wox" if x else "woy", 3 * ch + i, src, dst, xn if x else yn)

    def wo_x(i, ch):
        return wo_piece(i, ch, True)

    def wo_y(i, ch):
        return wo_piece(i, ch, False)

    def wo_own(ch):
        for i in BOTH:
            wo_x(i, ch).start()
            wo_y(i, ch).start()

    def wo_tick(ch):
        wo_y(0, ch).wait_recv()
        wo_x(1, ch).wait_recv()
        wo_x(2, ch).start()
        wo_y(2, ch).start()

        @pl.when(ch + AHEAD < CHUNKS)
        def _():
            wo_own(ch + AHEAD)

    def wo_arrive(ch):
        wo_x(0, ch).wait_recv()
        wo_y(1, ch).wait_recv()
        wo_x(2, ch).wait_recv()
        wo_y(2, ch).wait_recv()

    def load(g, slot, i, src, dst):
        return pltpu.make_async_copy(src, dst, ld.at[g, slot, i])

    def loads(g, ch, slot):
        w = wbuf.at[g, slot]
        rest = pl.ds(1, 3)
        return (load(g, slot, 0, wo_in.at[:, own_cols(ch)], w.at[0, 0]),
                load(g, slot, 1, wo_land.at[0, rest, :, cols(ch)], w.at[0, rest]),
                load(g, slot, 2, wo_land.at[1, :, :, cols(ch)], w.at[1]))

    lags = (e, 4 - 2 * e)

    skip = (1 - e) * len(EARLY)

    def each_load(step, act):
        for g, (lag, lowest) in enumerate(zip(lags, (skip, 0))):
            ch = step - lag

            @pl.when((ch >= lowest) & (ch < CHUNKS))
            def _():
                for c in loads(g, ch, lax.rem(step, 2)):
                    act(c)

    def kof(k):
        return zof(k + e * (lax.rem(k + 1, 3) + 2 * (k // 3) - k))

    def o_x(k, cc):
        lo = obuf.shape[3] // 2
        zz = kof(k)
        return send("ox", 2 * k + cc, obuf.at[zz, cc, :, pl.ds(0, lo)], obuf.at[zz, 1 - cc, :, pl.ds(lo, lo)], sib)

    x_copy, wkv_copy, wq_copy = (
        pltpu.make_async_copy(src, dst, loc.at[i])
        for i, (src, dst) in enumerate(((x_in, hbuf.at[z, 0]), (wkv_in, wbuf), (wq_in, wq.at[0]))))
    x_copy.start()
    wkv_copy.start()
    wq_copy.start()
    barrier = pltpu.get_barrier_semaphore()
    peers = zpeers + [xn, yn, dg, sib]
    for dev in peers:
        pl.semaphore_signal(barrier, device_id=(dev,), device_id_type=MESH)
    x_copy.wait()

    @pl.loop(0, 8)
    def _(i):
        rows = pl.ds(pl.multiple_of(i * 16, 16), 16)
        x = hbuf[z, 0, rows, :].astype(F32)
        cent = x - jnp.mean(x, axis=-1, keepdims=True)
        var = jnp.mean(cent * cent, axis=-1, keepdims=True)
        hbuf[z, 0, rows, :] = (cent * lax.rsqrt(var + NORM_EPS) * gain[:]).astype(BF16)

    wkv_copy.wait()
    kv[z, quad, core] = jnp.dot(hbuf[z, 0], wbuf[:].reshape(width, PAIR), preferred_element_type=F32).astype(BF16)
    pl.semaphore_wait(barrier, len(peers))
    for i in THREE:
        kv_p(i).start()
    for i in (0, 2, 1):
        w_x(i).start()
    for i in THREE:
        w_y(i).start()
    for i in BOTH:
        h_d(i).start()
    wo_sib().start()
    for i in THREE:
        kv_p(i).wait_recv()
    for i in THREE:
        kv_z(i).start()
    for i in BOTH:
        @pl.when(end)
        def _():
            h_own(i, hb_r).start()

        @pl.when(mid)
        def _():
            h_own_b(i).start()
            h_own(i, hf_r).start()

    @pl.loop(0, posk.shape[0] // HD)
    def _(i):
        blk = pl.ds(pl.multiple_of(i * HD, HD), HD)
        posk[blk, :] = jnp.broadcast_to(pos[:, blk], (HD, HD)).T

    def rows_of(ref, zz):
        return ref[zz].reshape(PAIR, ref.shape[3])

    def keep_q():
        q = qacc[:].astype(BF16)
        qbuf[:PAIR] = q[:, :HD]
        qbuf[PAIR:] = q[:, HD:]

    def parts(part):
        split = (part + 1) // 2
        return [[(g + split * (i - g), i + split * (part - 1 - i)) for i in BOTH] for g in BOTH]

    def head_pair(p, part, g):
        return p + g * ((part + 1) // 2)

    def q_dot(unit, js, ws):
        zz, p, part = unit
        for g in BOTH:
            rows = [hbuf[zz, cc, pl.ds(pl.multiple_of(r * hh, hh), hh), js] for cc, r in parts(part)[g]]
            w = wq[head_pair(p, part, g), ws].reshape(-1, PAIR)
            yield g, jnp.dot(jnp.concatenate(rows, axis=0), w, preferred_element_type=F32)

    def whole_q(unit):
        for g, part in q_dot(unit, slice(None), slice(None)):
            qacc[g * HD:(g + 1) * HD] = part
        keep_q()

    def unit_of(codes, last):
        k, p, part = (lax.rem(c + v, QUADS) for c, v in zip(codes, last))
        return kof(k), p, part

    wq_copy.wait()
    h_d_wait(0, 1)
    whole_q((z, 0, 0))
    for i in THREE:
        kv_z(i).wait_recv()
    kv_d().start()
    kv_d().wait_recv()
    kv_copies = [pltpu.make_async_copy(kv.at[:, :, :, :, pl.ds(HD * i, HD)], o, loc.at[3 + i]) for i, o in enumerate((k_out, v_out))]
    for c in kv_copies:
        c.start()
    for j in range(QUADS):
        v_t[:, j * KEYS:(j + 1) * KEYS] = kv[j].reshape(KEYS, PAIR)[:, HD:].T

    blocks = [(k, cc) for k in range(QUADS) for cc in BOTH]
    places = nb

    def place(i):
        return wq.at[i // places, lax.rem(i, places)]

    def y_send(i, ch, off, dev):
        return put(place(RECVS * CHUNKS + ch * SENDS + i), place(ch * RECVS + off), ys_s.at[ch * SENDS + i], yr_r.at[ch * RECVS + off], dev)

    def y_recv(ch, off):
        i = ch * RECVS + off
        put(place(i), place(i), ys_s.at[0], yr_r.at[i], fwd).wait_recv()
        return place(i)[:].astype(F32)

    def y_local(ch):
        return pltpu.make_async_copy(hbuf.at[0, 0, :, cols(ch)], y_out.at[:, own_cols(ch)], yl.at[ch])

    def y_sib(ch):
        return send("yd", ch, hbuf.at[0, 1, :, cols(ch)], y_out.at[:, own_cols(ch)], sib)

    def weights(g, sl):
        return wbuf[g, sl].reshape(obuf.shape[3], cw)

    def go_on(i, ch, off, dev):
        place(RECVS * CHUNKS + ch * SENDS + i)[:] = acc[i].astype(BF16)
        y_send(i, ch, off, dev).start()

    o_parts = ((EARLY[0] - 1, blocks[2:6]), (EARLY[0], blocks[:2]), (len(TILES) - 1, blocks[6:]))

    def early_send(c, i):
        return send("pre", 2 * c + i, early.at[1, c, i], early.at[0, c, i], fwd)

    def y_early(c):
        if c == 0:
            for b in o_parts[0][-1]:
                o_x(*b).wait_recv()
        wo_arrive(c)
        for cp in loads(c // 2, c, c % 2):
            cp.start()
        for cp in loads(c // 2, c, c % 2):
            cp.wait()
        for i in BOTH:
            early[1, c, i] = jnp.dot(rows_of(obuf, zof(2 - i)), weights(c // 2, c % 2), preferred_element_type=F32).astype(BF16)
            early_send(c, i).start()

    def y_recv_early(n, ch, off):
        @pl.when(ch < len(EARLY))
        def _():
            blk = early.at[0, ch, off - 1]
            put(blk, blk, ys_s.at[0], rcv.at[START["pre"] + 2 * ch + off - 1], bwd).wait_recv()
            acc[n] += blk[:].astype(F32)

        @pl.when(ch >= len(EARLY))
        def _():
            acc[n] += y_recv(ch, off)

    scale = HD ** -0.5 * LOG2E
    n = 2 * PAIR
    kq = width // QUADS

    def tile(s, carry):
        codes, ahead = carry[:3], carry[3:]
        zz, p, part = unit_of(codes, LAST)
        following = unit_of(ahead, TILES[0])
        carry = tuple(c // QUADS for c in carry)

        for i, at in enumerate(TICKS):
            @pl.when(s == at)
            def _():
                wo_tick(i)

        @pl.when((s == LATE[-1] - 1) & end)
        def _():
            f_half(5)

        q = qbuf[:]
        tok = (zz * QUADS + quad) * 2
        pq = [pos[:, pl.ds(pl.multiple_of((tok + c) * HD, HD), HD)] for c in (core, 1 - core)]
        pq = [[v[:, :hh], v[:, hh:]] for v in pq]
        split, second = (part + 1) // 2, part // 2
        of_core = [v[0] + second * (v[1] - v[0]) for v in pq]
        pq = [pq[g][i] + split * (of_core[i] - pq[g][i]) for g in BOTH for i in BOTH]
        pq = jnp.broadcast_to(jnp.concatenate(pq + pq, axis=1), (8, n))

        def scores(j):
            keys = kv[j].reshape(KEYS, PAIR)[:, :HD]
            sc = lax.dot_general(keys, q, (((1,), (1,)), ((), ())), preferred_element_type=F32)
            pk = posk[j * KEYS:(j + 1) * KEYS, :]
            pk = jnp.concatenate([pk] * (n // HD), axis=1).reshape(KEYS // 8, 8, n)
            sc = jnp.where(pk <= pq, sc.reshape(KEYS // 8, 8, n), MASKED)
            bufs[j % 2][0][:] = sc.reshape(KEYS, n)
            return jnp.max(jnp.max(sc, axis=0), axis=0, keepdims=True)

        def weigh(j, m):
            pr = jnp.exp2((bufs[j % 2][0][:].reshape(KEYS // 8, 8, n) - jnp.broadcast_to(m, (8, n))) * scale)
            bufs[j % 2][1][:] = pr.reshape(KEYS, n).astype(BF16)
            return jnp.sum(pr, axis=0)

        def add_values(j, alpha):
            got = jnp.dot(v_t[:, j * KEYS:(j + 1) * KEYS], bufs[j % 2][1][:], preferred_element_type=F32)
            out_t[:] = got if alpha is None else out_t[:] * alpha + got

        m = scores(0)
        alpha = den = None
        for j in range(QUADS):
            if j + 1 < QUADS:
                mn = jnp.maximum(m, scores(j + 1))
            for g, got in q_dot(following, slice(j * kq, (j + 1) * kq), slice(j * nb // QUADS, (j + 1) * nb // QUADS)):
                rows = slice(g * HD, (g + 1) * HD)
                qacc[rows] = got if j == 0 else qacc[rows] + got
            ps = weigh(j, m)
            if j > 0:
                add_values(j - 1, alpha if j > 1 else None)
            den = ps if j == 0 else den * now + ps
            if j > 0:
                alpha = now
            if j < QUADS - 1:
                now = jnp.exp2((m - mn) * scale)
                m = mn
        add_values(QUADS - 1, alpha)
        out = (out_t[:] / jnp.sum(den, axis=0, keepdims=True)).T.astype(BF16)
        for g in BOTH:
            hp = head_pair(p, part, g)
            for j, c in enumerate((2 * hp - hp // 2 + hp // 3, 2 * hp + 1 + (hp + 1) // 2 - hp // 2 - hp // 3)):
                for i, (cc, r) in enumerate(parts(part)[g]):
                    row = (2 * j + g) * HD + i * hh
                    obuf[zz, cc, pl.ds(pl.multiple_of(r * hh, hh), hh), pl.ds(pl.multiple_of(c * HD, HD), HD)] = out[row:row + hh]
        keep_q()

        def late(i):
            if i == 1:
                w_x(0).wait_recv()
                w_y(0).wait_recv()
                f_half(0)
                b_half(0)
            elif i == 2:
                f_half(1)
                b_half(1)
                h_d_wait(2, 3)
                w_x(2).wait_recv()
                w_y(1).wait_recv()
                for c in HANDED_ON:
                    w_x(c).start()
                    w_y(c).start()
                wo_sib().wait_recv()
                wo_own(0)
                wo_own(1)
            elif i == 4:
                w_x(1).wait_recv()
                w_y(2).wait_recv()
                f_half(2)
            elif i == 6:
                f_half(3)

                @pl.when(end)
                def _():
                    h_d_wait(4, 5)

                @pl.when(mid)
                def _():
                    h_d_wait(8, 9)
            elif i == 10:
                for c in HANDED_ON:
                    w_x(c).wait_recv()
                    w_y(c).wait_recv()
            else:
                c = 0 if i == 9 else 1

                @pl.when(end)
                def _():
                    if c == 0:
                        f_half(4)
                    h_d_wait(6 + c)

                @pl.when(mid)
                def _():
                    h_d_wait(4 + c)

        for i in LATE:
            @pl.when(s + 1 == i)
            def _():
                late(i)
        is_late = (s == LATE[0] - 1)
        for i in LATE[1:]:
            is_late = is_late | (s == i - 1)

        @pl.when(is_late)
        def _():
            whole_q(unit_of(carry[:3], LAST))

        for at, some in o_parts:
            @pl.when(s == at)
            def _():
                for b in some:
                    o_x(*b).start()

        for i, at in enumerate(EARLY):
            @pl.when((s == at) & end)
            def _():
                y_early(i)
        return carry

    lax.fori_loop(0, len(TILES), tile, tuple(jnp.int32(t) for t in TABLES))

    for i in BOTH:
        @pl.when(end)
        def _():
            h_own(i, hb_r).wait_send()
            h_d(6 + i).wait_send()

        @pl.when(mid)
        def _():
            h_own_b(i).wait_send()
            h_own(i, hf_r).wait_send()
            h_b2f(i).wait_send()
            h_d(8 + i).wait_send()
            h_f2b(i).wait_send()
            h_f2b(2 + i).wait_send()
        for c in range(3):
            h_d(2 * c + i).wait_send()
    for i in range(5):
        w_x(i).wait_send()
        w_y(i).wait_send()

    @pl.when(end)
    def _():
        pl.semaphore_signal(ready.at[1], device_id=(fwd,), device_id_type=MESH)

    @pl.when(mid)
    def _():
        pl.semaphore_signal(ready.at[0], device_id=(fwd,), device_id_type=MESH)
        pl.semaphore_signal(ready.at[0], device_id=(bwd,), device_id_type=MESH)

    @pl.when(mid)
    def _():
        for i in range(len(EARLY)):
            wo_arrive(i)
        for b in o_parts[0][-1]:
            o_x(*b).wait_recv()
    for b in blocks[:2] + blocks[6:]:
        o_x(*b).wait_recv()
    pl.semaphore_wait(ready.at[0], 1)

    @pl.when(mid)
    def _():
        pl.semaphore_wait(ready.at[1], 1)

    @pl.when(end)
    def _():
        for c in range(len(EARLY)):
            acc[0] = jnp.dot(rows_of(obuf, zof(3)), weights(c // 2, c % 2), preferred_element_type=F32)
            go_on(0, c, 0, fwd)

    def y_step(t, _):
        sl = lax.rem(t, 2)
        each_load(t, lambda c: c.wait())
        ch_a, ch_2, ch_b = t - lags[0], t - 2 * e, t - lags[1]

        @pl.when((ch_a >= skip) & (ch_a < CHUNKS))
        def _():
            for i in BOTH:
                acc[i] = jnp.dot(rows_of(obuf, zof(3 - i)), weights(0, sl), preferred_element_type=F32)

                @pl.when(mid)
                def _():
                    if i == 0:
                        acc[i] += y_recv(ch_a, i)
                    else:
                        y_recv_early(i, ch_a, i)
                go_on(i, ch_a, i + 3 * e, fwd)

        @pl.when((ch_2 >= skip) & (ch_2 < CHUNKS))
        def _():
            acc[2] = jnp.dot(rows_of(obuf, zof(1 - e)), weights(e, sl), preferred_element_type=F32)

            @pl.when(mid)
            def _():
                acc[2] += y_recv(ch_2, 3)
            go_on(2, ch_2, 2 + e, side)

        @pl.when((t + AHEAD >= len(TICKS)) & (t + AHEAD < CHUNKS))
        def _():
            wo_tick(t + AHEAD)

        @pl.when((t + 1 >= len(EARLY)) & (t + 1 < CHUNKS))
        def _():
            wo_arrive(t + 1)
        each_load(t + 1, lambda c: c.start())

        @pl.when((ch_b >= 0) & (ch_b < CHUNKS))
        def _():
            acc[3] = jnp.dot(rows_of(obuf, z), weights(1, sl), preferred_element_type=F32)

            @pl.when(end)
            def _():
                acc[3] += y_recv(ch_b, 3)

            @pl.when(mid)
            def _():
                y_recv_early(3, ch_b, 2)
                acc[3] += y_recv(ch_b, 4)
            hbuf[0, :, :, cols(ch_b)] = acc[3].astype(BF16).reshape(2, HD, cw)
            y_local(ch_b).start()
            y_sib(ch_b).start()
        return 0

    lax.fori_loop(0, CHUNKS + 4, y_step, 0)

    @pl.loop(0, CHUNKS)
    def _(ch):
        for i in THREE:
            wo_x(i, ch).wait_send()
            wo_y(i, ch).wait_send()
        y_send(0, ch, 3 * e, fwd).wait_send()

        @pl.when(ch >= skip)
        def _():
            y_send(1, ch, 1 + 3 * e, fwd).wait_send()
            y_send(2, ch, 2 + e, side).wait_send()
        y_local(ch).wait()
        y_sib(ch).wait_send()
        y_sib(ch).wait_recv()
    for b in blocks:
        o_x(*b).wait_send()

    @pl.when(end)
    def _():
        for i in range(len(EARLY)):
            early_send(i, 0).wait_send()
            early_send(i, 1).wait_send()
    for i in THREE:
        kv_z(i).wait_send()
        kv_p(i).wait_send()
    kv_d().wait_send()
    wo_sib().wait_send()
    for c in kv_copies:
        c.wait()


def solution(mesh):
    def local_step(x_loc, ln_gain, wq_loc, w_kv, wo_loc, positions):
        rows, width = x_loc.shape
        tokens = positions.shape[0]
        dma, vmem = pltpu.SemaphoreType.DMA, pltpu.VMEM
        hbm = pl.BlockSpec(memory_space=pl.ANY)
        vm = pl.BlockSpec(memory_space=pltpu.VMEM)
        half = width // 2
        cw = half // CHUNKS
        nb, n = width // PAIR, 2 * PAIR
        kv_shape = (QUADS, QUADS, 2, rows, HD)
        wbuf_shape = (2, 2, 2, QUADS, PAIR, cw)
        y, k, v, _ = pl.pallas_call(
            kernel,
            name="mqa_layer",
            out_shape=tuple(jax.ShapeDtypeStruct(s, BF16) for s in ((rows, width), kv_shape, kv_shape, (2, QUADS, PAIR, half))),
            in_specs=[hbm, vm, hbm, hbm, hbm, vm],
            out_specs=(hbm, hbm, hbm, hbm),
            scratch_shapes=[
                vmem((QUADS, 2, rows, width), BF16),
                vmem((QUADS, nb, PAIR, PAIR), BF16),
                vmem((QUADS, QUADS, 2, rows, PAIR), BF16),
                vmem((HD, tokens), BF16),
                vmem((tokens, HD), I32),
                vmem((QUADS, 2, rows, 2 * KEYS), BF16),
                vmem(wbuf_shape, BF16),
                vmem((QUADS, PAIR, cw), F32),
                vmem((2, len(EARLY), 2, PAIR, cw), BF16),
                vmem((KEYS, n), F32), vmem((KEYS, n), F32),
                vmem((KEYS, n), BF16), vmem((KEYS, n), BF16),
                vmem((HD, n), F32),
                vmem((PAIR, PAIR), F32),
                vmem((n, HD), BF16),
                dma((5,)), dma((TOTAL,)), dma((TOTAL,)), dma((6,)), dma((2,)), dma((2, 2, 3)),
                dma((CHUNKS * SENDS,)), dma((CHUNKS * RECVS,)), dma((CHUNKS,)),
                pltpu.SemaphoreType.REGULAR((2,)),
            ],
            compiler_params=pltpu.CompilerParams(
                collective_id=0, has_side_effects=True, vmem_limit_bytes=67043328),
        )(x_loc, ln_gain.reshape(1, width), wq_loc.reshape(nb, PAIR, PAIR), w_kv.reshape(wbuf_shape), wo_loc, positions.reshape(1, tokens))
        return y, k.reshape(tokens, HD), v.reshape(tokens, HD)

    split, whole = P("model", None), P(None, None)
    return jax.shard_map(
        local_step,
        mesh=mesh,
        in_specs=(split, P(None), P(None, "model"), whole, split, P(None)),
        out_specs=(split, whole, whole),
        check_vma=False,
    )
```

```python
import functools

import jax
import jax.numpy as jnp
from jax import lax
from jax.experimental import pallas as pl
from jax.experimental.pallas import tpu as pltpu
from jax.sharding import PartitionSpec as P

NORM_EPS = 1e-6
LOG2E = 1.4426950408889634
MESH = pl.DeviceIdType.MESH
BF16, F32, I32 = jnp.bfloat16, jnp.float32, jnp.int32
HD = 128
PAIR = 2 * HD
KEYS = 8 * HD
QUADS = 4
CHUNKS = 16
AHEAD = 2
MASKED = -1e30
BOTH, THREE = range(2), range(3)
HANDED_ON = (4, 5)

TILES = ((0, 0, 0), (0, 1, 0), (1, 0, 0), (1, 1, 0), (0, 2, 0), (1, 2, 0), (2, 0, 0), (2, 1, 0), (2, 2, 0), (3, 0, 1),
         (1, 3, 0), (2, 3, 0), (3, 2, 1), (0, 3, 0), (3, 0, 2), (3, 2, 2))
LATE = (1, 2, 4, 6, 9, 10, 14)
TICKS = range(11, 15)
EARLY = TICKS[1:]
LAST = TILES[-1]
NEXT = [TILES[0] if i in LATE else t for i, t in enumerate(TILES)][1:]


def digits(values):
    return sum((v % 4) << (2 * i) for i, v in enumerate(values))


TABLES = [digits(t[c] - LAST[c] for t in TILES) for c in range(3)] + [digits(t[c] for t in NEXT) for c in range(3)]

SENDS, RECVS = 3, 5
RING, Y_RING = 4, 8

KINDS = ("kvz", "kvp", "kvd", "h", "hd", "wx", "wy", "pre", "wod", "wox", "woy", "ox", "y", "yd")
SND = dict.fromkeys(KINDS, 1) | dict(kvz=3, kvp=3, h=10)
RCV = dict.fromkeys(KINDS, 1) | dict(kvz=3, kvp=3, hd=10, wx=6, wy=6, pre=9, wox=2 * RING, woy=2 * RING, ox=3, y=RECVS * Y_RING)


def odd(v):
    return lax.rem(v, 2)


def offsets(counts):
    out = {}
    for name in counts:
        out[name] = sum(counts[k] for k in out)
    return out


SND_AT, RCV_AT = offsets(SND), offsets(RCV)


def kernel(x_in, gain, wq_in, wkv_in, wo_in, pos, y_out, k_out, v_out, wo_land,
           hbuf, wq, kv, v_t, posk, obuf, wbuf, acc, early, sc0, sc1, pr0, pr1, out_t, qacc, qbuf,
           loc, snd, rcv, hf_r, hb_r, ld, ready):
    me = lax.axis_index("model")
    core = odd(me)
    quad = lax.rem(me // 2, QUADS)
    z = me // 8
    width = hbuf.shape[3]
    half = width // 2
    cw = half // CHUNKS
    upper = z // 2
    away = 1 - 2 * upper

    def zof(d):
        return d + upper * (3 - 2 * d)

    e = zof(z)
    end, mid = e == 0, e == 1
    base = me - 8 * z
    dx = 2 - 4 * odd(quad)
    dy = 4 - 8 * (quad // 2)
    sib, xn, yn, dg = me + 1 - 2 * core, me + dx, me + dy, me + dx + dy
    fwd = base + 8 * (z + away)
    bwd = base + 8 * (z - away * e)
    zpeers = [base + 8 * lax.rem(z + i, QUADS) for i in (1, 2, 3)]
    bufs = ((sc0, pr0), (sc1, pr1))

    def put(src, dst, ssem, rsem, dev):
        return pltpu.make_async_remote_copy(src, dst, ssem, rsem, device_id=(dev,), device_id_type=MESH)

    def send(kind, src, dst, dev, i=0):
        return put(src, dst, snd.at[SND_AT[kind] + (i if SND[kind] > 1 else 0)], rcv.at[RCV_AT[kind] + i], dev)

    def sent(kind, like):
        send(kind, like, like, sib).wait_send()

    def got(kind, like, i=0):
        send(kind, like, like, sib, i).wait_recv()

    def kv_z(i):
        blk = kv.at[z, :, core]
        return send("kvz", blk, blk, zpeers[i], i)

    def kv_p(i):
        blk = kv.at[z, quad, core]
        return send("kvp", blk, blk, (xn, yn, dg)[i], i)

    def kv_d():
        blk = kv.at[:, :, core]
        return send("kvd", blk, blk, sib)

    hh = HD // 2

    def hrows(zz, cc, i):
        return hbuf.at[zz, cc, pl.ds(hh * i, hh), :]

    def h_put(n, zz, i, rsem, dev):
        return put(hrows(zz, 0, i), hrows(zz, 0, i), snd.at[SND_AT["h"] + n], rsem, dev)

    def h_own(i, rsems):
        return h_put(i, z, i, rsems.at[i], fwd)

    def h_own_b(i):
        return h_put(2 + i, z, i, hf_r.at[i], bwd)

    def h_f2b(i):
        return h_put(4 + i, zof(e + 1 + i // 2), i % 2, hf_r.at[2 + i], bwd)

    def h_b2f(i):
        return h_put(8 + i, zof(e - 1), i, hf_r.at[2 + i], fwd)

    def h_d(i):
        zz = z if i < 2 else (zof(e + i // 2) if i < 8 else zof(e - 1))
        return send("hd", hrows(zz, 0, i % 2), hrows(zz, 1, i % 2), sib, i)

    def f_half(i):
        zz = zof(e + 1 + i // 2)
        h_put(0, zz, i % 2, hf_r.at[i], fwd).wait_recv()
        h_d(2 + i).start()
        if i < 4:
            @pl.when(mid)
            def _():
                h_f2b(i).start()

    def b_half(i):
        @pl.when(mid)
        def _():
            h_put(0, zof(e - 1), i, hb_r.at[i], bwd).wait_recv()
            h_d(8 + i).start()
            h_b2f(i).start()

    def h_block_wait(b):
        for i in BOTH:
            h_d(2 * b + i).wait_recv()

    nb = wq.shape[1]
    hb = nb // 2

    def w_piece(dev, i):
        x = dev is xn
        if i < 4:
            rows = (slice(3), slice(3, nb), slice(hb), slice(hb, nb))[i]
            h = i // 2
            src = wq_in.at[rows, :, pl.ds(HD * h, HD)]
            dst = wq.at[1 + h, rows, :, pl.ds(0 if x else HD, HD)]
        else:
            h = i - 4
            rows = slice(hb) if x else slice(hb, nb)
            src = wq.at[1 + h, rows, :, pl.ds(HD if x else 0, HD)]
            dst = wq.at[3, rows, :, pl.ds(HD * h, HD)]
        return send("wx" if x else "wy", src, dst, dev, i)

    w_x, w_y = (functools.partial(w_piece, dev) for dev in (xn, yn))

    def wo_sib():
        src = wo_in.at[:, pl.ds(pl.multiple_of((1 - core) * half, half), half)]
        return send("wod", src, wo_land.at[1, 0], sib)

    def cols(ch):
        return pl.ds(pl.multiple_of(ch * cw, cw), cw)

    def own_cols(ch):
        return pl.ds(pl.multiple_of(core * half + ch * cw, cw), cw)

    def wo_piece(dev, i, ch):
        x = dev is xn
        src = (wo_in.at[:, own_cols(ch)], wo_land.at[1, 0, :, cols(ch)], wo_land.at[0 if x else 1, 2 if x else 1, :, cols(ch)])[i]
        part = (0, 1, 0 if x else 1)[i]
        dst = wo_land.at[part, 3 if i == 2 else 1 if x else 2, :, cols(ch)]
        return send("wox" if x else "woy", src, dst, dev, 2 * lax.rem(ch, RING) + i // 2)

    wo_x, wo_y = (functools.partial(wo_piece, dev) for dev in (xn, yn))

    def wo_own(ch):
        for i in BOTH:
            wo_x(i, ch).start()
            wo_y(i, ch).start()

    def wo_tick(ch):
        got("wox", wo_land.at[:, 1, :, cols(ch)], 2 * lax.rem(ch, RING))
        got("woy", wo_land.at[:, 2, :, cols(ch)], 2 * lax.rem(ch, RING))
        wo_x(2, ch).start()
        wo_y(2, ch).start()

        @pl.when(ch + AHEAD < CHUNKS)
        def _():
            wo_own(ch + AHEAD)

    def wo_arrive(ch):
        wo_x(2, ch).wait_recv()
        wo_y(2, ch).wait_recv()

    def load(g, slot, src, dst):
        return pltpu.make_async_copy(src, dst, ld.at[g, slot])

    def loads(g, ch, slot):
        w = wbuf.at[g, slot]
        rest = slice(1, QUADS)
        return (load(g, slot, wo_in.at[:, own_cols(ch)], w.at[0, 0]),
                load(g, slot, wo_land.at[0, rest, :, cols(ch)], w.at[0, rest]),
                load(g, slot, wo_land.at[1, :, :, cols(ch)], w.at[1]))

    lags = (e, 2, 4 - e)

    def loaded(g, ch, slot):
        load(g, slot, wo_land.at[:, :, :, cols(ch)], wbuf.at[g, slot]).wait()

    skip = (1 - e) * len(EARLY)

    def start_loads(g, ch, slot):
        for c in loads(g, ch, slot):
            c.start()

    def each_load(step, act):
        for g, (lag, lowest, past) in enumerate(zip(lags, (skip, 0, 0), (CHUNKS - 1, e * CHUNKS, CHUNKS))):
            ch = step - lag

            @pl.when((ch >= lowest) & (ch < past))
            def _():
                act(g, ch, odd(ch))

    def kof(k):
        return zof(k + e * (lax.rem(k + 1, 3) + 2 * (k // 3) - k))

    def o_x(k, cc):
        lo = obuf.shape[3] // 2
        zz = kof(k)
        group = (1, 0, 0, 2)[k]
        return send("ox", obuf.at[zz, cc, :, :lo], obuf.at[zz, 1 - cc, :, lo:], sib, group)

    def o_got(group):
        rows = slice(1 if group else 2)
        got("ox", obuf.at[rows, :, :, :obuf.shape[3] // 2], group)

    x_copy, wkv_copy, wq_copy = (
        pltpu.make_async_copy(src, dst, loc.at[i])
        for i, (src, dst) in enumerate(((x_in, hbuf.at[z, 0]), (wkv_in, wbuf.at[:2]), (wq_in, wq.at[0]))))
    x_copy.start()
    wkv_copy.start()
    wq_copy.start()
    barrier = pltpu.get_barrier_semaphore()
    peers = zpeers + [xn, yn, dg, sib]
    for dev in peers:
        pl.semaphore_signal(barrier, device_id=(dev,), device_id_type=MESH)
    pl.semaphore_wait(barrier, len(peers))
    w_x(0).start()
    w_y(0).start()
    x_copy.wait()

    @pl.loop(0, 8)
    def _(i):
        rows = pl.ds(pl.multiple_of(i * 16, 16), 16)
        x = hbuf[z, 0, rows, :].astype(F32)
        cent = x - jnp.mean(x, axis=-1, keepdims=True)
        var = jnp.mean(cent * cent, axis=-1, keepdims=True)
        hbuf[z, 0, rows, :] = (cent * lax.rsqrt(var + NORM_EPS) * gain[:]).astype(BF16)

    wkv_copy.wait()
    kv[z, quad, core] = jnp.dot(hbuf[z, 0], wbuf[:2].reshape(width, PAIR), preferred_element_type=F32).astype(BF16)
    for i in THREE:
        kv_p(i).start()
    for i in (1, 3, 2):
        w_x(i).start()
    for i in (1, 2, 3):
        w_y(i).start()
    for i in BOTH:
        h_d(i).start()
    wo_sib().start()
    for i in THREE:
        kv_p(i).wait_recv()
    for i in THREE:
        kv_z(i).start()
    for i in BOTH:
        @pl.when(end)
        def _():
            h_own(i, hb_r).start()

        @pl.when(mid)
        def _():
            h_own_b(i).start()
            h_own(i, hf_r).start()

    @pl.loop(0, posk.shape[0] // HD)
    def _(i):
        blk = pl.ds(pl.multiple_of(i * HD, HD), HD)
        posk[blk, :] = jnp.broadcast_to(pos[:, blk], (HD, HD)).T

    def rows_of(ref, zz):
        return ref[zz].reshape(PAIR, ref.shape[3])

    def keep_q():
        q = qacc[:].astype(BF16)
        qbuf[:PAIR] = q[:, :HD]
        qbuf[PAIR:] = q[:, HD:]

    def parts(part):
        split = (part + 1) // 2
        return [[(g + split * (i - g), i + split * (part - 1 - i)) for i in BOTH] for g in BOTH]

    def head_pair(p, part, g):
        return p + g * ((part + 1) // 2)

    def q_dot(unit, js, ws):
        zz, p, part = unit
        for g in BOTH:
            rows = [hbuf[zz, cc, pl.ds(pl.multiple_of(r * hh, hh), hh), js] for cc, r in parts(part)[g]]
            w = wq[head_pair(p, part, g), ws].reshape(-1, PAIR)
            yield g, jnp.dot(jnp.concatenate(rows, axis=0), w, preferred_element_type=F32)

    def whole_q(unit):
        for g, part in q_dot(unit, slice(None), slice(None)):
            qacc[g * HD:(g + 1) * HD] = part
        keep_q()

    def unit_of(codes, last):
        k, p, part = (lax.rem(c + v, QUADS) for c, v in zip(codes, last))
        return kof(k), p, part

    wq_copy.wait()
    h_block_wait(0)
    whole_q((z, 0, 0))
    for i in THREE:
        kv_z(i).wait_recv()
    kv_d().start()
    kv_d().wait_recv()
    kv_copies = [pltpu.make_async_copy(kv.at[:, :, :, :, pl.ds(HD * i, HD)], o, loc.at[3 + i]) for i, o in enumerate((k_out, v_out))]
    for c in kv_copies:
        c.start()
    for j in range(QUADS):
        v_t[:, j * KEYS:(j + 1) * KEYS] = kv[j].reshape(KEYS, PAIR)[:, HD:].T

    blocks = [(k, cc) for k in range(QUADS) for cc in BOTH]
    places = nb

    def place(i):
        return wq.at[i // places, lax.rem(i, places)]

    def y_send(i, ch, off, dev):
        return send("y", place(RECVS * CHUNKS + ch * SENDS + i), place(ch * RECVS + off), dev, RECVS * lax.rem(ch, Y_RING) + off)

    def y_recv(ch, off):
        blk = place(ch * RECVS + off)
        got("y", blk, RECVS * lax.rem(ch, Y_RING) + off)
        return blk[:].astype(F32)

    def y_local(ch):
        return pltpu.make_async_copy(hbuf.at[0, 0, :, cols(ch)], y_out.at[:, own_cols(ch)], loc.at[5])

    def y_sib(ch):
        return send("yd", hbuf.at[0, 1, :, cols(ch)], y_out.at[:, own_cols(ch)], sib)

    def weights(g, ch):
        return wbuf[g, odd(ch)].reshape(obuf.shape[3], cw)

    def go_on(j, ch, i, off, dev):
        place(RECVS * CHUNKS + ch * SENDS + i)[:] = acc[j].astype(BF16)
        y_send(i, ch, off, dev).start()

    o_parts = ((EARLY[0] - 1, blocks[2:6]), (EARLY[1], blocks[:2]), (len(TILES) - 1, blocks[6:]))

    def early_send(c, i):
        return send("pre", early.at[1, c, i], early.at[0, c, i], fwd, SENDS * c + i)

    def y_early(c):
        start_loads(c // 2, c, c % 2)
        loaded(c // 2, c, c % 2)
        for i in (1, 2):
            early_sum(c, i)

    def early_sum(c, i):
        early[1, c, i] = jnp.dot(rows_of(obuf, zof(3 - i)), weights(c // 2, c), preferred_element_type=F32).astype(BF16)
        early_send(c, i).start()

    def y_recv_early(n, ch, off):
        @pl.when(ch < len(EARLY))
        def _():
            blk = early.at[0, ch, off]
            got("pre", blk, SENDS * ch + off)
            acc[n] += blk[:].astype(F32)

        @pl.when(ch >= len(EARLY))
        def _():
            acc[n] += y_recv(ch, off)

    scale = HD ** -0.5 * LOG2E
    n = 2 * PAIR
    kq = width // QUADS

    def tile(s, carry):
        codes, ahead = carry[:3], carry[3:]
        zz, p, part = unit_of(codes, LAST)
        following = unit_of(ahead, TILES[0])
        carry = tuple(c // QUADS for c in carry)

        for i, at in enumerate(TICKS):
            @pl.when(s == at)
            def _():
                wo_tick(i)

        @pl.when((s == LATE[-1] - 1) & end)
        def _():
            f_half(5)

        q = qbuf[:]
        tok = (zz * QUADS + quad) * 2
        pq = [pos[:, pl.ds(pl.multiple_of((tok + c) * HD, HD), HD)] for c in (core, 1 - core)]
        pq = [[v[:, :hh], v[:, hh:]] for v in pq]
        split, second = (part + 1) // 2, part // 2
        of_core = [v[0] + second * (v[1] - v[0]) for v in pq]
        pq = [pq[g][i] + split * (of_core[i] - pq[g][i]) for g in BOTH for i in BOTH]
        pq = jnp.broadcast_to(jnp.concatenate(pq + pq, axis=1), (8, n))

        def scores(j):
            keys = kv[j].reshape(KEYS, PAIR)[:, :HD]
            sc = lax.dot_general(keys, q, (((1,), (1,)), ((), ())), preferred_element_type=F32)
            pk = posk[j * KEYS:(j + 1) * KEYS, :]
            pk = jnp.concatenate([pk] * (n // HD), axis=1).reshape(KEYS // 8, 8, n)
            sc = jnp.where(pk <= pq, sc.reshape(KEYS // 8, 8, n), MASKED)
            bufs[j % 2][0][:] = sc.reshape(KEYS, n)
            return jnp.max(jnp.max(sc, axis=0), axis=0, keepdims=True)

        def weigh(j, m):
            pr = jnp.exp2((bufs[j % 2][0][:].reshape(KEYS // 8, 8, n) - jnp.broadcast_to(m, (8, n))) * scale)
            bufs[j % 2][1][:] = pr.reshape(KEYS, n).astype(BF16)
            return jnp.sum(pr, axis=0)

        def add_values(j, alpha):
            got = jnp.dot(v_t[:, j * KEYS:(j + 1) * KEYS], bufs[j % 2][1][:], preferred_element_type=F32)
            out_t[:] = got if alpha is None else out_t[:] * alpha + got

        m = scores(0)
        alpha = den = None
        for j in range(QUADS):
            if j + 1 < QUADS:
                mn = jnp.maximum(m, scores(j + 1))
            for g, got in q_dot(following, slice(j * kq, (j + 1) * kq), slice(j * nb // QUADS, (j + 1) * nb // QUADS)):
                rows = slice(g * HD, (g + 1) * HD)
                qacc[rows] = got if j == 0 else qacc[rows] + got
            ps = weigh(j, m)
            if j > 0:
                add_values(j - 1, alpha if j > 1 else None)
            den = ps if j == 0 else den * now + ps
            if j > 0:
                alpha = now
            if j < QUADS - 1:
                now = jnp.exp2((m - mn) * scale)
                m = mn
        add_values(QUADS - 1, alpha)
        out = (out_t[:] / jnp.sum(den, axis=0, keepdims=True)).T.astype(BF16)
        for g in BOTH:
            hp = head_pair(p, part, g)
            for j, c in enumerate((2 * hp - hp // 2 + hp // 3, 2 * hp + 1 + (hp + 1) // 2 - hp // 2 - hp // 3)):
                for i, (cc, r) in enumerate(parts(part)[g]):
                    row = (2 * j + g) * HD + i * hh
                    obuf[zz, cc, pl.ds(pl.multiple_of(r * hh, hh), hh), pl.ds(pl.multiple_of(c * HD, HD), HD)] = out[row:row + hh]
        keep_q()

        def late(i):
            if i == 1:
                for c in BOTH:
                    w_x(c).wait_recv()
                    w_y(c).wait_recv()
                f_half(0)
                b_half(0)
            elif i == 2:
                f_half(1)
                b_half(1)
                h_block_wait(1)
                w_x(3).wait_recv()
                w_y(2).wait_recv()
                for c in HANDED_ON:
                    w_x(c).start()
                    w_y(c).start()
                wo_sib().wait_recv()
                wo_own(0)
                wo_own(1)
            elif i == 4:
                w_x(2).wait_recv()
                w_y(3).wait_recv()
                f_half(2)
            elif i == 6:
                f_half(3)

                @pl.when(end)
                def _():
                    h_block_wait(2)

                @pl.when(mid)
                def _():
                    h_block_wait(4)
            elif i == LATE[5]:
                for c in HANDED_ON:
                    w_x(c).wait_recv()
                    w_y(c).wait_recv()
            else:
                c = 0 if i == LATE[4] else 1

                @pl.when(end)
                def _():
                    if c == 0:
                        f_half(4)
                    h_d(6 + c).wait_recv()

                @pl.when(mid)
                def _():
                    h_d(4 + c).wait_recv()

        for i in LATE:
            @pl.when(s + 1 == i)
            def _():
                late(i)
        is_late = (s == LATE[0] - 1)
        for i in LATE[1:]:
            is_late = is_late | (s == i - 1)

        @pl.when(is_late)
        def _():
            whole_q(unit_of(carry[:3], LAST))

        for at, some in o_parts:
            @pl.when(s == at)
            def _():
                for b in some:
                    o_x(*b).start()

        for i, at in enumerate(EARLY):
            @pl.when(s == at)
            def _():
                wo_arrive(i)
                if i == 0:
                    o_got(0)

            @pl.when((s == at) & end)
            def _():
                y_early(i)
        return carry

    lax.fori_loop(0, len(TILES), tile, tuple(jnp.int32(t) for t in TABLES))

    o_got(2)

    @pl.when(end)
    def _():
        for c in THREE:
            early_sum(c, 0)
    for i in BOTH:
        @pl.when(end)
        def _():
            h_own(i, hb_r).wait_send()

        @pl.when(mid)
        def _():
            h_own_b(i).wait_send()
            h_own(i, hf_r).wait_send()
            h_b2f(i).wait_send()
            h_f2b(i).wait_send()
            h_f2b(2 + i).wait_send()
    sent("hd", hbuf.at[:, 0])
    w_bytes = wq.at[:3, :hb]
    sent("wx", w_bytes)
    sent("wy", w_bytes)

    @pl.when(end)
    def _():
        pl.semaphore_signal(ready.at[1], device_id=(fwd,), device_id_type=MESH)

    @pl.when(mid)
    def _():
        pl.semaphore_signal(ready.at[0], device_id=(fwd,), device_id_type=MESH)
        pl.semaphore_signal(ready.at[0], device_id=(bwd,), device_id_type=MESH)

    o_got(1)
    pl.semaphore_wait(ready.at[0], 1)

    @pl.when(mid)
    def _():
        pl.semaphore_wait(ready.at[1], 1)

    def y_step(t, _):
        each_load(t, loaded)
        ch_a, ch_b, ch_c = (t - lag for lag in lags)

        @pl.when(ch_a == CHUNKS - 2)
        def _():
            loaded(0, CHUNKS - 1, 1)

        def farther(count, off):
            last = (ch_a + 2) // CHUNKS
            for j in range(count):
                u = (ch_a + 2 - CHUNKS) * count + j
                i = j + last * (u // 2 - j)
                ch = ch_a + last * (CHUNKS - 2 + odd(u + 6 * CHUNKS) - ch_a)
                acc[j] = jnp.dot(rows_of(obuf, zof(3 - i)), weights(0, ch), preferred_element_type=F32)
                if off:
                    y_recv_early(j, ch, i)
                go_on(j, ch, i, i + off, fwd)

        in_range = (ch_a >= skip) & (ch_a < CHUNKS)

        @pl.when(end & in_range)
        def _():
            farther(3, 0)

        @pl.when(mid & in_range)
        def _():
            farther(2, 3)

        @pl.when(mid & (ch_b >= 0) & (ch_b < CHUNKS))
        def _():
            acc[2] = jnp.dot(rows_of(obuf, zof(0)), weights(1, ch_b), preferred_element_type=F32)
            acc[2] += y_recv(ch_b, 3)
            go_on(2, ch_b, 2, 3, bwd)

        @pl.when((t + AHEAD >= len(TICKS)) & (t + AHEAD < CHUNKS))
        def _():
            wo_tick(t + AHEAD)

        nxt = t + 1

        @pl.when((nxt >= len(EARLY)) & (nxt < CHUNKS - 1 + e))
        def _():
            wo_arrive(nxt)

        @pl.when(end & (t == CHUNKS - 3))
        def _():
            wo_arrive(CHUNKS - 1)

        @pl.when(ch_a == CHUNKS - 3)
        def _():
            start_loads(0, CHUNKS - 1, 1)
        each_load(nxt, start_loads)

        @pl.when((ch_c >= 0) & (ch_c < CHUNKS))
        def _():
            acc[3] = jnp.dot(rows_of(obuf, z), weights(2, ch_c), preferred_element_type=F32)

            @pl.when(end)
            def _():
                acc[3] += y_recv(ch_c, 3)

            @pl.when(mid)
            def _():
                y_recv_early(3, ch_c, 2)
                acc[3] += y_recv(ch_c, 4)
            hbuf[0, :, :, cols(ch_c)] = acc[3].astype(BF16).reshape(2, HD, cw)
            y_local(ch_c).start()
            y_sib(ch_c).start()
        return 0

    lax.fori_loop(0, CHUNKS + 4, y_step, 0)

    sent("wox", w_bytes)
    sent("woy", w_bytes)
    whole = slice(half)
    pltpu.make_async_copy(hbuf.at[0, 0, :, whole], y_out.at[:, whole], loc.at[5]).wait()
    sent("yd", hbuf.at[0, 1, :, whole])
    got("yd", hbuf.at[0, 1, :, whole])
    sent("ox", obuf.at[:, :, :, :obuf.shape[3] // 2])

    @pl.when(end)
    def _():
        sent("y", wq.at[:SENDS, :CHUNKS - len(EARLY)])
        sent("pre", early.at[1])

    @pl.when(mid)
    def _():
        sent("y", wq.at[:SENDS, :CHUNKS])
    for i in THREE:
        kv_z(i).wait_send()
        kv_p(i).wait_send()
    kv_d().wait_send()
    wo_sib().wait_send()
    for c in kv_copies:
        c.wait()


def finish(y_in, k_in, v_in, y_out, k_out, v_out, y_buf, kv_buf, read, written):
    parts = [(y_in.at[:, pl.ds(c * KEYS, KEYS)], y_buf.at[c], y_out.at[:, pl.ds(c * KEYS, KEYS)]) for c in range(y_buf.shape[0])]
    parts += [(k_in, kv_buf.at[0], k_out), (v_in, kv_buf.at[1], v_out)]
    copies = [(pltpu.make_async_copy(src, buf, read.at[i]), pltpu.make_async_copy(buf, dst, written.at[i]))
              for i, (src, buf, dst) in enumerate(parts)]
    for c, _ in copies:
        c.start()
    for c, d in copies:
        c.wait()
        d.start()
    for _, d in copies:
        d.wait()


def solution(mesh):
    def local_step(x_loc, ln_gain, wq_loc, w_kv, wo_loc, positions):
        rows, width = x_loc.shape
        tokens = positions.shape[0]
        dma, vmem = pltpu.SemaphoreType.DMA, pltpu.VMEM
        hbm = pl.BlockSpec(memory_space=pl.ANY)
        vm = pl.BlockSpec(memory_space=pltpu.VMEM)
        half = width // 2
        cw = half // CHUNKS
        nb, n = width // PAIR, 2 * PAIR
        kv_shape = (QUADS, QUADS, 2, rows, HD)
        wkv_shape = (2, 2, 2, QUADS, PAIR, cw)
        y, k, v, _ = pl.pallas_call(
            kernel,
            name="mqa_layer",
            out_shape=tuple(jax.ShapeDtypeStruct(s, BF16) for s in ((rows, width), kv_shape, kv_shape, (2, QUADS, PAIR, half))),
            in_specs=[hbm, vm, hbm, hbm, hbm, vm],
            out_specs=(hbm, hbm, hbm, hbm),
            scratch_shapes=[
                vmem((QUADS, 2, rows, width), BF16),
                vmem((QUADS, nb, PAIR, PAIR), BF16),
                vmem((QUADS, QUADS, 2, rows, PAIR), BF16),
                vmem((HD, tokens), BF16),
                vmem((tokens, HD), I32),
                vmem((QUADS, 2, rows, 2 * KEYS), BF16),
                vmem((3,) + wkv_shape[1:], BF16),
                vmem((QUADS, PAIR, cw), F32),
                vmem((2, len(EARLY), SENDS, PAIR, cw), BF16),
                vmem((KEYS, n), F32), vmem((KEYS, n), F32),
                vmem((KEYS, n), BF16), vmem((KEYS, n), BF16),
                vmem((HD, n), F32),
                vmem((PAIR, PAIR), F32),
                vmem((n, HD), BF16),
                dma((6,)), dma((sum(SND.values()),)), dma((sum(RCV.values()),)), dma((6,)), dma((2,)), dma((3, 2)),
                pltpu.SemaphoreType.REGULAR((2,)),
            ],
            compiler_params=pltpu.CompilerParams(
                collective_id=0, has_side_effects=True, vmem_limit_bytes=67043328),
        )(x_loc, ln_gain.reshape(1, width), wq_loc.reshape(nb, PAIR, PAIR), w_kv.reshape(wkv_shape), wo_loc, positions.reshape(1, tokens))
        parts = width // KEYS
        return pl.pallas_call(
            finish,
            name="outputs",
            out_shape=tuple(jax.ShapeDtypeStruct(s, BF16) for s in ((rows, width), (tokens, HD), (tokens, HD))),
            in_specs=[hbm] * 3,
            out_specs=(hbm,) * 3,
            scratch_shapes=[vmem((parts, rows, KEYS), BF16), vmem((2, tokens, HD), BF16), dma((parts + 2,)), dma((parts + 2,))],
        )(y, k.reshape(tokens, HD), v.reshape(tokens, HD))

    split, whole = P("model", None), P(None, None)
    return jax.shard_map(
        local_step,
        mesh=mesh,
        in_specs=(split, P(None), P(None, "model"), whole, split, P(None)),
        out_specs=(split, whole, whole),
        check_vma=False,
    )
```

```python
import functools

import jax
import jax.numpy as jnp
from jax import lax
from jax.experimental import pallas as pl
from jax.experimental.pallas import tpu as pltpu
from jax.sharding import PartitionSpec as P

NORM_EPS = 1e-6
LOG2E = 1.4426950408889634
MESH = pl.DeviceIdType.MESH
BF16, F32, I32 = jnp.bfloat16, jnp.float32, jnp.int32
HD = 128
PAIR = 2 * HD
KEYS = 8 * HD
QUADS = 4
CHUNKS = 16
AHEAD = 2
MASKED = -1e30
BOTH, THREE = range(2), range(3)
HANDED_ON = (4, 5)

TILES = ((0, 0, 0), (0, 1, 0), (1, 0, 0), (1, 1, 0), (0, 2, 0), (1, 2, 0), (2, 0, 0), (2, 1, 0), (2, 2, 0), (1, 3, 0),
         (2, 3, 0), (3, 0, 1), (3, 2, 1), (3, 0, 2), (3, 2, 2), (0, 3, 0))
LATE = (1, 2, 4, 6, 9, 13)
EARLY = range(11, 14)
FAR = 14
LAST = TILES[-1]
NEXT = [TILES[0] if i in LATE else t for i, t in enumerate(TILES)][1:]


def digits(values):
    return sum((v % 4) << (2 * i) for i, v in enumerate(values))


TABLES = [digits(t[c] - LAST[c] for t in TILES) for c in THREE] + [digits(t[c] for t in NEXT) for c in THREE]

SENDS, RECVS = 3, 5
RING, Y_RING = 4, 8

KINDS = ("kvz", "kvp", "kvd", "h", "hd", "wx", "wy", "pre", "wod", "wox", "woy", "ox", "y", "yd")
SND = dict.fromkeys(KINDS, 1) | dict(kvz=3, kvp=3, h=10)
RCV = dict.fromkeys(KINDS, 1) | dict(kvz=3, kvp=3, hd=10, wx=6, wy=6, pre=9, wox=2 * RING, woy=2 * RING, ox=3, y=RECVS * Y_RING)


def odd(v):
    return lax.rem(v, 2)


def offsets(counts):
    out = {}
    for name in counts:
        out[name] = sum(counts[k] for k in out)
    return out


SND_AT, RCV_AT = offsets(SND), offsets(RCV)


def kernel(x_in, gain_in, wq_in, wkv_in, wo_in, pos_in, y_out, k_out, v_out, wo_land,
           hbuf, gain, pos, wq, kv, v_t, posk, obuf, wbuf, acc, early, sc0, sc1, pr0, pr1, out_t, qacc, qbuf,
           loc, snd, rcv, hf_r, hb_r, ld, ready):
    me = lax.axis_index("model")
    core = odd(me)
    quad = lax.rem(me // 2, QUADS)
    z = me // 8
    width = hbuf.shape[3]
    half = width // 2
    cw = half // CHUNKS
    upper = z // 2
    away = 1 - 2 * upper

    def zof(d):
        return d + upper * (3 - 2 * d)

    e = zof(z)
    end, mid = e == 0, e == 1
    base = me - 8 * z
    dx = 2 - 4 * odd(quad)
    dy = 4 - 8 * (quad // 2)
    sib, xn, yn, dg = me + 1 - 2 * core, me + dx, me + dy, me + dx + dy
    fwd = base + 8 * (z + away)
    bwd = base + 8 * (z - away * e)
    zpeers = [base + 8 * lax.rem(z + i, QUADS) for i in (1, 2, 3)]
    bufs = ((sc0, pr0), (sc1, pr1))

    def put(src, dst, ssem, rsem, dev):
        return pltpu.make_async_remote_copy(src, dst, ssem, rsem, device_id=(dev,), device_id_type=MESH)

    def send(kind, src, dst, dev, i=0):
        return put(src, dst, snd.at[SND_AT[kind] + (i if SND[kind] > 1 else 0)], rcv.at[RCV_AT[kind] + i], dev)

    def sent(kind, like):
        send(kind, like, like, sib).wait_send()

    def got(kind, like, i=0):
        send(kind, like, like, sib, i).wait_recv()

    def kv_z(i):
        blk = kv.at[z, :, core]
        return send("kvz", blk, blk, zpeers[i], i)

    def kv_p(i):
        blk = kv.at[z, quad, core]
        return send("kvp", blk, blk, (xn, yn, dg)[i], i)

    def kv_d():
        blk = kv.at[:, :, core]
        return send("kvd", blk, blk, sib)

    hh = HD // 2

    def hrows(zz, cc, i):
        return hbuf.at[zz, cc, pl.ds(hh * i, hh), :]

    def h_put(n, zz, i, rsem, dev):
        return put(hrows(zz, 0, i), hrows(zz, 0, i), snd.at[SND_AT["h"] + n], rsem, dev)

    def h_own(i, rsems):
        return h_put(i, z, i, rsems.at[i], fwd)

    def h_own_b(i):
        return h_put(2 + i, z, i, hf_r.at[i], bwd)

    def h_f2b(i):
        return h_put(4 + i, zof(e + 1 + i // 2), i % 2, hf_r.at[2 + i], bwd)

    def h_b2f(i):
        return h_put(8 + i, zof(e - 1), i, hf_r.at[2 + i], fwd)

    def h_d(i):
        zz = z if i < 2 else (zof(e + i // 2) if i < 8 else zof(e - 1))
        return send("hd", hrows(zz, 0, i % 2), hrows(zz, 1, i % 2), sib, i)

    def f_half(i):
        zz = zof(e + 1 + i // 2)
        h_put(0, zz, i % 2, hf_r.at[i], fwd).wait_recv()
        h_d(2 + i).start()
        if i < 4:
            @pl.when(mid)
            def _():
                h_f2b(i).start()

    def b_half(i):
        @pl.when(mid)
        def _():
            h_put(0, zof(e - 1), i, hb_r.at[i], bwd).wait_recv()
            h_d(8 + i).start()
            h_b2f(i).start()

    def h_block_wait(b):
        for i in BOTH:
            h_d(2 * b + i).wait_recv()

    def half_block_wait(c):
        pl.when(end)(lambda: h_d(6 + c).wait_recv())
        pl.when(mid)(lambda: h_d(4 + c).wait_recv())

    nb = wq.shape[1]
    hb = nb // 2

    def w_piece(dev, i):
        x = dev is xn
        lower, upper = slice(hb), slice(hb, nb)
        halves = (upper, lower) if x else (lower, upper)
        if i < 4:
            rows = (slice(3), slice(3, nb), *halves)[i]
            h = i // 2
            src = wq_in.at[rows, :, pl.ds(HD * h, HD)]
            dst = wq.at[1 + h, rows, :, pl.ds(0 if x else HD, HD)]
        else:
            h = i - 4
            rows = halves[1]
            src = wq.at[1 + h, rows, :, pl.ds(HD if x else 0, HD)]
            dst = wq.at[3, rows, :, pl.ds(HD * h, HD)]
        return send("wx" if x else "wy", src, dst, dev, i)

    def w_start(*pieces):
        for i in pieces:
            w_piece(xn, i).start()
            w_piece(yn, i).start()

    def w_got(*pieces):
        for i in pieces:
            w_piece(xn, i).wait_recv()
            w_piece(yn, i).wait_recv()

    def wo_sib():
        src = wo_in.at[:, pl.ds(pl.multiple_of((1 - core) * half, half), half)]
        return send("wod", src, wo_land.at[1, 0], sib)

    def cols(ch):
        return pl.ds(pl.multiple_of(ch * cw, cw), cw)

    def own_cols(ch):
        return pl.ds(pl.multiple_of(core * half + ch * cw, cw), cw)

    def wo_piece(dev, i, ch):
        x = dev is xn
        src = (wo_in.at[:, own_cols(ch)], wo_land.at[1, 0, :, cols(ch)], wo_land.at[0 if x else 1, 2 if x else 1, :, cols(ch)])[i]
        part = (0, 1, 0 if x else 1)[i]
        dst = wo_land.at[part, 3 if i == 2 else 1 if x else 2, :, cols(ch)]
        return send("wox" if x else "woy", src, dst, dev, 2 * lax.rem(ch, RING) + i // 2)

    wo_x, wo_y = (functools.partial(wo_piece, dev) for dev in (xn, yn))

    def wo_own(ch):
        for i in BOTH:
            wo_x(i, ch).start()
            wo_y(i, ch).start()

    def wo_pass(ch, *more):
        got("wox", wo_land.at[:, 1, :, cols(ch)], 2 * lax.rem(ch, RING))
        got("woy", wo_land.at[:, 2, :, cols(ch)], 2 * lax.rem(ch, RING))
        wo_x(2, ch).start()
        wo_y(2, ch).start()
        for nxt in more:
            @pl.when(nxt < CHUNKS)
            def _():
                wo_own(nxt)

    def wo_arrive(ch):
        wo_x(2, ch).wait_recv()
        wo_y(2, ch).wait_recv()

    def load(g, slot, src, dst):
        return pltpu.make_async_copy(src, dst, ld.at[g, slot])

    def loads(g, ch, slot):
        w = wbuf.at[g, slot]
        rest = slice(1, QUADS)
        return (load(g, slot, wo_in.at[:, own_cols(ch)], w.at[0, 0]),
                load(g, slot, wo_land.at[0, rest, :, cols(ch)], w.at[0, rest]),
                load(g, slot, wo_land.at[1, :, :, cols(ch)], w.at[1]))

    lags = (e, 2, 4 - e)

    def loaded(g, ch, slot):
        load(g, slot, wo_land.at[:, :, :, cols(ch)], wbuf.at[g, slot]).wait()

    skip = (1 - e) * len(EARLY)

    def start_loads(g, ch, slot):
        for c in loads(g, ch, slot):
            c.start()

    def each_load(step, act):
        for g, (lag, lowest, past) in enumerate(zip(lags, (skip, 0, 0), (CHUNKS - 1, e * CHUNKS, CHUNKS))):
            ch = step - lag

            @pl.when((ch >= lowest) & (ch < past))
            def _():
                act(g, ch, odd(ch))

    def kof(k):
        return zof(k + e * (lax.rem(k + 1, 3) + 2 * (k // 3) - k))

    def o_x(k, cc):
        lo = obuf.shape[3] // 2
        zz = kof(k)
        group = (1, 0, 0, 2)[k]
        return send("ox", obuf.at[zz, cc, :, :lo], obuf.at[zz, 1 - cc, :, lo:], sib, group)

    def o_got(group):
        rows = slice(1 if group else 2)
        got("ox", obuf.at[rows, :, :, :obuf.shape[3] // 2], group)

    x_copy, gain_copy, wkv_copy, wq_copy, pos_copy = first = [
        pltpu.make_async_copy(src, dst, loc.at[i])
        for i, (src, dst) in enumerate(((x_in, hbuf.at[z, 0]), (gain_in, gain), (wkv_in, wbuf.at[:2]), (wq_in, wq.at[0]), (pos_in, pos)))]
    for c in first:
        c.start()
    barrier = pltpu.get_barrier_semaphore()
    peers = zpeers + [xn, yn, dg, sib]
    for dev in peers:
        pl.semaphore_signal(barrier, device_id=(dev,), device_id_type=MESH)
    pl.semaphore_wait(barrier, len(peers))
    w_start(0)
    x_copy.wait()
    gain_copy.wait()

    @pl.loop(0, 8)
    def _(i):
        rows = pl.ds(pl.multiple_of(i * 16, 16), 16)
        x = hbuf[z, 0, rows, :].astype(F32)
        cent = x - jnp.mean(x, axis=-1, keepdims=True)
        var = jnp.mean(cent * cent, axis=-1, keepdims=True)
        hbuf[z, 0, rows, :] = (cent * lax.rsqrt(var + NORM_EPS) * gain[:]).astype(BF16)

    wkv_copy.wait()
    kv[z, quad, core] = jnp.dot(hbuf[z, 0], wbuf[:2].reshape(width, PAIR), preferred_element_type=F32).astype(BF16)
    for i in THREE:
        kv_p(i).start()
    w_start(1, 2, 3)
    for i in BOTH:
        h_d(i).start()
    wo_sib().start()
    for i in THREE:
        kv_p(i).wait_recv()
    for i in THREE:
        kv_z(i).start()
    for i in BOTH:
        @pl.when(end)
        def _():
            h_own(i, hb_r).start()

        @pl.when(mid)
        def _():
            h_own_b(i).start()
            h_own(i, hf_r).start()

    pos_copy.wait()

    @pl.loop(0, posk.shape[0] // HD)
    def _(i):
        blk = pl.ds(pl.multiple_of(i * HD, HD), HD)
        posk[blk, :] = jnp.broadcast_to(pos[:, blk], (HD, HD)).T

    def rows_of(ref, zz):
        return ref[zz].reshape(PAIR, ref.shape[3])

    def keep_q():
        q = qacc[:].astype(BF16)
        qbuf[:PAIR] = q[:, :HD]
        qbuf[PAIR:] = q[:, HD:]

    def parts(part):
        split = (part + 1) // 2
        return [[(g + split * (i - g), i + split * (part - 1 - i)) for i in BOTH] for g in BOTH]

    def head_pair(p, part, g):
        return p + g * ((part + 1) // 2)

    def q_dot(unit, js, ws):
        zz, p, part = unit
        for g in BOTH:
            rows = [hbuf[zz, cc, pl.ds(pl.multiple_of(r * hh, hh), hh), js] for cc, r in parts(part)[g]]
            w = wq[head_pair(p, part, g), ws].reshape(-1, PAIR)
            yield g, jnp.dot(jnp.concatenate(rows, axis=0), w, preferred_element_type=F32)

    def whole_q(unit):
        for g, part in q_dot(unit, slice(None), slice(None)):
            qacc[g * HD:(g + 1) * HD] = part
        keep_q()

    def unit_of(codes, last):
        k, p, part = (lax.rem(c + v, QUADS) for c, v in zip(codes, last))
        return kof(k), p, part

    wq_copy.wait()
    h_block_wait(0)
    whole_q((z, 0, 0))
    for i in THREE:
        kv_z(i).wait_recv()
    kv_d().start()
    kv_d().wait_recv()
    kv_copies = [pltpu.make_async_copy(kv.at[:, :, :, :, pl.ds(HD * i, HD)], o, loc.at[len(first) + i]) for i, o in enumerate((k_out, v_out))]
    for c in kv_copies:
        c.start()
    for j in range(QUADS):
        v_t[:, j * KEYS:(j + 1) * KEYS] = kv[j].reshape(KEYS, PAIR)[:, HD:].T

    blocks = [(k, cc) for k in range(QUADS) for cc in BOTH]
    places = nb

    def place(i):
        return wq.at[i // places, lax.rem(i, places)]

    def y_send(i, ch, off, dev):
        return send("y", place(RECVS * CHUNKS + ch * SENDS + i), place(ch * RECVS + off), dev, RECVS * lax.rem(ch, Y_RING) + off)

    def y_recv(ch, off):
        blk = place(ch * RECVS + off)
        got("y", blk, RECVS * lax.rem(ch, Y_RING) + off)
        return blk[:].astype(F32)

    def y_local(ch):
        return pltpu.make_async_copy(hbuf.at[0, 0, :, cols(ch)], y_out.at[:, own_cols(ch)], loc.at[7])

    def y_sib(ch):
        return send("yd", hbuf.at[0, 1, :, cols(ch)], y_out.at[:, own_cols(ch)], sib)

    def weights(g, ch):
        return wbuf[g, odd(ch)].reshape(obuf.shape[3], cw)

    def go_on(j, ch, i, off, dev):
        place(RECVS * CHUNKS + ch * SENDS + i)[:] = acc[j].astype(BF16)
        y_send(i, ch, off, dev).start()

    o_parts = ((EARLY[0] - 1, blocks[2:6]), (FAR + 1, blocks[:2]), (FAR, blocks[6:]))

    def early_send(c, i):
        return send("pre", early.at[1, c, i], early.at[0, c, i], fwd, SENDS * c + i)

    def y_early(c):
        start_loads(c // 2, c, c % 2)
        loaded(c // 2, c, c % 2)
        for i in (1, 2):
            early_sum(c, i)

    def early_sum(c, i):
        early[1, c, i] = jnp.dot(rows_of(obuf, zof(3 - i)), weights(c // 2, c), preferred_element_type=F32).astype(BF16)
        early_send(c, i).start()

    def y_recv_early(n, ch, off):
        @pl.when(ch < len(EARLY))
        def _():
            blk = early.at[0, ch, off]
            got("pre", blk, SENDS * ch + off)
            acc[n] += blk[:].astype(F32)

        @pl.when(ch >= len(EARLY))
        def _():
            acc[n] += y_recv(ch, off)

    def pairs_0():
        w_got(*BOTH)
        f_half(0)
        b_half(0)

    def rows_1():
        f_half(1)
        b_half(1)
        h_block_wait(1)
        w_got(2)
        w_start(*HANDED_ON)
        wo_sib().wait_recv()
        wo_own(0)
        wo_own(1)

    def pairs_1():
        w_got(3)
        f_half(2)

    def rows_2():
        f_half(3)
        pl.when(end)(lambda: h_block_wait(2))
        pl.when(mid)(lambda: h_block_wait(4))

    def pairs_2():
        pl.when(end)(lambda: f_half(4))
        w_got(*HANDED_ON)

    late = dict(zip(LATE, (pairs_0, rows_1, pairs_1, rows_2, pairs_2, lambda: half_block_wait(1))))

    def before(i):
        if i == LATE[4] + 1:
            yield lambda: half_block_wait(0)
        if i == EARLY[0]:
            yield lambda: wo_pass(0)
        if i == FAR + 1:
            yield lambda: wo_pass(4, 6)

    def after(i):
        for at, some in o_parts:
            if at == i:
                for b in some:
                    yield lambda b=b: o_x(*b).start()
        if i == LATE[-1] - 1:
            yield lambda: pl.when(end)(lambda: f_half(5))
        if i in EARLY:
            c = EARLY.index(i)
            if c == 0:
                yield lambda: wo_pass(1, 2)
                yield lambda: o_got(0)
            yield lambda: wo_arrive(c)
            yield lambda: pl.when(end)(lambda: y_early(c))
            if c == 1:
                yield lambda: wo_pass(2, 3, 4)
        if i == FAR:
            yield lambda: wo_pass(3, 5)
            yield lambda: o_got(2)
            for c in THREE:
                yield lambda c=c: pl.when(end)(lambda: early_sum(c, 0))
        if i + 1 in late:
            yield late[i + 1]

    def by_tile(s, due, lo=0, hi=len(TILES)):
        if not any(True for i in range(lo, hi) for _ in due(i)):
            return
        if hi - lo == 1:
            for act in due(lo):
                act()
            return
        half_way = (lo + hi) // 2
        pl.when(s < half_way)(lambda: by_tile(s, due, lo, half_way))
        pl.when(s >= half_way)(lambda: by_tile(s, due, half_way, hi))

    scale = HD ** -0.5 * LOG2E
    n = 2 * PAIR
    kq = width // QUADS

    def tile(s, carry):
        codes, ahead = carry[:3], carry[3:]
        zz, p, part = unit_of(codes, LAST)
        following = unit_of(ahead, TILES[0])
        carry = tuple(c // QUADS for c in carry)

        by_tile(s, before)
        q = qbuf[:]
        tok = (zz * QUADS + quad) * 2
        pq = [pos[:, pl.ds(pl.multiple_of((tok + c) * HD, HD), HD)] for c in (core, 1 - core)]
        pq = [[v[:, :hh], v[:, hh:]] for v in pq]
        split, second = (part + 1) // 2, part // 2
        of_core = [v[0] + second * (v[1] - v[0]) for v in pq]
        pq = [pq[g][i] + split * (of_core[i] - pq[g][i]) for g in BOTH for i in BOTH]
        pq = jnp.broadcast_to(jnp.concatenate(pq + pq, axis=1), (8, n))

        def scores(j):
            keys = kv[j].reshape(KEYS, PAIR)[:, :HD]
            sc = lax.dot_general(keys, q, (((1,), (1,)), ((), ())), preferred_element_type=F32)
            pk = posk[j * KEYS:(j + 1) * KEYS, :]
            pk = jnp.concatenate([pk] * (n // HD), axis=1).reshape(KEYS // 8, 8, n)
            sc = jnp.where(pk <= pq, sc.reshape(KEYS // 8, 8, n), MASKED)
            bufs[j % 2][0][:] = sc.reshape(KEYS, n)
            return jnp.max(jnp.max(sc, axis=0), axis=0, keepdims=True)

        def weigh(j, m):
            pr = jnp.exp2((bufs[j % 2][0][:].reshape(KEYS // 8, 8, n) - jnp.broadcast_to(m, (8, n))) * scale)
            bufs[j % 2][1][:] = pr.reshape(KEYS, n).astype(BF16)
            return jnp.sum(pr, axis=0)

        def add_values(j, alpha):
            got = jnp.dot(v_t[:, j * KEYS:(j + 1) * KEYS], bufs[j % 2][1][:], preferred_element_type=F32)
            out_t[:] = got if alpha is None else out_t[:] * alpha + got

        m = scores(0)
        alpha = den = None
        for j in range(QUADS):
            if j + 1 < QUADS:
                mn = jnp.maximum(m, scores(j + 1))
            for g, got in q_dot(following, slice(j * kq, (j + 1) * kq), slice(j * nb // QUADS, (j + 1) * nb // QUADS)):
                rows = slice(g * HD, (g + 1) * HD)
                qacc[rows] = got if j == 0 else qacc[rows] + got
            ps = weigh(j, m)
            if j > 0:
                add_values(j - 1, alpha if j > 1 else None)
            den = ps if j == 0 else den * now + ps
            if j > 0:
                alpha = now
            if j < QUADS - 1:
                now = jnp.exp2((m - mn) * scale)
                m = mn
        add_values(QUADS - 1, alpha)
        out = (out_t[:] / jnp.sum(den, axis=0, keepdims=True)).T.astype(BF16)
        for g in BOTH:
            hp = head_pair(p, part, g)
            for j, c in enumerate((2 * hp - hp // 2 + hp // 3, 2 * hp + 1 + (hp + 1) // 2 - hp // 2 - hp // 3)):
                for i, (cc, r) in enumerate(parts(part)[g]):
                    row = (2 * j + g) * HD + i * hh
                    obuf[zz, cc, pl.ds(pl.multiple_of(r * hh, hh), hh), pl.ds(pl.multiple_of(c * HD, HD), HD)] = out[row:row + hh]
        keep_q()

        by_tile(s, after)
        is_late = s == LATE[0] - 1
        for i in LATE[1:]:
            is_late = is_late | (s == i - 1)

        @pl.when(is_late)
        def _():
            whole_q(unit_of(carry[:3], LAST))

        return carry

    lax.fori_loop(0, len(TILES), tile, tuple(jnp.int32(t) for t in TABLES))

    for i in BOTH:
        @pl.when(end)
        def _():
            h_own(i, hb_r).wait_send()

        @pl.when(mid)
        def _():
            h_own_b(i).wait_send()
            h_own(i, hf_r).wait_send()
            h_b2f(i).wait_send()
            h_f2b(i).wait_send()
            h_f2b(2 + i).wait_send()
    sent("hd", hbuf.at[:, 0])
    w_bytes = wq.at[:3, :hb]
    sent("wx", w_bytes)
    sent("wy", w_bytes)

    pl.semaphore_signal(ready.at[1 - e], device_id=(fwd,), device_id_type=MESH)

    @pl.when(mid)
    def _():
        pl.semaphore_signal(ready.at[0], device_id=(bwd,), device_id_type=MESH)
        pl.semaphore_wait(ready.at[1])
    pl.semaphore_wait(ready.at[0])

    def y_step(t, _):
        each_load(t, loaded)
        ch_a, ch_b, ch_c = (t - lag for lag in lags)

        @pl.when(ch_a == CHUNKS - 2)
        def _():
            loaded(0, CHUNKS - 1, 1)

        def farther(count, off):
            last = (ch_a + 2) // CHUNKS
            for j in range(count):
                u = (ch_a + 2 - CHUNKS) * count + j
                i = j + last * (u // 2 - j)
                ch = ch_a + last * (CHUNKS - 2 + odd(u + 6 * CHUNKS) - ch_a)
                acc[j] = jnp.dot(rows_of(obuf, zof(3 - i)), weights(0, ch), preferred_element_type=F32)
                if off:
                    y_recv_early(j, ch, i)
                go_on(j, ch, i, i + off, fwd)

        in_range = (ch_a >= skip) & (ch_a < CHUNKS)

        @pl.when(end & in_range)
        def _():
            farther(3, 0)

        @pl.when(mid & in_range)
        def _():
            farther(2, 3)

        @pl.when(mid & (ch_b >= 0) & (ch_b < CHUNKS))
        def _():
            acc[2] = jnp.dot(rows_of(obuf, zof(0)), weights(1, ch_b), preferred_element_type=F32)
            acc[2] += y_recv(ch_b, 3)
            go_on(2, ch_b, 2, 3, bwd)

        passing = t + AHEAD

        @pl.when((passing > 4) & (passing < CHUNKS))
        def _():
            wo_pass(passing, passing + AHEAD)

        nxt = t + 1

        @pl.when((nxt >= len(EARLY)) & (nxt < CHUNKS - 1 + e))
        def _():
            wo_arrive(nxt)

        @pl.when(end & (t == CHUNKS - 3))
        def _():
            wo_arrive(CHUNKS - 1)

        @pl.when(ch_a == CHUNKS - 3)
        def _():
            start_loads(0, CHUNKS - 1, 1)
        each_load(nxt, start_loads)

        @pl.when(ch_c == 0)
        def _():
            o_got(1)

        @pl.when((ch_c >= 0) & (ch_c < CHUNKS))
        def _():
            acc[3] = jnp.dot(rows_of(obuf, z), weights(2, ch_c), preferred_element_type=F32)

            @pl.when(end)
            def _():
                acc[3] += y_recv(ch_c, 3)

            @pl.when(mid)
            def _():
                y_recv_early(3, ch_c, 2)
                acc[3] += y_recv(ch_c, 4)
            hbuf[0, :, :, cols(ch_c)] = acc[3].astype(BF16).reshape(2, HD, cw)
            y_local(ch_c).start()
            y_sib(ch_c).start()
        return 0

    lax.fori_loop(0, CHUNKS + 4, y_step, 0)

    sent("wox", w_bytes)
    sent("woy", w_bytes)
    whole = slice(half)
    pltpu.make_async_copy(hbuf.at[0, 0, :, whole], y_out.at[:, whole], loc.at[7]).wait()
    sent("yd", hbuf.at[0, 1, :, whole])
    got("yd", hbuf.at[0, 1, :, whole])
    sent("ox", obuf.at[:, :, :, :obuf.shape[3] // 2])

    @pl.when(end)
    def _():
        sent("y", wq.at[:SENDS, :CHUNKS - len(EARLY)])
        sent("pre", early.at[1])

    @pl.when(mid)
    def _():
        sent("y", wq.at[:SENDS, :CHUNKS])
    for i in THREE:
        kv_z(i).wait_send()
        kv_p(i).wait_send()
    kv_d().wait_send()
    wo_sib().wait_send()
    for c in kv_copies:
        c.wait()


def finish(y_in, k_in, v_in, y_out, k_out, v_out, y_buf, kv_buf, read, written):
    parts = [(y_in.at[:, pl.ds(c * KEYS, KEYS)], y_buf.at[c], y_out.at[:, pl.ds(c * KEYS, KEYS)]) for c in range(y_buf.shape[0])]
    parts += [(i.at[pl.ds(c * KEYS, KEYS)], kv_buf.at[n, c], o.at[pl.ds(c * KEYS, KEYS)])
              for c in range(QUADS) for n, (i, o) in enumerate(((k_in, k_out), (v_in, v_out)))]
    copies = [(pltpu.make_async_copy(src, buf, read.at[i]), pltpu.make_async_copy(buf, dst, written.at[i]))
              for i, (src, buf, dst) in enumerate(parts)]
    for c, _ in copies:
        c.start()
    for c, d in copies:
        c.wait()
        d.start()
    for _, d in copies:
        d.wait()


def solution(mesh):
    def local_step(x_loc, ln_gain, wq_loc, w_kv, wo_loc, positions):
        rows, width = x_loc.shape
        tokens = positions.shape[0]
        dma, vmem = pltpu.SemaphoreType.DMA, pltpu.VMEM
        hbm = pl.BlockSpec(memory_space=pl.ANY)
        half = width // 2
        cw = half // CHUNKS
        nb, n = width // PAIR, 2 * PAIR
        kv_shape = (QUADS, QUADS, 2, rows, HD)
        wkv_shape = (2, 2, 2, QUADS, PAIR, cw)
        y, k, v, _ = pl.pallas_call(
            kernel,
            name="mqa_layer",
            out_shape=tuple(jax.ShapeDtypeStruct(s, BF16) for s in ((rows, width), kv_shape, kv_shape, (2, QUADS, PAIR, half))),
            in_specs=[hbm] * 6,
            out_specs=(hbm, hbm, hbm, hbm),
            scratch_shapes=[
                vmem((QUADS, 2, rows, width), BF16),
                vmem((1, width), F32), vmem((1, tokens), I32),
                vmem((QUADS, nb, PAIR, PAIR), BF16),
                vmem((QUADS, QUADS, 2, rows, PAIR), BF16),
                vmem((HD, tokens), BF16),
                vmem((tokens, HD), I32),
                vmem((QUADS, 2, rows, 2 * KEYS), BF16),
                vmem((3,) + wkv_shape[1:], BF16),
                vmem((QUADS, PAIR, cw), F32),
                vmem((2, len(EARLY), SENDS, PAIR, cw), BF16),
                vmem((KEYS, n), F32), vmem((KEYS, n), F32),
                vmem((KEYS, n), BF16), vmem((KEYS, n), BF16),
                vmem((HD, n), F32),
                vmem((PAIR, PAIR), F32),
                vmem((n, HD), BF16),
                dma((8,)), dma((sum(SND.values()),)), dma((sum(RCV.values()),)), dma((6,)), dma((2,)), dma((3, 2)),
                pltpu.SemaphoreType.REGULAR((2,)),
            ],
            compiler_params=pltpu.CompilerParams(
                collective_id=0, has_side_effects=True, vmem_limit_bytes=67043328),
        )(x_loc, ln_gain.reshape(1, width), wq_loc.reshape(nb, PAIR, PAIR), w_kv.reshape(wkv_shape), wo_loc, positions.reshape(1, tokens))
        parts = width // KEYS
        return pl.pallas_call(
            finish,
            name="outputs",
            out_shape=tuple(jax.ShapeDtypeStruct(s, BF16) for s in ((rows, width), (tokens, HD), (tokens, HD))),
            in_specs=[hbm] * 3,
            out_specs=(hbm,) * 3,
            scratch_shapes=[vmem((parts, rows, KEYS), BF16), vmem((2, QUADS, KEYS, HD), BF16)] + [dma((parts + 2 * QUADS,))] * 2,
        )(y, k.reshape(tokens, HD), v.reshape(tokens, HD))

    split, whole = P("model", None), P(None, None)
    return jax.shard_map(
        local_step,
        mesh=mesh,
        in_specs=(split, P(), P(None, "model"), whole, split, P()),
        out_specs=(split, whole, whole),
        check_vma=False,
    )
```

```python
import functools

import jax
import jax.numpy as jnp
from jax import lax
from jax.experimental import pallas as pl
from jax.experimental.pallas import tpu as pltpu
from jax.sharding import PartitionSpec as P

NORM_EPS = 1e-6
LOG2E = 1.4426950408889634
MESH = pl.DeviceIdType.MESH
BF16, F32, I32 = jnp.bfloat16, jnp.float32, jnp.int32
HD = 128
PAIR = 2 * HD
KEYS = 8 * HD
QUADS = 4
CHUNKS = 16
AHEAD = 2
MASKED = -1e30
BOTH, THREE = range(2), range(3)
HANDED_ON = (4, 5)

TILES = ((0, 0, 0), (0, 1, 0), (1, 0, 0), (1, 1, 0), (0, 2, 0), (1, 2, 0), (2, 0, 0), (2, 1, 0), (2, 2, 0), (3, 0, 1),
         (1, 3, 0), (2, 3, 0), (3, 2, 1), (3, 0, 2), (3, 2, 2), (0, 3, 0))
LATE = (1, 2, 4, 6, 9, 10, 13)
FAR = 14
EARLY = (FAR - 2, FAR - 2, FAR - 1)
LAST = TILES[-1]
NEXT = [TILES[0] if i in LATE else t for i, t in enumerate(TILES)][1:]


def digits(values):
    return sum((v % 4) << (2 * i) for i, v in enumerate(values))


TABLES = [digits(t[c] - LAST[c] for t in TILES) for c in THREE] + [digits(t[c] for t in NEXT) for c in THREE]

SENDS, RECVS = 3, 5
RING, Y_RING = 4, 8

KINDS = ("kvz", "kvp", "kvd", "h", "hd", "wx", "wy", "pre", "wod", "wox", "woy", "ox", "y", "yd")
SND = dict.fromkeys(KINDS, 1) | dict(kvz=3, kvp=3, h=10)
RCV = dict.fromkeys(KINDS, 1) | dict(kvz=3, kvp=3, hd=10, wx=6, wy=6, pre=9, wox=2 * RING, woy=2 * RING, ox=3, y=RECVS * Y_RING)


def odd(v):
    return lax.rem(v, 2)


def offsets(counts):
    out = {}
    for name in counts:
        out[name] = sum(counts[k] for k in out)
    return out


SND_AT, RCV_AT = offsets(SND), offsets(RCV)


def kernel(x_in, gain_in, wq_in, wkv_in, wo_in, pos_in, y_out, kv, wo_land,
           hbuf, gain, pos, wq, v_t, posk, obuf, wbuf, acc, early, sc0, sc1, pr0, pr1, out_t, qacc, qbuf,
           loc, snd, rcv, hf_r, hb_r, ld, ready):
    me = lax.axis_index("model")
    core = odd(me)
    quad = lax.rem(me // 2, QUADS)
    z = me // 8
    width = hbuf.shape[3]
    half = width // 2
    cw = half // CHUNKS
    upper = z // 2
    away = 1 - 2 * upper

    def zof(d):
        return d + upper * (3 - 2 * d)

    e = zof(z)
    end, mid = e == 0, e == 1
    base = me - 8 * z
    dx = 2 - 4 * odd(quad)
    dy = 4 - 8 * (quad // 2)
    sib, xn, yn, dg = me + 1 - 2 * core, me + dx, me + dy, me + dx + dy
    fwd = base + 8 * (z + away)
    bwd = base + 8 * (z - away * e)
    zpeers = [base + 8 * lax.rem(z + i, QUADS) for i in (1, 2, 3)]
    bufs = ((sc0, pr0), (sc1, pr1))

    def put(src, dst, ssem, rsem, dev):
        return pltpu.make_async_remote_copy(src, dst, ssem, rsem, device_id=(dev,), device_id_type=MESH)

    def send(kind, src, dst, dev, i=0):
        return put(src, dst, snd.at[SND_AT[kind] + (i if SND[kind] > 1 else 0)], rcv.at[RCV_AT[kind] + i], dev)

    def sent(kind, like):
        send(kind, like, like, sib).wait_send()

    def got(kind, like, i=0):
        send(kind, like, like, sib, i).wait_recv()

    def kv_z(i):
        blk = kv.at[z, :, core]
        return send("kvz", blk, blk, zpeers[i], i)

    def kv_p(i):
        blk = kv.at[z, quad, core]
        return send("kvp", blk, blk, (xn, yn, dg)[i], i)

    def kv_d():
        blk = kv.at[:, :, core]
        return send("kvd", blk, blk, sib)

    hh = HD // 2

    def hrows(zz, cc, i):
        return hbuf.at[zz, cc, pl.ds(hh * i, hh), :]

    def h_put(n, zz, i, rsem, dev):
        return put(hrows(zz, 0, i), hrows(zz, 0, i), snd.at[SND_AT["h"] + n], rsem, dev)

    def h_own(i, rsems):
        return h_put(i, z, i, rsems.at[i], fwd)

    def h_own_b(i):
        return h_put(2 + i, z, i, hf_r.at[i], bwd)

    def h_f2b(i):
        return h_put(4 + i, zof(e + 1 + i // 2), i % 2, hf_r.at[2 + i], bwd)

    def h_b2f(i):
        return h_put(8 + i, zof(e - 1), i, hf_r.at[2 + i], fwd)

    def h_d(i):
        zz = z if i < 2 else (zof(e + i // 2) if i < 8 else zof(e - 1))
        return send("hd", hrows(zz, 0, i % 2), hrows(zz, 1, i % 2), sib, i)

    def f_half(i):
        zz = zof(e + 1 + i // 2)
        h_put(0, zz, i % 2, hf_r.at[i], fwd).wait_recv()
        h_d(2 + i).start()
        if i < 4:
            @pl.when(mid)
            def _():
                h_f2b(i).start()

    def b_half(i):
        @pl.when(mid)
        def _():
            h_put(0, zof(e - 1), i, hb_r.at[i], bwd).wait_recv()
            h_d(8 + i).start()
            h_b2f(i).start()

    def h_block_wait(b):
        for i in BOTH:
            h_d(2 * b + i).wait_recv()

    def half_block_wait(c):
        pl.when(end)(lambda: h_d(6 + c).wait_recv())
        pl.when(mid)(lambda: h_d(4 + c).wait_recv())

    nb = wq.shape[1]
    hb = nb // 2

    def w_piece(dev, i):
        x = dev is xn
        lower, upper = slice(hb), slice(hb, nb)
        halves = (upper, lower) if x else (lower, upper)
        if i < 4:
            rows = (slice(4), slice(4, nb), *halves)[i]
            h = i // 2
            src = wq_in.at[rows, :, pl.ds(HD * h, HD)]
            dst = wq.at[1 + h, rows, :, pl.ds(0 if x else HD, HD)]
        else:
            h = i - 4
            rows = halves[1]
            src = wq.at[1 + h, rows, :, pl.ds(HD if x else 0, HD)]
            dst = wq.at[3, rows, :, pl.ds(HD * h, HD)]
        return send("wx" if x else "wy", src, dst, dev, i)

    def w_start(*pieces):
        for i in pieces:
            w_piece(xn, i).start()
            w_piece(yn, i).start()

    def w_got(*pieces):
        for i in pieces:
            w_piece(xn, i).wait_recv()
            w_piece(yn, i).wait_recv()

    def wo_sib():
        src = wo_in.at[:, pl.ds(pl.multiple_of((1 - core) * half, half), half)]
        return send("wod", src, wo_land.at[1, 0], sib)

    def cols(ch):
        return pl.ds(pl.multiple_of(ch * cw, cw), cw)

    def own_cols(ch):
        return pl.ds(pl.multiple_of(core * half + ch * cw, cw), cw)

    def wo_piece(dev, i, ch):
        x = dev is xn
        src = (wo_in.at[:, own_cols(ch)], wo_land.at[1, 0, :, cols(ch)], wo_land.at[0 if x else 1, 2 if x else 1, :, cols(ch)])[i]
        part = (0, 1, 0 if x else 1)[i]
        dst = wo_land.at[part, 3 if i == 2 else 1 if x else 2, :, cols(ch)]
        return send("wox" if x else "woy", src, dst, dev, 2 * lax.rem(ch, RING) + i // 2)

    wo_x, wo_y = (functools.partial(wo_piece, dev) for dev in (xn, yn))

    def wo_own(ch):
        for i in BOTH:
            wo_x(i, ch).start()
            wo_y(i, ch).start()

    def wo_pass(ch, *more):
        got("wox", wo_land.at[:, 1, :, cols(ch)], 2 * lax.rem(ch, RING))
        got("woy", wo_land.at[:, 2, :, cols(ch)], 2 * lax.rem(ch, RING))
        wo_x(2, ch).start()
        wo_y(2, ch).start()
        for nxt in more:
            @pl.when(nxt < CHUNKS)
            def _():
                wo_own(nxt)

    def wo_arrive(ch):
        wo_x(2, ch).wait_recv()
        wo_y(2, ch).wait_recv()

    def load(g, slot, src, dst):
        return pltpu.make_async_copy(src, dst, ld.at[g, slot])

    def loads(g, ch, slot):
        w = wbuf.at[g, slot]
        rest = slice(1, QUADS)
        return (load(g, slot, wo_in.at[:, own_cols(ch)], w.at[0, 0]),
                load(g, slot, wo_land.at[0, rest, :, cols(ch)], w.at[0, rest]),
                load(g, slot, wo_land.at[1, :, :, cols(ch)], w.at[1]))

    lags = (e, 2, 4 - e)

    def loaded(g, ch, slot):
        load(g, slot, wo_land.at[:, :, :, cols(ch)], wbuf.at[g, slot]).wait()

    skip = (1 - e) * len(EARLY)

    def start_loads(g, ch, slot):
        for c in loads(g, ch, slot):
            c.start()

    def each_load(step, act):
        for g, (lag, lowest, past) in enumerate(zip(lags, (skip, 0, 0), (CHUNKS - 1, e * CHUNKS, CHUNKS))):
            ch = step - lag

            @pl.when((ch >= lowest) & (ch < past))
            def _():
                act(g, ch, odd(ch))

    def kof(k):
        return zof(k + e * (lax.rem(k + 1, 3) + 2 * (k // 3) - k))

    def o_x(k, cc):
        lo = obuf.shape[3] // 2
        zz = kof(k)
        group = (1, 0, 0, 2)[k]
        return send("ox", obuf.at[zz, cc, :, :lo], obuf.at[zz, 1 - cc, :, lo:], sib, group)

    def o_got(group):
        rows = slice(1 if group else 2)
        got("ox", obuf.at[rows, :, :, :obuf.shape[3] // 2], group)

    x_copy, gain_copy, wkv_copy, wq_copy, pos_copy = first = [
        pltpu.make_async_copy(src, dst, loc.at[i])
        for i, (src, dst) in enumerate(((x_in, hbuf.at[z, 0]), (gain_in, gain), (wkv_in, wbuf.at[:2]), (wq_in, wq.at[0]), (pos_in, pos)))]
    for c in first:
        c.start()
    barrier = pltpu.get_barrier_semaphore()
    peers = zpeers + [xn, yn, dg, sib]
    for dev in peers:
        pl.semaphore_signal(barrier, device_id=(dev,), device_id_type=MESH)
    pl.semaphore_wait(barrier, len(peers))
    w_start(0)
    x_copy.wait()
    gain_copy.wait()

    @pl.loop(0, 8)
    def _(i):
        rows = pl.ds(pl.multiple_of(i * 16, 16), 16)
        x = hbuf[z, 0, rows, :].astype(F32)
        cent = x - jnp.mean(x, axis=-1, keepdims=True)
        var = jnp.mean(cent * cent, axis=-1, keepdims=True)
        hbuf[z, 0, rows, :] = (cent * lax.rsqrt(var + NORM_EPS) * gain[:]).astype(BF16)

    wkv_copy.wait()
    kv[z, quad, core] = jnp.dot(hbuf[z, 0], wbuf[:2].reshape(width, PAIR), preferred_element_type=F32).astype(BF16)
    for i in THREE:
        kv_p(i).start()
    w_start(1, 2, 3)
    for i in BOTH:
        h_d(i).start()
    wo_sib().start()
    def own_rows(i):
        @pl.when(end)
        def _():
            h_own(i, hb_r).start()

        @pl.when(mid)
        def _():
            h_own_b(i).start()
            h_own(i, hf_r).start()

    own_rows(0)
    for i in THREE:
        kv_p(i).wait_recv()
    for i in THREE:
        kv_z(i).start()
    own_rows(1)

    pos_copy.wait()

    @pl.loop(0, posk.shape[0] // HD)
    def _(i):
        blk = pl.ds(pl.multiple_of(i * HD, HD), HD)
        posk[blk, :] = jnp.broadcast_to(pos[:, blk], (HD, HD)).T

    def rows_of(ref, zz):
        return ref[zz].reshape(PAIR, ref.shape[3])

    def keep_q():
        q = qacc[:].astype(BF16)
        qbuf[:PAIR] = q[:, :HD]
        qbuf[PAIR:] = q[:, HD:]

    def parts(part):
        split = (part + 1) // 2
        return [[(g + split * (i - g), i + split * (part - 1 - i)) for i in BOTH] for g in BOTH]

    def head_pair(p, part, g):
        return p + g * ((part + 1) // 2)

    def q_dot(unit, js, ws):
        zz, p, part = unit
        for g in BOTH:
            rows = [hbuf[zz, cc, pl.ds(pl.multiple_of(r * hh, hh), hh), js] for cc, r in parts(part)[g]]
            w = wq[head_pair(p, part, g), ws].reshape(-1, PAIR)
            yield g, jnp.dot(jnp.concatenate(rows, axis=0), w, preferred_element_type=F32)

    def whole_q(unit):
        for g, part in q_dot(unit, slice(None), slice(None)):
            qacc[g * HD:(g + 1) * HD] = part
        keep_q()

    def unit_of(codes, last):
        k, p, part = (lax.rem(c + v, QUADS) for c, v in zip(codes, last))
        return kof(k), p, part

    wq_copy.wait()
    h_block_wait(0)
    whole_q((z, 0, 0))
    for i in THREE:
        kv_z(i).wait_recv()
    kv_d().start()
    kv_d().wait_recv()
    for j in range(QUADS):
        v_t[:, j * KEYS:(j + 1) * KEYS] = kv[j].reshape(KEYS, PAIR)[:, HD:].T

    blocks = [(k, cc) for k in range(QUADS) for cc in BOTH]
    places = nb

    def place(i):
        return wq.at[i // places, lax.rem(i, places)]

    def y_send(i, ch, off, dev):
        return send("y", place(RECVS * CHUNKS + ch * SENDS + i), place(ch * RECVS + off), dev, RECVS * lax.rem(ch, Y_RING) + off)

    def y_recv(ch, off):
        blk = place(ch * RECVS + off)
        got("y", blk, RECVS * lax.rem(ch, Y_RING) + off)
        return blk[:].astype(F32)

    def y_sib(ch):
        return send("yd", hbuf.at[0, 1, :, cols(ch)], y_out.at[:, own_cols(ch)], sib)

    def weights(g, ch):
        return wbuf[g, odd(ch)].reshape(obuf.shape[3], cw)

    def go_on(j, ch, i, off, dev):
        place(RECVS * CHUNKS + ch * SENDS + i)[:] = acc[j].astype(BF16)
        y_send(i, ch, off, dev).start()

    o_parts = ((EARLY[0] - 1, blocks[2:6]), (FAR + 1, blocks[:2]), (FAR, blocks[6:]))

    def early_send(c, i):
        return send("pre", early.at[1, c, i], early.at[0, c, i], fwd, SENDS * c + i)

    def y_early(c):
        start_loads(c // 2, c, c % 2)
        loaded(c // 2, c, c % 2)
        for i in (1, 2):
            early_sum(c, i)

    def early_sum(c, i):
        early[1, c, i] = jnp.dot(rows_of(obuf, zof(3 - i)), weights(c // 2, c), preferred_element_type=F32).astype(BF16)
        early_send(c, i).start()

    def y_recv_early(n, ch, off):
        @pl.when(ch < len(EARLY))
        def _():
            blk = early.at[0, ch, off]
            got("pre", blk, SENDS * ch + off)
            acc[n] += blk[:].astype(F32)

        @pl.when(ch >= len(EARLY))
        def _():
            acc[n] += y_recv(ch, off)

    def pairs_0():
        w_got(*BOTH)
        f_half(0)
        b_half(0)

    def rows_1():
        f_half(1)
        b_half(1)
        h_block_wait(1)
        w_got(2)
        w_start(*HANDED_ON)
        wo_sib().wait_recv()
        wo_own(0)
        wo_own(1)

    def pairs_1():
        w_got(3)
        f_half(2)

    def rows_2():
        f_half(3)
        pl.when(end)(lambda: h_block_wait(2))
        pl.when(mid)(lambda: h_block_wait(4))

    def rows_3():
        pl.when(end)(lambda: f_half(4))
        half_block_wait(0)

    late = dict(zip(LATE, (pairs_0, rows_1, pairs_1, rows_2, rows_3, lambda: w_got(*HANDED_ON), lambda: half_block_wait(1))))

    def before(i):
        if i == EARLY[0] - 1:
            yield lambda: wo_pass(0)
        if i == EARLY[0]:
            yield lambda: wo_pass(1, 2)
        if i == FAR + 1:
            yield lambda: wo_pass(4, 6)

    def after(i):
        for at, some in o_parts:
            if at == i:
                for b in some:
                    yield lambda b=b: o_x(*b).start()
        for c, at in enumerate(EARLY):
            if at == i:
                if c == 0:
                    yield lambda: o_got(0)
                if c == 1:
                    yield lambda: pl.when(end)(lambda: f_half(5))
                yield lambda c=c: wo_arrive(c)
                yield lambda c=c: pl.when(end)(lambda: y_early(c))
        if i == EARLY[1]:
            yield lambda: wo_pass(2, 3, 4)
        if i == FAR:
            yield lambda: wo_pass(3, 5)
            yield lambda: o_got(2)
            for c in THREE:
                yield lambda c=c: pl.when(end)(lambda: early_sum(c, 0))
        if i + 1 in late:
            yield late[i + 1]

    def by_tile(s, due, lo=0, hi=len(TILES)):
        if not any(True for i in range(lo, hi) for _ in due(i)):
            return
        if hi - lo == 1:
            for act in due(lo):
                act()
            return
        half_way = (lo + hi) // 2
        pl.when(s < half_way)(lambda: by_tile(s, due, lo, half_way))
        pl.when(s >= half_way)(lambda: by_tile(s, due, half_way, hi))

    scale = HD ** -0.5 * LOG2E
    n = 2 * PAIR
    kq = width // QUADS

    def tile(s, carry):
        codes, ahead = carry[:3], carry[3:]
        zz, p, part = unit_of(codes, LAST)
        following = unit_of(ahead, TILES[0])
        carry = tuple(c // QUADS for c in carry)

        by_tile(s, before)
        q = qbuf[:]
        tok = (zz * QUADS + quad) * 2
        pq = [pos[:, pl.ds(pl.multiple_of((tok + c) * HD, HD), HD)] for c in (core, 1 - core)]
        pq = [[v[:, :hh], v[:, hh:]] for v in pq]
        split, second = (part + 1) // 2, part // 2
        of_core = [v[0] + second * (v[1] - v[0]) for v in pq]
        pq = [pq[g][i] + split * (of_core[i] - pq[g][i]) for g in BOTH for i in BOTH]
        pq = jnp.broadcast_to(jnp.concatenate(pq + pq, axis=1), (8, n))

        def scores(j):
            keys = kv[j].reshape(KEYS, PAIR)[:, :HD]
            sc = lax.dot_general(keys, q, (((1,), (1,)), ((), ())), preferred_element_type=F32)
            pk = posk[j * KEYS:(j + 1) * KEYS, :]
            pk = jnp.concatenate([pk] * (n // HD), axis=1).reshape(KEYS // 8, 8, n)
            sc = jnp.where(pk <= pq, sc.reshape(KEYS // 8, 8, n), MASKED)
            bufs[j % 2][0][:] = sc.reshape(KEYS, n)
            return jnp.max(jnp.max(sc, axis=0), axis=0, keepdims=True)

        def weigh(j, m):
            pr = jnp.exp2((bufs[j % 2][0][:].reshape(KEYS // 8, 8, n) - jnp.broadcast_to(m, (8, n))) * scale)
            bufs[j % 2][1][:] = pr.reshape(KEYS, n).astype(BF16)
            return jnp.sum(pr, axis=0)

        def add_values(j, alpha):
            got = jnp.dot(v_t[:, j * KEYS:(j + 1) * KEYS], bufs[j % 2][1][:], preferred_element_type=F32)
            out_t[:] = got if alpha is None else out_t[:] * alpha + got

        m = scores(0)
        alpha = den = None
        for j in range(QUADS):
            if j + 1 < QUADS:
                mn = jnp.maximum(m, scores(j + 1))
            for g, got in q_dot(following, slice(j * kq, (j + 1) * kq), slice(j * nb // QUADS, (j + 1) * nb // QUADS)):
                rows = slice(g * HD, (g + 1) * HD)
                qacc[rows] = got if j == 0 else qacc[rows] + got
            ps = weigh(j, m)
            if j > 0:
                add_values(j - 1, alpha if j > 1 else None)
            den = ps if j == 0 else den * now + ps
            if j > 0:
                alpha = now
            if j < QUADS - 1:
                now = jnp.exp2((m - mn) * scale)
                m = mn
        add_values(QUADS - 1, alpha)
        out = (out_t[:] / jnp.sum(den, axis=0, keepdims=True)).T.astype(BF16)
        for g in BOTH:
            hp = head_pair(p, part, g)
            for j, c in enumerate((2 * hp - hp // 2 + hp // 3, 2 * hp + 1 + (hp + 1) // 2 - hp // 2 - hp // 3)):
                for i, (cc, r) in enumerate(parts(part)[g]):
                    row = (2 * j + g) * HD + i * hh
                    obuf[zz, cc, pl.ds(pl.multiple_of(r * hh, hh), hh), pl.ds(pl.multiple_of(c * HD, HD), HD)] = out[row:row + hh]
        keep_q()

        by_tile(s, after)
        is_late = s == LATE[0] - 1
        for i in LATE[1:]:
            is_late = is_late | (s == i - 1)

        @pl.when(is_late)
        def _():
            whole_q(unit_of(carry[:3], LAST))

        return carry

    lax.fori_loop(0, len(TILES), tile, tuple(jnp.int32(t) for t in TABLES))

    for i in BOTH:
        @pl.when(end)
        def _():
            h_own(i, hb_r).wait_send()

        @pl.when(mid)
        def _():
            h_own_b(i).wait_send()
            h_own(i, hf_r).wait_send()
            h_b2f(i).wait_send()
            h_f2b(i).wait_send()
            h_f2b(2 + i).wait_send()
    sent("hd", hbuf.at[:, 0])
    w_bytes = wq.at[:3, :hb]
    sent("wx", w_bytes)
    sent("wy", w_bytes)

    pl.semaphore_signal(ready.at[1 - e], device_id=(fwd,), device_id_type=MESH)

    @pl.when(mid)
    def _():
        pl.semaphore_signal(ready.at[0], device_id=(bwd,), device_id_type=MESH)
        pl.semaphore_wait(ready.at[1])
    pl.semaphore_wait(ready.at[0])

    def y_step(t, _):
        each_load(t, loaded)
        ch_a, ch_b, ch_c = (t - lag for lag in lags)

        @pl.when(ch_a == CHUNKS - 2)
        def _():
            loaded(0, CHUNKS - 1, 1)

        def farther(count, off):
            last = (ch_a + 2) // CHUNKS
            for j in range(count):
                u = (ch_a + 2 - CHUNKS) * count + j
                i = j + last * (u // 2 - j)
                ch = ch_a + last * (CHUNKS - 2 + odd(u + 6 * CHUNKS) - ch_a)
                acc[j] = jnp.dot(rows_of(obuf, zof(3 - i)), weights(0, ch), preferred_element_type=F32)
                if off:
                    y_recv_early(j, ch, i)
                go_on(j, ch, i, i + off, fwd)

        in_range = (ch_a >= skip) & (ch_a < CHUNKS)

        @pl.when(end & in_range)
        def _():
            farther(3, 0)

        @pl.when(mid & in_range)
        def _():
            farther(2, 3)

        @pl.when(mid & (ch_b >= 0) & (ch_b < CHUNKS))
        def _():
            acc[2] = jnp.dot(rows_of(obuf, zof(0)), weights(1, ch_b), preferred_element_type=F32)
            acc[2] += y_recv(ch_b, 3)
            go_on(2, ch_b, 2, 3, bwd)

        passing = t + AHEAD

        @pl.when((passing > 4) & (passing < CHUNKS))
        def _():
            wo_pass(passing, passing + AHEAD)

        nxt = t + 1

        @pl.when((nxt >= len(EARLY)) & (nxt < CHUNKS - 1 + e))
        def _():
            wo_arrive(nxt)

        @pl.when(end & (t == CHUNKS - 3))
        def _():
            wo_arrive(CHUNKS - 1)

        @pl.when(ch_a == CHUNKS - 3)
        def _():
            start_loads(0, CHUNKS - 1, 1)
        each_load(nxt, start_loads)

        @pl.when(ch_c == 0)
        def _():
            o_got(1)

        @pl.when((ch_c >= 0) & (ch_c < CHUNKS))
        def _():
            acc[3] = jnp.dot(rows_of(obuf, z), weights(2, ch_c), preferred_element_type=F32)

            @pl.when(end)
            def _():
                acc[3] += y_recv(ch_c, 3)

            @pl.when(mid)
            def _():
                y_recv_early(3, ch_c, 2)
                acc[3] += y_recv(ch_c, 4)
            y_out[:, own_cols(ch_c)] = acc[3, :HD].astype(BF16)
            hbuf[0, 1, :, cols(ch_c)] = acc[3, HD:].astype(BF16)
            y_sib(ch_c).start()
        return 0

    lax.fori_loop(0, CHUNKS + 4, y_step, 0)

    sent("wox", w_bytes)
    sent("woy", w_bytes)
    whole = slice(half)
    sent("yd", hbuf.at[0, 1, :, whole])
    got("yd", hbuf.at[0, 1, :, whole])
    sent("ox", obuf.at[:, :, :, :obuf.shape[3] // 2])

    @pl.when(end)
    def _():
        sent("y", wq.at[:SENDS, :CHUNKS - len(EARLY)])
        sent("pre", early.at[1])

    @pl.when(mid)
    def _():
        sent("y", wq.at[:SENDS, :CHUNKS])
    for i in THREE:
        kv_z(i).wait_send()
        kv_p(i).wait_send()
    kv_d().wait_send()
    wo_sib().wait_send()


def finish(y, kv, y_out, k_out, v_out, sems):
    copies = [pltpu.make_async_copy(src, dst, sems.at[i]) for i, (src, dst) in enumerate((
        (y, y_out), (kv.at[:, :, :, :, pl.ds(0, HD)], k_out), (kv.at[:, :, :, :, pl.ds(HD, HD)], v_out)))]
    for c in copies:
        c.start()
    for c in copies:
        c.wait()


def solution(mesh):
    def local_step(x_loc, ln_gain, wq_loc, w_kv, wo_loc, positions):
        rows, width = x_loc.shape
        tokens = positions.shape[0]
        dma, vmem = pltpu.SemaphoreType.DMA, pltpu.VMEM
        hbm = pl.BlockSpec(memory_space=pl.ANY)
        half = width // 2
        cw = half // CHUNKS
        nb, n = width // PAIR, 2 * PAIR
        kv_shape = (QUADS, QUADS, 2, rows, HD)
        wkv_shape = (2, 2, 2, QUADS, PAIR, cw)
        vm = pl.BlockSpec(memory_space=pltpu.VMEM)
        kv_all = (QUADS, QUADS, 2, rows, PAIR)
        y, kv, _ = pl.pallas_call(
            kernel,
            name="mqa_layer",
            out_shape=(vmem((rows, width), BF16), vmem(kv_all, BF16), jax.ShapeDtypeStruct((2, QUADS, PAIR, half), BF16)),
            in_specs=[hbm] * 6,
            out_specs=(vm, vm, hbm),
            scratch_shapes=[
                vmem((QUADS, 2, rows, width), BF16),
                vmem((1, width), F32), vmem((1, tokens), I32),
                vmem((QUADS, nb, PAIR, PAIR), BF16),
                vmem((HD, tokens), BF16),
                vmem((tokens, HD), I32),
                vmem((QUADS, 2, rows, 2 * KEYS), BF16),
                vmem((3,) + wkv_shape[1:], BF16),
                vmem((QUADS, PAIR, cw), F32),
                vmem((2, len(EARLY), SENDS, PAIR, cw), BF16),
                vmem((KEYS, n), F32), vmem((KEYS, n), F32),
                vmem((KEYS, n), BF16), vmem((KEYS, n), BF16),
                vmem((HD, n), F32),
                vmem((PAIR, PAIR), F32),
                vmem((n, HD), BF16),
                dma((5,)), dma((sum(SND.values()),)), dma((sum(RCV.values()),)), dma((6,)), dma((2,)), dma((3, 2)),
                pltpu.SemaphoreType.REGULAR((2,)),
            ],
            compiler_params=pltpu.CompilerParams(
                collective_id=0, has_side_effects=True, vmem_limit_bytes=58 << 20),
        )(x_loc, ln_gain.reshape(1, width), wq_loc.reshape(nb, PAIR, PAIR), w_kv.reshape(wkv_shape), wo_loc, positions.reshape(1, tokens))
        y, k, v = pl.pallas_call(
            finish,
            name="outputs",
            out_shape=tuple(jax.ShapeDtypeStruct(s, BF16) for s in ((rows, width), kv_shape, kv_shape)),
            in_specs=[vm] * 2,
            out_specs=(hbm,) * 3,
            scratch_shapes=[dma((3,))],
            compiler_params=pltpu.CompilerParams(vmem_limit_bytes=1 << 20),
        )(pltpu.with_memory_space_constraint(y, pltpu.VMEM), pltpu.with_memory_space_constraint(kv, pltpu.VMEM))
        return y, k.reshape(tokens, HD), v.reshape(tokens, HD)

    split, whole = P("model", None), P(None, None)
    return jax.shard_map(
        local_step,
        mesh=mesh,
        in_specs=(split, P(), P(None, "model"), whole, split, P()),
        out_specs=(split, whole, whole),
        check_vma=False,
    )
```

```python
import functools

import jax
import jax.numpy as jnp
from jax import lax
from jax.experimental import pallas as pl
from jax.experimental.pallas import tpu as pltpu
from jax.sharding import PartitionSpec as P

NORM_EPS = 1e-6
LOG2E = 1.4426950408889634
MESH = pl.DeviceIdType.MESH
BF16, F32, I32 = jnp.bfloat16, jnp.float32, jnp.int32
HD = 128
PAIR = 2 * HD
KEYS = 8 * HD
QUADS = 4
CHUNKS = 16
LASTS = CHUNKS - 2
AHEAD = 2
MASKED = -1e30
BOTH, THREE = range(2), range(3)
HANDED_ON = (4, 5)

TILES = ((0, 0, 0), (0, 1, 0), (1, 0, 0), (1, 1, 0), (0, 2, 0), (1, 2, 0), (2, 0, 0), (2, 1, 0), (2, 2, 0), (3, 0, 1),
         (1, 3, 0), (2, 3, 0), (3, 2, 1), (3, 0, 2), (3, 2, 2), (0, 3, 0))
LATE = (1, 2, 4, 6, 9, 10, 13)
FAR = 14
EARLY = (FAR - 2, FAR - 2, FAR - 1)
LAST = TILES[-1]
NEXT = [TILES[0] if i in LATE else t for i, t in enumerate(TILES)][1:]


def digits(values):
    return sum((v % 4) << (2 * i) for i, v in enumerate(values))


TABLES = [digits(t[c] - LAST[c] for t in TILES) for c in THREE] + [digits(t[c] for t in NEXT) for c in THREE]

SENDS, RECVS = 3, 5
RING, Y_RING = 4, 8

KINDS = ("kvz", "kvp", "kvd", "h", "hd", "wx", "wy", "pre", "wod", "wox", "woy", "ox", "y", "yd")
SND = dict.fromkeys(KINDS, 1) | dict(kvz=3, kvp=3, h=10)
RCV = dict.fromkeys(KINDS, 1) | dict(kvz=3, kvp=3, hd=10, wx=6, wy=6, pre=9, wox=2 * RING, woy=2 * RING, ox=3, y=RECVS * Y_RING)


def odd(v):
    return lax.rem(v, 2)


def offsets(counts):
    out = {}
    for name in counts:
        out[name] = sum(counts[k] for k in out)
    return out


SND_AT, RCV_AT = offsets(SND), offsets(RCV)


def kernel(x_in, gain_in, wq_in, wkv_in, wo_in, pos_in, y_out, kv, wo_land,
           hbuf, gain, pos, wq, v_t, posk, obuf, wbuf, acc, early, sc0, sc1, pr0, pr1, out_t, qacc, qbuf,
           loc, snd, rcv, hf_r, hb_r, ld, ready):
    me = lax.axis_index("model")
    core = odd(me)
    quad = lax.rem(me // 2, QUADS)
    z = me // 8
    width = hbuf.shape[3]
    half = width // 2
    cw = half // CHUNKS
    upper = z // 2
    away = 1 - 2 * upper

    def zof(d):
        return d + upper * (3 - 2 * d)

    e = zof(z)
    end, mid = e == 0, e == 1
    base = me - 8 * z
    dx = 2 - 4 * odd(quad)
    dy = 4 - 8 * (quad // 2)
    sib, xn, yn, dg = me + 1 - 2 * core, me + dx, me + dy, me + dx + dy
    fwd = base + 8 * (z + away)
    bwd = base + 8 * (z - away * e)
    zpeers = [base + 8 * lax.rem(z + i, QUADS) for i in (1, 2, 3)]
    bufs = ((sc0, pr0), (sc1, pr1))

    def put(src, dst, ssem, rsem, dev):
        return pltpu.make_async_remote_copy(src, dst, ssem, rsem, device_id=(dev,), device_id_type=MESH)

    def send(kind, src, dst, dev, i=0):
        return put(src, dst, snd.at[SND_AT[kind] + (i if SND[kind] > 1 else 0)], rcv.at[RCV_AT[kind] + i], dev)

    def sent(kind, like):
        send(kind, like, like, sib).wait_send()

    def got(kind, like, i=0):
        send(kind, like, like, sib, i).wait_recv()

    def kv_z(i):
        blk = kv.at[z, :, core]
        return send("kvz", blk, blk, zpeers[i], i)

    def kv_p(i):
        blk = kv.at[z, quad, core]
        return send("kvp", blk, blk, (xn, yn, dg)[i], i)

    def kv_d():
        blk = kv.at[:, :, core]
        return send("kvd", blk, blk, sib)

    hh = HD // 2

    def hrows(zz, cc, i):
        return hbuf.at[zz, cc, pl.ds(hh * i, hh), :]

    def h_put(n, zz, i, rsem, dev):
        return put(hrows(zz, 0, i), hrows(zz, 0, i), snd.at[SND_AT["h"] + n], rsem, dev)

    def h_own(i, rsems):
        return h_put(i, z, i, rsems.at[i], fwd)

    def h_own_b(i):
        return h_put(2 + i, z, i, hf_r.at[i], bwd)

    def h_f2b(i):
        return h_put(4 + i, zof(e + 1 + i // 2), i % 2, hf_r.at[2 + i], bwd)

    def h_b2f(i):
        return h_put(8 + i, zof(e - 1), i, hf_r.at[2 + i], fwd)

    def h_d(i):
        zz = z if i < 2 else (zof(e + i // 2) if i < 8 else zof(e - 1))
        return send("hd", hrows(zz, 0, i % 2), hrows(zz, 1, i % 2), sib, i)

    def f_half(i):
        zz = zof(e + 1 + i // 2)
        h_put(0, zz, i % 2, hf_r.at[i], fwd).wait_recv()
        h_d(2 + i).start()
        if i < 4:
            @pl.when(mid)
            def _():
                h_f2b(i).start()

    def b_half(i):
        @pl.when(mid)
        def _():
            h_put(0, zof(e - 1), i, hb_r.at[i], bwd).wait_recv()
            h_d(8 + i).start()
            h_b2f(i).start()

    def h_block_wait(b):
        for i in BOTH:
            h_d(2 * b + i).wait_recv()

    def half_block_wait(c):
        pl.when(end)(lambda: h_d(6 + c).wait_recv())
        pl.when(mid)(lambda: h_d(4 + c).wait_recv())

    nb = wq.shape[1]
    hb = nb // 2

    def w_piece(dev, i):
        y = int(dev is yn)
        lower, upper = slice(hb), slice(hb, nb)
        halves = (lower, upper) if y else (upper, lower)
        if i < 4:
            rows = (slice(4), slice(4, nb), *halves)[i]
            h = i // 2
            src = wq_in.at[rows, :, pl.ds(HD * h, HD)]
            dst = wq.at[1 + h, rows, :, pl.ds(HD * y, HD)]
        else:
            h = i - 4
            rows = halves[1]
            src = wq.at[1 + h, rows, :, pl.ds(HD - HD * y, HD)]
            dst = wq.at[3, rows, :, pl.ds(HD * h, HD)]
        return send("wy" if y else "wx", src, dst, dev, i)

    def w_start(*pieces):
        for i in pieces:
            w_piece(xn, i).start()
            w_piece(yn, i).start()

    def w_got(*pieces):
        for i in pieces:
            w_piece(xn, i).wait_recv()
            w_piece(yn, i).wait_recv()

    def wo_sib():
        src = wo_in.at[:, pl.ds(pl.multiple_of((1 - core) * half, half), half)]
        return send("wod", src, wo_land.at[1, 0], sib)

    def cols(ch):
        return pl.ds(pl.multiple_of(ch * cw, cw), cw)

    def own_cols(ch):
        return pl.ds(pl.multiple_of(core * half + ch * cw, cw), cw)

    def wo_piece(dev, i, ch):
        y = int(dev is yn)
        part = (0, 1, y)[i]
        src = (wo_in.at[:, own_cols(ch)], wo_land.at[1, 0, :, cols(ch)], wo_land.at[y, 2 - y, :, cols(ch)])[i]
        dst = wo_land.at[part, 3 if i == 2 else 1 + y, :, cols(ch)]
        return send("woy" if y else "wox", src, dst, dev, 2 * lax.rem(ch, RING) + i // 2)

    wo_x, wo_y = (functools.partial(wo_piece, dev) for dev in (xn, yn))

    def wo_own(ch):
        for i in BOTH:
            wo_x(i, ch).start()
            wo_y(i, ch).start()

    def wo_pass(ch, *more):
        got("wox", wo_land.at[:, 1, :, cols(ch)], 2 * lax.rem(ch, RING))
        got("woy", wo_land.at[:, 2, :, cols(ch)], 2 * lax.rem(ch, RING))
        wo_x(2, ch).start()
        wo_y(2, ch).start()
        for nxt in more:
            @pl.when(nxt < CHUNKS)
            def _():
                wo_own(nxt)

    def wo_arrive(ch):
        wo_x(2, ch).wait_recv()
        wo_y(2, ch).wait_recv()

    def load(g, slot, src, dst):
        return pltpu.make_async_copy(src, dst, ld.at[g, slot])

    def loads(g, ch, slot):
        w = wbuf.at[g, slot]
        rest = slice(1, QUADS)
        return (load(g, slot, wo_in.at[:, own_cols(ch)], w.at[0, 0]),
                load(g, slot, wo_land.at[0, rest, :, cols(ch)], w.at[0, rest]),
                load(g, slot, wo_land.at[1, :, :, cols(ch)], w.at[1]))

    lags = (e, 2, 4 - e)

    def loaded(g, ch, slot):
        load(g, slot, wo_land.at[:, :, :, cols(ch)], wbuf.at[g, slot]).wait()

    skip = (1 - e) * len(EARLY)

    def start_loads(g, ch, slot):
        for c in loads(g, ch, slot):
            c.start()

    def each_load(step, act):
        for g, (lag, lowest, past) in enumerate(zip(lags, (skip, 0, 0), (CHUNKS - 1, e * LASTS, CHUNKS))):
            ch = step - lag

            @pl.when((ch >= lowest) & (ch < past))
            def _():
                act(g, ch, odd(ch))

    def kof(k):
        return zof(k + e * (lax.rem(k + 1, 3) + 2 * (k // 3) - k))

    def o_x(k, cc):
        lo = obuf.shape[3] // 2
        zz = kof(k)
        group = (1, 0, 0, 2)[k]
        return send("ox", obuf.at[zz, cc, :, :lo], obuf.at[zz, 1 - cc, :, lo:], sib, group)

    def o_got(group):
        rows = slice(1 if group else 2)
        got("ox", obuf.at[rows, :, :, :obuf.shape[3] // 2], group)

    x_copy, gain_copy, wkv_copy, wq_copy, pos_copy = first = [
        pltpu.make_async_copy(src, dst, loc.at[i])
        for i, (src, dst) in enumerate(((x_in, hbuf.at[z, 0]), (gain_in, gain), (wkv_in, wbuf.at[:2]), (wq_in, wq.at[0]), (pos_in, pos)))]
    for c in first:
        c.start()
    barrier = pltpu.get_barrier_semaphore()
    peers = zpeers + [xn, yn, dg, sib]
    for dev in peers:
        pl.semaphore_signal(barrier, device_id=(dev,), device_id_type=MESH)
    pl.semaphore_wait(barrier, len(peers))
    w_start(0)
    x_copy.wait()
    gain_copy.wait()

    @pl.loop(0, 8)
    def _(i):
        rows = pl.ds(pl.multiple_of(i * 16, 16), 16)
        x = hbuf[z, 0, rows, :].astype(F32)
        cent = x - jnp.mean(x, axis=-1, keepdims=True)
        var = jnp.mean(cent * cent, axis=-1, keepdims=True)
        hbuf[z, 0, rows, :] = (cent * lax.rsqrt(var + NORM_EPS) * gain[:]).astype(BF16)

    wkv_copy.wait()
    kv[z, quad, core] = jnp.dot(hbuf[z, 0], wbuf[:2].reshape(width, PAIR), preferred_element_type=F32).astype(BF16)
    for i in THREE:
        kv_p(i).start()
    w_start(1, 2, 3)
    for i in BOTH:
        h_d(i).start()
    wo_sib().start()
    def own_rows(i):
        @pl.when(end)
        def _():
            h_own(i, hb_r).start()

        @pl.when(mid)
        def _():
            h_own_b(i).start()
            h_own(i, hf_r).start()

    own_rows(0)
    for i in THREE:
        kv_p(i).wait_recv()
    for i in THREE:
        kv_z(i).start()
    own_rows(1)

    pos_copy.wait()

    @pl.loop(0, posk.shape[0] // HD)
    def _(i):
        blk = pl.ds(pl.multiple_of(i * HD, HD), HD)
        posk[blk, :] = jnp.broadcast_to(pos[:, blk], (HD, HD)).T

    def rows_of(ref, zz):
        return ref[zz].reshape(PAIR, ref.shape[3])

    def keep_q():
        q = qacc[:].astype(BF16)
        qbuf[:PAIR] = q[:, :HD]
        qbuf[PAIR:] = q[:, HD:]

    def parts(part):
        split = (part + 1) // 2
        return [[(g + split * (i - g), i + split * (part - 1 - i)) for i in BOTH] for g in BOTH]

    def head_pair(p, part, g):
        return p + g * ((part + 1) // 2)

    def q_dot(unit, js, ws):
        zz, p, part = unit
        for g in BOTH:
            rows = [hbuf[zz, cc, pl.ds(pl.multiple_of(r * hh, hh), hh), js] for cc, r in parts(part)[g]]
            w = wq[head_pair(p, part, g), ws].reshape(-1, PAIR)
            yield g, jnp.dot(jnp.concatenate(rows, axis=0), w, preferred_element_type=F32)

    def whole_q(unit):
        for g, part in q_dot(unit, slice(None), slice(None)):
            qacc[g * HD:(g + 1) * HD] = part
        keep_q()

    def unit_of(codes, last):
        k, p, part = (lax.rem(c + v, QUADS) for c, v in zip(codes, last))
        return kof(k), p, part

    wq_copy.wait()
    h_block_wait(0)
    whole_q((z, 0, 0))
    for i in THREE:
        kv_z(i).wait_recv()
    kv_d().start()
    kv_d().wait_recv()
    for j in range(QUADS):
        v_t[:, j * KEYS:(j + 1) * KEYS] = kv[j].reshape(KEYS, PAIR)[:, HD:].T

    blocks = [(k, cc) for k in range(QUADS) for cc in BOTH]
    places = nb

    def place(i):
        return wq.at[i // places, lax.rem(i, places)]

    def y_send(i, ch, off, dev):
        return send("y", place(RECVS * CHUNKS + ch * SENDS + i), place(ch * RECVS + off), dev, RECVS * lax.rem(ch, Y_RING) + off)

    def y_recv(ch, off):
        blk = place(ch * RECVS + off)
        got("y", blk, RECVS * lax.rem(ch, Y_RING) + off)
        return blk[:].astype(F32)

    def y_sib(ch):
        return send("yd", hbuf.at[0, 1, :, cols(ch)], y_out.at[:, own_cols(ch)], sib)

    def weights(g, ch):
        return wbuf[g, odd(ch)].reshape(obuf.shape[3], cw)

    def go_on(j, ch, i, off, dev):
        place(RECVS * CHUNKS + ch * SENDS + i)[:] = acc[j].astype(BF16)
        y_send(i, ch, off, dev).start()

    o_parts = ((EARLY[0] - 1, blocks[2:6]), (FAR + 1, blocks[:2]), (FAR, blocks[6:]))

    def early_send(c, i):
        return send("pre", early.at[1, c, i], early.at[0, c, i], fwd, SENDS * c + i)

    def y_early(c):
        start_loads(c // 2, c, c % 2)
        loaded(c // 2, c, c % 2)
        for i in (1, 2):
            early_sum(c, i)

    def early_sum(c, i):
        early[1, c, i] = jnp.dot(rows_of(obuf, zof(3 - i)), weights(c // 2, c), preferred_element_type=F32).astype(BF16)
        early_send(c, i).start()

    def y_recv_early(n, ch, off):
        @pl.when(ch < len(EARLY))
        def _():
            blk = early.at[0, ch, off]
            got("pre", blk, SENDS * ch + off)
            acc[n] += blk[:].astype(F32)

        @pl.when(ch >= len(EARLY))
        def _():
            acc[n] += y_recv(ch, off)

    def pairs_0():
        w_got(*BOTH)
        f_half(0)
        b_half(0)

    def rows_1():
        f_half(1)
        b_half(1)
        h_block_wait(1)
        w_got(2)
        w_start(*HANDED_ON)
        wo_sib().wait_recv()
        wo_own(0)
        wo_own(1)

    def pairs_1():
        w_got(3)
        f_half(2)

    def rows_2():
        f_half(3)
        pl.when(end)(lambda: h_block_wait(2))
        pl.when(mid)(lambda: h_block_wait(4))

    def rows_3():
        pl.when(end)(lambda: f_half(4))
        half_block_wait(0)

    late = dict(zip(LATE, (pairs_0, rows_1, pairs_1, rows_2, rows_3, lambda: w_got(*HANDED_ON), lambda: half_block_wait(1))))

    def before(i):
        if i == EARLY[0] - 1:
            yield lambda: wo_pass(0)
        if i == EARLY[0]:
            yield lambda: wo_pass(1, 2)
        if i == FAR + 1:
            yield lambda: wo_pass(4, 6)

    def after(i):
        for at, some in o_parts:
            if at == i:
                for b in some:
                    yield lambda b=b: o_x(*b).start()
        for c, at in enumerate(EARLY):
            if at == i:
                if c == 0:
                    yield lambda: o_got(0)
                if c == 1:
                    yield lambda: pl.when(end)(lambda: f_half(5))
                yield lambda c=c: wo_arrive(c)
                yield lambda c=c: pl.when(end)(lambda: y_early(c))
        if i == EARLY[1]:
            yield lambda: wo_pass(2, 3, 4)
        if i == FAR:
            yield lambda: wo_pass(3, 5)
            yield lambda: o_got(2)
            for c in THREE:
                yield lambda c=c: pl.when(end)(lambda: early_sum(c, 0))
        if i + 1 in late:
            yield late[i + 1]

    def by_tile(s, due, lo=0, hi=len(TILES)):
        if not any(True for i in range(lo, hi) for _ in due(i)):
            return
        if hi - lo == 1:
            for act in due(lo):
                act()
            return
        half_way = (lo + hi) // 2
        pl.when(s < half_way)(lambda: by_tile(s, due, lo, half_way))
        pl.when(s >= half_way)(lambda: by_tile(s, due, half_way, hi))

    scale = HD ** -0.5 * LOG2E
    n = 2 * PAIR
    kq = width // QUADS

    def tile(s, carry):
        codes, ahead = carry[:3], carry[3:]
        zz, p, part = unit_of(codes, LAST)
        following = unit_of(ahead, TILES[0])
        carry = tuple(c // QUADS for c in carry)

        by_tile(s, before)
        q = qbuf[:]
        tok = (zz * QUADS + quad) * 2
        pq = [pos[:, pl.ds(pl.multiple_of((tok + c) * HD, HD), HD)] for c in (core, 1 - core)]
        pq = [[v[:, :hh], v[:, hh:]] for v in pq]
        split, second = (part + 1) // 2, part // 2
        of_core = [v[0] + second * (v[1] - v[0]) for v in pq]
        pq = [pq[g][i] + split * (of_core[i] - pq[g][i]) for g in BOTH for i in BOTH]
        pq = jnp.broadcast_to(jnp.concatenate(pq + pq, axis=1), (8, n))

        def scores(j):
            keys = kv[j].reshape(KEYS, PAIR)[:, :HD]
            sc = lax.dot_general(keys, q, (((1,), (1,)), ((), ())), preferred_element_type=F32)
            pk = posk[j * KEYS:(j + 1) * KEYS, :]
            pk = jnp.concatenate([pk] * (n // HD), axis=1).reshape(KEYS // 8, 8, n)
            sc = jnp.where(pk <= pq, sc.reshape(KEYS // 8, 8, n), MASKED)
            bufs[j % 2][0][:] = sc.reshape(KEYS, n)
            return jnp.max(jnp.max(sc, axis=0), axis=0, keepdims=True)

        def weigh(j, m):
            pr = jnp.exp2((bufs[j % 2][0][:].reshape(KEYS // 8, 8, n) - jnp.broadcast_to(m, (8, n))) * scale)
            bufs[j % 2][1][:] = pr.reshape(KEYS, n).astype(BF16)
            return jnp.sum(pr, axis=0)

        def add_values(j, alpha):
            got = jnp.dot(v_t[:, j * KEYS:(j + 1) * KEYS], bufs[j % 2][1][:], preferred_element_type=F32)
            out_t[:] = got if alpha is None else out_t[:] * alpha + got

        m = scores(0)
        alpha = den = None
        for j in range(QUADS):
            if j + 1 < QUADS:
                mn = jnp.maximum(m, scores(j + 1))
            for g, got in q_dot(following, slice(j * kq, (j + 1) * kq), slice(j * nb // QUADS, (j + 1) * nb // QUADS)):
                rows = slice(g * HD, (g + 1) * HD)
                qacc[rows] = got if j == 0 else qacc[rows] + got
            ps = weigh(j, m)
            if j > 0:
                add_values(j - 1, alpha if j > 1 else None)
            den = ps if j == 0 else den * now + ps
            if j > 0:
                alpha = now
            if j < QUADS - 1:
                now = jnp.exp2((m - mn) * scale)
                m = mn
        add_values(QUADS - 1, alpha)
        out = (out_t[:] / jnp.sum(den, axis=0, keepdims=True)).T.astype(BF16)
        for g in BOTH:
            hp = head_pair(p, part, g)
            for j, c in enumerate((2 * hp - hp // 2 + hp // 3, 2 * hp + 1 + (hp + 1) // 2 - hp // 2 - hp // 3)):
                for i, (cc, r) in enumerate(parts(part)[g]):
                    row = (2 * j + g) * HD + i * hh
                    obuf[zz, cc, pl.ds(pl.multiple_of(r * hh, hh), hh), pl.ds(pl.multiple_of(c * HD, HD), HD)] = out[row:row + hh]
        keep_q()

        by_tile(s, after)
        is_late = s == LATE[0] - 1
        for i in LATE[1:]:
            is_late = is_late | (s == i - 1)

        @pl.when(is_late)
        def _():
            whole_q(unit_of(carry[:3], LAST))

        return carry

    lax.fori_loop(0, len(TILES), tile, tuple(jnp.int32(t) for t in TABLES))

    for i in BOTH:
        @pl.when(end)
        def _():
            h_own(i, hb_r).wait_send()

        @pl.when(mid)
        def _():
            h_own_b(i).wait_send()
            h_own(i, hf_r).wait_send()
            h_b2f(i).wait_send()
            h_f2b(i).wait_send()
            h_f2b(2 + i).wait_send()
    sent("hd", hbuf.at[:, 0])
    w_bytes = wq.at[:3, :hb]
    sent("wx", w_bytes)
    sent("wy", w_bytes)

    pl.semaphore_signal(ready.at[1 - e], device_id=(fwd,), device_id_type=MESH)

    @pl.when(mid)
    def _():
        pl.semaphore_signal(ready.at[0], device_id=(bwd,), device_id_type=MESH)
        pl.semaphore_wait(ready.at[1])
    pl.semaphore_wait(ready.at[0])

    def y_step(t, _):
        each_load(t, loaded)
        ch_a, ch_b, ch_c = (t - lag for lag in lags)

        @pl.when(ch_a == LASTS)
        def _():
            loaded(0, CHUNKS - 1, 1)

        def farther(count, off):
            last = ch_a // LASTS
            for j in range(count):
                u = (ch_a - LASTS) * count + j
                i = j + last * (u // 2 - j)
                ch = ch_a + last * (LASTS + odd(u + 6 * CHUNKS) - ch_a)
                acc[j] = jnp.dot(rows_of(obuf, zof(3 - i)), weights(0, ch), preferred_element_type=F32)
                if off:
                    y_recv_early(j, ch, i)
                go_on(j, ch, i, i + off, fwd)

        def nearest(g, ch):
            acc[2] = jnp.dot(rows_of(obuf, zof(0)), weights(g, ch), preferred_element_type=F32)
            acc[2] += y_recv(ch, 3)
            go_on(2, ch, 2, 3, bwd)

        @pl.when(mid & (t == CHUNKS))
        def _():
            for ch in range(LASTS, CHUNKS):
                nearest(0, ch)

        in_range = (ch_a >= skip) & (ch_a < CHUNKS)

        @pl.when(end & in_range)
        def _():
            farther(3, 0)

        @pl.when(mid & in_range)
        def _():
            farther(2, 3)

        @pl.when(mid & (ch_b >= 0) & (ch_b < LASTS))
        def _():
            nearest(1, ch_b)

        passing = t + AHEAD

        @pl.when((passing > 4) & (passing < CHUNKS))
        def _():
            wo_pass(passing, passing + AHEAD)

        nxt = t + 1

        @pl.when((nxt >= len(EARLY)) & (nxt < CHUNKS - 1 + e))
        def _():
            wo_arrive(nxt)

        @pl.when(end & (t == CHUNKS - 3))
        def _():
            wo_arrive(CHUNKS - 1)

        @pl.when(ch_a == CHUNKS - 3)
        def _():
            start_loads(0, CHUNKS - 1, 1)
        each_load(nxt, start_loads)

        @pl.when(ch_c == 0)
        def _():
            o_got(1)

        @pl.when((ch_c >= 0) & (ch_c < CHUNKS))
        def _():
            acc[3] = jnp.dot(rows_of(obuf, z), weights(2, ch_c), preferred_element_type=F32)

            @pl.when(end)
            def _():
                acc[3] += y_recv(ch_c, 3)

            @pl.when(mid)
            def _():
                y_recv_early(3, ch_c, 2)
                acc[3] += y_recv(ch_c, 4)
            y_out[:, own_cols(ch_c)] = acc[3, :HD].astype(BF16)
            hbuf[0, 1, :, cols(ch_c)] = acc[3, HD:].astype(BF16)
            y_sib(ch_c).start()
        return 0

    lax.fori_loop(0, CHUNKS + 4, y_step, 0)

    sent("wox", w_bytes)
    sent("woy", w_bytes)
    whole = slice(half)
    sent("yd", hbuf.at[0, 1, :, whole])
    got("yd", hbuf.at[0, 1, :, whole])
    sent("ox", obuf.at[:, :, :, :obuf.shape[3] // 2])

    @pl.when(end)
    def _():
        sent("y", wq.at[:SENDS, :CHUNKS - len(EARLY)])
        sent("pre", early.at[1])

    @pl.when(mid)
    def _():
        sent("y", wq.at[:SENDS, :CHUNKS])
    for i in THREE:
        kv_z(i).wait_send()
        kv_p(i).wait_send()
    kv_d().wait_send()
    wo_sib().wait_send()


def finish(y, kv, y_out, k_out, v_out, sems):
    copies = [pltpu.make_async_copy(src, dst, sems.at[i]) for i, (src, dst) in enumerate((
        (y, y_out), (kv.at[:, :, :, :, :HD], k_out), (kv.at[:, :, :, :, HD:], v_out)))]
    for c in copies:
        c.start()
    for c in copies:
        c.wait()


def solution(mesh):
    def local_step(x_loc, ln_gain, wq_loc, w_kv, wo_loc, positions):
        rows, width = x_loc.shape
        tokens = positions.shape[0]
        dma, vmem = pltpu.SemaphoreType.DMA, pltpu.VMEM
        hbm = pl.BlockSpec(memory_space=pl.ANY)
        half = width // 2
        cw = half // CHUNKS
        nb, n = width // PAIR, 2 * PAIR
        kv_shape = (QUADS, QUADS, 2, rows, HD)
        wkv_shape = (2, 2, 2, QUADS, PAIR, cw)
        vm = pl.BlockSpec(memory_space=pltpu.VMEM)
        kv_all = (QUADS, QUADS, 2, rows, PAIR)
        y, kv, _ = pl.pallas_call(
            kernel,
            name="mqa_layer",
            out_shape=(vmem((rows, width), BF16), vmem(kv_all, BF16), jax.ShapeDtypeStruct((2, QUADS, PAIR, half), BF16)),
            in_specs=[hbm] * 6,
            out_specs=(vm, vm, hbm),
            scratch_shapes=[
                vmem((QUADS, 2, rows, width), BF16),
                vmem((1, width), F32), vmem((1, tokens), I32),
                vmem((QUADS, nb, PAIR, PAIR), BF16),
                vmem((HD, tokens), BF16),
                vmem((tokens, HD), I32),
                vmem((QUADS, 2, rows, 2 * KEYS), BF16),
                vmem((3,) + wkv_shape[1:], BF16),
                vmem((QUADS, PAIR, cw), F32),
                vmem((2, len(EARLY), SENDS, PAIR, cw), BF16),
                vmem((KEYS, n), F32), vmem((KEYS, n), F32),
                vmem((KEYS, n), BF16), vmem((KEYS, n), BF16),
                vmem((HD, n), F32),
                vmem((PAIR, PAIR), F32),
                vmem((n, HD), BF16),
                dma((5,)), dma((sum(SND.values()),)), dma((sum(RCV.values()),)), dma((6,)), dma((2,)), dma((3, 2)),
                pltpu.SemaphoreType.REGULAR((2,)),
            ],
            compiler_params=pltpu.CompilerParams(
                collective_id=0, has_side_effects=True, vmem_limit_bytes=58 << 20),
        )(x_loc, ln_gain.reshape(1, width), wq_loc.reshape(nb, PAIR, PAIR), w_kv.reshape(wkv_shape), wo_loc, positions.reshape(1, tokens))
        y, k, v = pl.pallas_call(
            finish,
            name="outputs",
            out_shape=tuple(jax.ShapeDtypeStruct(s, BF16) for s in ((rows, width), kv_shape, kv_shape)),
            in_specs=[vm] * 2,
            out_specs=(hbm,) * 3,
            scratch_shapes=[dma((3,))],
            compiler_params=pltpu.CompilerParams(vmem_limit_bytes=1 << 20),
        )(pltpu.with_memory_space_constraint(y, pltpu.VMEM), pltpu.with_memory_space_constraint(kv, pltpu.VMEM))
        return y, k.reshape(tokens, HD), v.reshape(tokens, HD)

    split, whole = P("model", None), P(None, None)
    return jax.shard_map(
        local_step,
        mesh=mesh,
        in_specs=(split, P(), P(None, "model"), whole, split, P()),
        out_specs=(split, whole, whole),
        check_vma=False,
    )
```

```python
import functools

import jax
import jax.numpy as jnp
from jax import lax
from jax.experimental import pallas as pl
from jax.experimental.pallas import tpu as pltpu
from jax.sharding import PartitionSpec as P

NORM_EPS = 1e-6
LOG2E = 1.4426950408889634
MESH = pl.DeviceIdType.MESH
BF16, F32, I32 = jnp.bfloat16, jnp.float32, jnp.int32
SUB, ROWS = 8, 16
HD = 128
PAIR = 2 * HD
KEYS = SUB * HD
QUADS = 4
CHUNKS = 16
LASTS = CHUNKS - 2
AHEAD = 2
MASKED = -1e30
BOTH, THREE = range(2), range(3)
NEARER = (1, 2)
HANDED_ON = (4, 5)

TILES = ((0, 0, 0), (0, 1, 0), (1, 0, 0), (1, 1, 0), (0, 2, 0), (1, 2, 0), (2, 0, 0), (2, 1, 0), (2, 2, 0), (3, 0, 1),
         (1, 3, 0), (2, 3, 0), (3, 2, 1), (3, 0, 2), (3, 2, 2), (0, 3, 0))
LATE = (1, 2, 4, 6, 9, 10, 13)
FAR = 14
EARLY = (FAR - 2, FAR - 2, FAR - 1)
LAST = TILES[-1]
NEXT = [TILES[0] if i in LATE else t for i, t in enumerate(TILES)][1:]


def digits(values):
    return sum((v % 4) << (2 * i) for i, v in enumerate(values))


SPARE = (0, 3, 0)
TABLES = [digits(t[c] - LAST[c] for t in TILES) for c in THREE] + [digits(t[c] - SPARE[c] for t in NEXT) for c in THREE]

SENDS, RECVS = 3, 5
RING, Y_RING = 4, 8

KINDS = ("kvz", "kvp", "kvd", "h", "hd", "wx", "wy", "pre", "wod", "wox", "woy", "ox", "y", "yd")
SND = dict.fromkeys(KINDS, 1) | dict(kvz=3, kvp=3, h=10)
RCV = dict.fromkeys(KINDS, 1) | dict(kvz=3, kvp=3, hd=10, wx=6, wy=6, pre=9, wox=2 * RING, woy=2 * RING, ox=3, y=RECVS * Y_RING)


def odd(v):
    return lax.rem(v, 2)


def offsets(counts):
    out = {}
    for name in counts:
        out[name] = sum(counts[k] for k in out)
    return out


SND_AT, RCV_AT = offsets(SND), offsets(RCV)


def kernel(x_in, gain_in, wq_in, wkv_in, wo_in, pos_in, y_out, kv, wo_land,
           hbuf, gain, pos, wq, v_t, posk, obuf, wbuf, acc, early, sc0, sc1, pr0, pr1, out_t, qacc, qbuf,
           loc, snd, rcv, hf_r, hb_r, ld, ready):
    me = lax.axis_index("model")
    core = odd(me)
    quad = lax.rem(me // 2, QUADS)
    z = me // 8
    width = hbuf.shape[3]
    half = width // 2
    cw = half // CHUNKS
    upper = z // 2
    away = 1 - 2 * upper

    def zof(d):
        return d + upper * (3 - 2 * d)

    e = zof(z)
    end, mid = e == 0, e == 1
    base = me - 8 * z
    dx = 2 - 4 * odd(quad)
    dy = 4 - 8 * (quad // 2)
    sib, xn, yn, dg = me + 1 - 2 * core, me + dx, me + dy, me + dx + dy
    fwd = base + 8 * (z + away)
    bwd = base + 8 * (z - away * e)
    zpeers = [base + 8 * lax.rem(z + i, QUADS) for i in (1, 2, 3)]
    bufs = ((sc0, pr0), (sc1, pr1))

    def put(src, dst, ssem, rsem, dev):
        return pltpu.make_async_remote_copy(src, dst, ssem, rsem, device_id=(dev,), device_id_type=MESH)

    def send(kind, src, dst, dev, i=0):
        return put(src, dst, snd.at[SND_AT[kind] + (i if SND[kind] > 1 else 0)], rcv.at[RCV_AT[kind] + i], dev)

    def sent(kind, like):
        send(kind, like, like, sib).wait_send()

    def got(kind, like, i=0):
        send(kind, like, like, sib, i).wait_recv()

    def kv_z(i):
        blk = kv.at[z, :, core]
        return send("kvz", blk, blk, zpeers[i], i)

    def kv_p(i):
        blk = kv.at[z, quad, core]
        return send("kvp", blk, blk, (xn, yn, dg)[i], i)

    def kv_d():
        blk = kv.at[:, :, core]
        return send("kvd", blk, blk, sib)

    hh = HD // 2

    def hrows(zz, cc, i):
        return hbuf.at[zz, cc, pl.ds(hh * i, hh), :]

    def h_put(n, zz, i, rsem, dev):
        return put(hrows(zz, 0, i), hrows(zz, 0, i), snd.at[SND_AT["h"] + n], rsem, dev)

    def h_own(i, rsems):
        return h_put(i, z, i, rsems.at[i], fwd)

    def h_own_b(i):
        return h_put(2 + i, z, i, hf_r.at[i], bwd)

    def h_f2b(i):
        return h_put(4 + i, zof(e + 1 + i // 2), i % 2, hf_r.at[2 + i], bwd)

    def h_b2f(i):
        return h_put(8 + i, zof(e - 1), i, hf_r.at[2 + i], fwd)

    def h_d(i):
        zz = z if i < 2 else (zof(e + i // 2) if i < 8 else zof(e - 1))
        return send("hd", hrows(zz, 0, i % 2), hrows(zz, 1, i % 2), sib, i)

    def f_half(i):
        zz = zof(e + 1 + i // 2)
        h_put(0, zz, i % 2, hf_r.at[i], fwd).wait_recv()
        h_d(2 + i).start()
        if i < 4:
            @pl.when(mid)
            def _():
                h_f2b(i).start()

    def b_half(i):
        @pl.when(mid)
        def _():
            h_put(0, zof(e - 1), i, hb_r.at[i], bwd).wait_recv()
            h_d(8 + i).start()
            h_b2f(i).start()

    def h_block_wait(b):
        for i in BOTH:
            h_d(2 * b + i).wait_recv()

    def half_block_wait(c):
        pl.when(end)(lambda: h_d(6 + c).wait_recv())
        pl.when(mid)(lambda: h_d(4 + c).wait_recv())

    nb = wq.shape[1]
    hb = nb // 2

    def w_piece(dev, i):
        y = int(dev is yn)
        lower, upper = slice(hb), slice(hb, nb)
        halves = (lower, upper) if y else (upper, lower)
        if i < 4:
            rows = (slice(4), slice(4, nb), *halves)[i]
            h = i // 2
            src = wq_in.at[rows, :, pl.ds(HD * h, HD)]
            dst = wq.at[1 + h, rows, :, pl.ds(HD * y, HD)]
        else:
            h = i - 4
            rows = halves[1]
            src = wq.at[1 + h, rows, :, pl.ds(HD - HD * y, HD)]
            dst = wq.at[3, rows, :, pl.ds(HD * h, HD)]
        return send("wy" if y else "wx", src, dst, dev, i)

    def w_start(*pieces):
        for i in pieces:
            w_piece(xn, i).start()
            w_piece(yn, i).start()

    def w_got(*pieces):
        for i in pieces:
            w_piece(xn, i).wait_recv()
            w_piece(yn, i).wait_recv()

    def wo_sib():
        src = wo_in.at[:, pl.ds(pl.multiple_of((1 - core) * half, half), half)]
        return send("wod", src, wo_land.at[1, 0], sib)

    def cols(ch):
        return pl.ds(pl.multiple_of(ch * cw, cw), cw)

    def own_cols(ch):
        return pl.ds(pl.multiple_of(core * half + ch * cw, cw), cw)

    def wo_piece(dev, i, ch, near=False):
        y = int(dev is yn)
        part = (0, 1, y)[i]
        src = (wo_in.at[:, own_cols(ch)], wo_land.at[1, 0, :, cols(ch)], wo_land.at[y, 2 - y, :, cols(ch)])[i]
        dst = wbuf.at[(*divmod(ch, 2), part, 3)] if near else wo_land.at[part, 3 if i == 2 else 1 + y, :, cols(ch)]
        return send("woy" if y else "wox", src, dst, dev, 2 * lax.rem(ch, RING) + i // 2)

    wo_x, wo_y = (functools.partial(wo_piece, dev) for dev in (xn, yn))

    def wo_own(ch):
        for i in BOTH:
            wo_x(i, ch).start()
            wo_y(i, ch).start()

    def wo_pass(ch, *more):
        got("wox", wo_land.at[:, 1, :, cols(ch)], 2 * lax.rem(ch, RING))
        got("woy", wo_land.at[:, 2, :, cols(ch)], 2 * lax.rem(ch, RING))

        def hand_on(near):
            wo_x(2, ch, near).start()
            wo_y(2, ch, near).start()

        if isinstance(ch, int) and ch < len(EARLY):
            pl.when(mid)(lambda: hand_on(False))

            @pl.when(end)
            def _():
                hand_on(True)
                for c in near_loads(ch):
                    c.start()
        else:
            hand_on(False)
        for nxt in more:
            @pl.when(nxt < CHUNKS)
            def _():
                wo_own(nxt)

    def wo_arrive(ch):
        wo_x(2, ch).wait_recv()
        wo_y(2, ch).wait_recv()

    def load(g, slot, src, dst):
        return pltpu.make_async_copy(src, dst, ld.at[g, slot])

    def loads(g, ch, slot):
        w = wbuf.at[g, slot]
        rest = slice(1, QUADS)
        return (load(g, slot, wo_in.at[:, own_cols(ch)], w.at[0, 0]),
                load(g, slot, wo_land.at[0, rest, :, cols(ch)], w.at[0, rest]),
                load(g, slot, wo_land.at[1, :, :, cols(ch)], w.at[1]))

    def near_loads(c):
        g, slot = divmod(c, 2)
        w, most = wbuf.at[g, slot], slice(1, 3)
        return (load(g, slot, wo_in.at[:, own_cols(c)], w.at[0, 0]),
                load(g, slot, wo_land.at[0, most, :, cols(c)], w.at[0, most]),
                load(g, slot, wo_land.at[1, :3, :, cols(c)], w.at[1, :3]))

    def near_loaded(c):
        g, slot = divmod(c, 2)
        load(g, slot, wo_land.at[:, :3, :, cols(c)], wbuf.at[g, slot, :, :3]).wait()

    def kept(c):
        return pltpu.make_async_copy(wbuf.at[(*divmod(c, 2), slice(None), 3)], wo_land.at[:, 3, :, cols(c)], loc.at[c])

    lags = (e, 2, 4 - e)

    def loaded(g, ch, slot):
        load(g, slot, wo_land.at[:, :, :, cols(ch)], wbuf.at[g, slot]).wait()

    skip = (1 - e) * len(EARLY)

    def start_loads(g, ch, slot):
        for c in loads(g, ch, slot):
            c.start()

    def each_load(step, act):
        for g, (lag, lowest, past) in enumerate(zip(lags, (skip, 0, 0), (CHUNKS, e * LASTS, CHUNKS))):
            ch = step - lag

            @pl.when((ch >= lowest) & (ch < past))
            def _():
                act(g, ch, odd(ch))

    def kof(k):
        return zof(k + e * (lax.rem(k + 1, 3) + 2 * (k // 3) - k))

    def o_x(k, cc):
        lo = obuf.shape[3] // 2
        zz = kof(k)
        group = (1, 0, 0, 2)[k]
        return send("ox", obuf.at[zz, cc, :, :lo], obuf.at[zz, 1 - cc, :, lo:], sib, group)

    def o_got(group):
        rows = slice(1 if group else 2)
        got("ox", obuf.at[rows, :, :, :obuf.shape[3] // 2], group)

    x_copy, gain_copy, wkv_copy, wq_copy, pos_copy = first = [
        pltpu.make_async_copy(src, dst, loc.at[i])
        for i, (src, dst) in enumerate(((x_in, hbuf.at[z, 0]), (gain_in, gain), (wkv_in, wbuf.at[:2]), (wq_in, wq.at[0]), (pos_in, pos)))]
    for c in first:
        c.start()
    barrier = pltpu.get_barrier_semaphore()
    peers = zpeers + [xn, yn, dg, sib]
    for dev in peers:
        pl.semaphore_signal(barrier, device_id=(dev,), device_id_type=MESH)
    pl.semaphore_wait(barrier, len(peers))
    w_start(0)
    x_copy.wait()
    gain_copy.wait()

    @pl.loop(0, SUB)
    def _(i):
        rows = pl.ds(pl.multiple_of(i * ROWS, ROWS), ROWS)
        x = hbuf[z, 0, rows, :].astype(F32)
        cent = x - jnp.mean(x, axis=-1, keepdims=True)
        var = jnp.mean(cent * cent, axis=-1, keepdims=True)
        hbuf[z, 0, rows, :] = (cent * lax.rsqrt(var + NORM_EPS) * gain[:]).astype(BF16)

    wkv_copy.wait()
    kv[z, quad, core] = jnp.dot(hbuf[z, 0], wbuf[:2].reshape(width, PAIR), preferred_element_type=F32).astype(BF16)
    for i in THREE:
        kv_p(i).start()
    w_start(1, 2, 3)
    for i in BOTH:
        h_d(i).start()
    wo_sib().start()
    def own_rows(i):
        @pl.when(end)
        def _():
            h_own(i, hb_r).start()

        @pl.when(mid)
        def _():
            h_own_b(i).start()
            h_own(i, hf_r).start()

    own_rows(0)
    for i in THREE:
        kv_p(i).wait_recv()
    for i in THREE:
        kv_z(i).start()
    own_rows(1)

    pos_copy.wait()

    @pl.loop(0, posk.shape[0] // HD)
    def _(i):
        blk = pl.ds(pl.multiple_of(i * HD, HD), HD)
        posk[blk, :] = jnp.broadcast_to(pos[:, blk], (HD, HD)).T

    def rows_of(ref, zz):
        return ref[zz].reshape(PAIR, ref.shape[3])

    def keep_q():
        q = qacc[:].astype(BF16)
        qbuf[:PAIR] = q[:, :HD]
        qbuf[PAIR:] = q[:, HD:]

    def parts(part):
        split = (part + 1) // 2
        return [[(g + split * (i - g), i + split * (part - 1 - i)) for i in BOTH] for g in BOTH]

    def head_pair(p, part, g):
        return p + g * ((part + 1) // 2)

    def q_dot(unit, js, ws):
        zz, p, part = unit
        for g in BOTH:
            rows = [hbuf[zz, cc, pl.ds(pl.multiple_of(r * hh, hh), hh), js] for cc, r in parts(part)[g]]
            w = wq[head_pair(p, part, g), ws].reshape(-1, PAIR)
            yield g, jnp.dot(jnp.concatenate(rows, axis=0), w, preferred_element_type=F32)

    def whole_q(unit):
        for g, part in q_dot(unit, slice(None), slice(None)):
            qacc[g * HD:(g + 1) * HD] = part
        keep_q()

    def unit_of(codes, last):
        k, p, part = (lax.rem(c + v, QUADS) for c, v in zip(codes, last))
        return kof(k), p, part

    wq_copy.wait()
    h_block_wait(0)
    whole_q((z, 0, 0))
    for i in THREE:
        kv_z(i).wait_recv()
    kv_d().start()
    kv_d().wait_recv()
    for j in range(QUADS):
        v_t[:, j * KEYS:(j + 1) * KEYS] = kv[j].reshape(KEYS, PAIR)[:, HD:].T

    blocks = [(k, cc) for k in range(QUADS) for cc in BOTH]
    places = nb

    def place(i):
        return wq.at[i // places, lax.rem(i, places)]

    def y_send(i, ch, off, dev):
        return send("y", place(RECVS * CHUNKS + ch * SENDS + i), place(ch * RECVS + off), dev, RECVS * lax.rem(ch, Y_RING) + off)

    def y_recv(ch, off):
        blk = place(ch * RECVS + off)
        got("y", blk, RECVS * lax.rem(ch, Y_RING) + off)
        return blk[:].astype(F32)

    def y_sib(ch):
        return send("yd", hbuf.at[0, 1, :, cols(ch)], y_out.at[:, own_cols(ch)], sib)

    def weights(g, ch):
        return wbuf[g, odd(ch)].reshape(obuf.shape[3], cw)

    def go_on(j, ch, i, off, dev):
        place(RECVS * CHUNKS + ch * SENDS + i)[:] = acc[j].astype(BF16)
        y_send(i, ch, off, dev).start()

    o_parts = ((EARLY[0] - 1, blocks[2:6]), (FAR + 1, blocks[:2]), (FAR, blocks[6:]))

    def early_send(c, i):
        return send("pre", early.at[1, c, i], early.at[0, c, i], fwd, SENDS * c + i)

    def y_early(c):
        near_loaded(c)
        kept(c).start()
        for i in NEARER:
            early_sum(c, i)

    def early_sum(c, i):
        early[1, c, i] = jnp.dot(rows_of(obuf, zof(3 - i)), weights(c // 2, c), preferred_element_type=F32).astype(BF16)
        early_send(c, i).start()

    def y_recv_early(n, ch, off):
        @pl.when(ch < len(EARLY))
        def _():
            blk = early.at[0, ch, off]
            got("pre", blk, SENDS * ch + off)
            acc[n] += blk[:].astype(F32)

        @pl.when(ch >= len(EARLY))
        def _():
            acc[n] += y_recv(ch, off)

    def pairs_0():
        w_got(*BOTH)
        f_half(0)
        b_half(0)

    def rows_1():
        f_half(1)
        b_half(1)
        h_block_wait(1)
        w_got(2)
        w_start(*HANDED_ON)
        wo_sib().wait_recv()
        wo_own(0)
        wo_own(1)

    def pairs_1():
        w_got(3)
        f_half(2)

    def rows_2():
        f_half(3)
        pl.when(end)(lambda: h_block_wait(2))
        pl.when(mid)(lambda: h_block_wait(4))

    def rows_3():
        pl.when(end)(lambda: f_half(4))
        half_block_wait(0)

    late = dict(zip(LATE, (pairs_0, rows_1, pairs_1, rows_2, rows_3, lambda: w_got(*HANDED_ON), lambda: half_block_wait(1))))

    w_bytes = wq.at[:3, :hb]

    def tell(sem, dev):
        pl.semaphore_signal(sem, device_id=(dev,), device_id_type=MESH)

    def get_ready():
        sent("wx", w_bytes)
        sent("wy", w_bytes)
        tell(ready.at[1 - e], fwd)
        pl.when(mid)(lambda: tell(ready.at[0], bwd))

    def before(i):
        if i == EARLY[0] - 1:
            yield lambda: wo_pass(0)
        if i == EARLY[0]:
            yield lambda: wo_pass(1, 2)
        if i == FAR + 1:
            yield lambda: wo_pass(4, 6)

    def after(i):
        for at, some in o_parts:
            if at == i:
                for b in some:
                    yield lambda b=b: o_x(*b).start()
        for c, at in enumerate(EARLY):
            if at == i:
                if c == 0:
                    yield lambda: o_got(0)
                if c == 1:
                    yield lambda: pl.when(end)(lambda: f_half(5))
                yield lambda c=c: wo_arrive(c)
                yield lambda c=c: pl.when(end)(lambda: y_early(c))
        if i == EARLY[1]:
            yield lambda: wo_pass(2, 3, 4)
        if i == FAR:
            yield get_ready
            yield lambda: wo_pass(3, 5)
            yield lambda: o_got(2)
            for c in THREE:
                yield lambda c=c: pl.when(end)(lambda: early_sum(c, 0))
        if i + 1 in late:
            yield late[i + 1]

    def by_tile(s, due, lo=0, hi=len(TILES)):
        if not any(True for i in range(lo, hi) for _ in due(i)):
            return
        if hi - lo == 1:
            for act in due(lo):
                act()
            return
        half_way = (lo + hi) // 2
        pl.when(s < half_way)(lambda: by_tile(s, due, lo, half_way))
        pl.when(s >= half_way)(lambda: by_tile(s, due, half_way, hi))

    scale = HD ** -0.5 * LOG2E
    n = 2 * PAIR
    kq = width // QUADS

    def tile(s, carry):
        codes, ahead = carry[:3], carry[3:]
        zz, p, part = unit_of(codes, LAST)
        following = unit_of(ahead, SPARE)
        carry = tuple(c // QUADS for c in carry)

        by_tile(s, before)
        q = qbuf[:]
        tok = (zz * QUADS + quad) * 2
        pq = [pos[:, pl.ds(pl.multiple_of((tok + c) * HD, HD), HD)] for c in (core, 1 - core)]
        pq = [[v[:, :hh], v[:, hh:]] for v in pq]
        split, second = (part + 1) // 2, part // 2
        of_core = [v[0] + second * (v[1] - v[0]) for v in pq]
        pq = [pq[g][i] + split * (of_core[i] - pq[g][i]) for g in BOTH for i in BOTH]
        pq = jnp.broadcast_to(jnp.concatenate(pq + pq, axis=1), (SUB, n))

        def scores(j):
            keys = kv[j].reshape(KEYS, PAIR)[:, :HD]
            sc = lax.dot_general(keys, q, (((1,), (1,)), ((), ())), preferred_element_type=F32)
            pk = posk[j * KEYS:(j + 1) * KEYS, :]
            pk = jnp.concatenate([pk] * (n // HD), axis=1).reshape(KEYS // SUB, SUB, n)
            sc = jnp.where(pk <= pq, sc.reshape(KEYS // SUB, SUB, n), MASKED)
            bufs[j % 2][0][:] = sc.reshape(KEYS, n)
            return jnp.max(jnp.max(sc, axis=0), axis=0, keepdims=True)

        def weigh(j, m):
            pr = jnp.exp2((bufs[j % 2][0][:].reshape(KEYS // SUB, SUB, n) - jnp.broadcast_to(m, (SUB, n))) * scale)
            bufs[j % 2][1][:] = pr.reshape(KEYS, n).astype(BF16)
            return jnp.sum(pr, axis=0)

        def add_values(j, alpha):
            got = jnp.dot(v_t[:, j * KEYS:(j + 1) * KEYS], bufs[j % 2][1][:], preferred_element_type=F32)
            out_t[:] = got if alpha is None else out_t[:] * alpha + got

        m = scores(0)
        alpha = den = None
        for j in range(QUADS):
            if j + 1 < QUADS:
                mn = jnp.maximum(m, scores(j + 1))
            for g, got in q_dot(following, slice(j * kq, (j + 1) * kq), slice(j * nb // QUADS, (j + 1) * nb // QUADS)):
                rows = slice(g * HD, (g + 1) * HD)
                qacc[rows] = got if j == 0 else qacc[rows] + got
            ps = weigh(j, m)
            if j > 0:
                add_values(j - 1, alpha if j > 1 else None)
            den = ps if j == 0 else den * now + ps
            if j > 0:
                alpha = now
            if j < QUADS - 1:
                now = jnp.exp2((m - mn) * scale)
                m = mn
        add_values(QUADS - 1, alpha)
        out = (out_t[:] / jnp.sum(den, axis=0, keepdims=True)).T.astype(BF16)
        for g in BOTH:
            hp = head_pair(p, part, g)
            for j, c in enumerate((2 * hp - hp // 2 + hp // 3, 2 * hp + 1 + (hp + 1) // 2 - hp // 2 - hp // 3)):
                for i, (cc, r) in enumerate(parts(part)[g]):
                    row = (2 * j + g) * HD + i * hh
                    obuf[zz, cc, pl.ds(pl.multiple_of(r * hh, hh), hh), pl.ds(pl.multiple_of(c * HD, HD), HD)] = out[row:row + hh]
        keep_q()

        by_tile(s, after)
        is_late = s == LATE[0] - 1
        for i in LATE[1:]:
            is_late = is_late | (s == i - 1)

        @pl.when(is_late)
        def _():
            whole_q(unit_of(carry[:3], LAST))

        return carry

    lax.fori_loop(0, len(TILES), tile, tuple(jnp.int32(t) for t in TABLES))

    @pl.when(end)
    def _():
        for c in THREE:
            kept(c).wait()
    for i in BOTH:
        @pl.when(end)
        def _():
            h_own(i, hb_r).wait_send()

        @pl.when(mid)
        def _():
            h_own_b(i).wait_send()
            h_own(i, hf_r).wait_send()
            h_b2f(i).wait_send()
            h_f2b(i).wait_send()
            h_f2b(2 + i).wait_send()
    sent("hd", hbuf.at[:, 0])
    pl.when(mid)(lambda: pl.semaphore_wait(ready.at[1]))
    pl.semaphore_wait(ready.at[0])

    def y_step(t, _):
        each_load(t, loaded)
        ch_a, ch_b, ch_c = (t - lag for lag in lags)

        def farther(i, ch, off):
            acc[i] = jnp.dot(rows_of(obuf, zof(3 - i)), weights(0, ch), preferred_element_type=F32)
            if off:
                y_recv_early(i, ch, i)
            go_on(i, ch, i, i + off, fwd)

        def nearest(g, ch):
            acc[2] = jnp.dot(rows_of(obuf, zof(0)), weights(g, ch), preferred_element_type=F32)
            acc[2] += y_recv(ch, 3)
            go_on(2, ch, 2, 3, bwd)

        @pl.when(end & (ch_a >= skip) & (ch_a < CHUNKS))
        def _():
            farther(0, ch_a, 0)

            @pl.when(ch_a < LASTS)
            def _():
                farther(1, ch_a, 0)
                farther(2, ch_a, 0)

            @pl.when(ch_a > LASTS)
            def _():
                for i in NEARER:
                    for ch in range(LASTS, CHUNKS):
                        farther(i, ch, 0)

        @pl.when(mid & (ch_a >= 0) & (ch_a < CHUNKS))
        def _():
            farther(0, ch_a, 3)

            @pl.when(ch_a < LASTS)
            def _():
                farther(1, ch_a, 3)

            @pl.when(ch_a > LASTS)
            def _():
                for ch in range(LASTS, CHUNKS):
                    nearest(0, ch)
                    farther(1, ch, 3)

        @pl.when(mid & (ch_b >= 0) & (ch_b < LASTS))
        def _():
            nearest(1, ch_b)

        passing = t + AHEAD

        @pl.when((passing > 4) & (passing < CHUNKS))
        def _():
            wo_pass(passing, passing + AHEAD)

        nxt = t + 1

        @pl.when((nxt >= len(EARLY)) & (nxt < CHUNKS))
        def _():
            wo_arrive(nxt)

        each_load(nxt, start_loads)

        @pl.when(ch_c == 0)
        def _():
            o_got(1)

        @pl.when((ch_c >= 0) & (ch_c < CHUNKS))
        def _():
            acc[3] = jnp.dot(rows_of(obuf, z), weights(2, ch_c), preferred_element_type=F32)

            @pl.when(end)
            def _():
                acc[3] += y_recv(ch_c, 3)

            @pl.when(mid)
            def _():
                y_recv_early(3, ch_c, 2)
                acc[3] += y_recv(ch_c, 4)
            y_out[:, own_cols(ch_c)] = acc[3, :HD].astype(BF16)
            hbuf[0, 1, :, cols(ch_c)] = acc[3, HD:].astype(BF16)
            y_sib(ch_c).start()
        return 0

    lax.fori_loop(0, CHUNKS + 4, y_step, 0)

    sent("wox", w_bytes)
    sent("woy", w_bytes)
    whole = slice(half)
    sent("yd", hbuf.at[0, 1, :, whole])
    got("yd", hbuf.at[0, 1, :, whole])
    sent("ox", obuf.at[:, :, :, :obuf.shape[3] // 2])

    @pl.when(end)
    def _():
        sent("y", wq.at[:SENDS, :CHUNKS - len(EARLY)])
        sent("pre", early.at[1])

    @pl.when(mid)
    def _():
        sent("y", wq.at[:SENDS, :CHUNKS])
    for i in THREE:
        kv_z(i).wait_send()
        kv_p(i).wait_send()
    kv_d().wait_send()
    wo_sib().wait_send()


def finish(y, kv, y_out, k_out, v_out, sems):
    copies = [pltpu.make_async_copy(src, dst, sems.at[i]) for i, (src, dst) in enumerate((
        (y, y_out), (kv.at[:, :, :, :, :HD], k_out), (kv.at[:, :, :, :, HD:], v_out)))]
    for c in copies:
        c.start()
    for c in copies:
        c.wait()


def solution(mesh):
    def local_step(x_loc, ln_gain, wq_loc, w_kv, wo_loc, positions):
        rows, width = x_loc.shape
        tokens = positions.shape[0]
        dma, vmem = pltpu.SemaphoreType.DMA, pltpu.VMEM
        hbm = pl.BlockSpec(memory_space=pl.ANY)
        half = width // 2
        cw = half // CHUNKS
        nb, n = width // PAIR, 2 * PAIR
        kv_shape = (QUADS, QUADS, 2, rows, HD)
        wkv_shape = (2, 2, 2, QUADS, PAIR, cw)
        vm = pl.BlockSpec(memory_space=pltpu.VMEM)
        kv_all = (QUADS, QUADS, 2, rows, PAIR)
        y, kv, _ = pl.pallas_call(
            kernel,
            name="mqa_layer",
            out_shape=(vmem((rows, width), BF16), vmem(kv_all, BF16), jax.ShapeDtypeStruct((2, QUADS, PAIR, half), BF16)),
            in_specs=[hbm] * 6,
            out_specs=(vm, vm, hbm),
            scratch_shapes=[
                vmem((QUADS, 2, rows, width), BF16),
                vmem((1, width), F32), vmem((1, tokens), I32),
                vmem((QUADS, nb, PAIR, PAIR), BF16),
                vmem((HD, tokens), BF16),
                vmem((tokens, HD), I32),
                vmem((QUADS, 2, rows, 2 * KEYS), BF16),
                vmem((3,) + wkv_shape[1:], BF16),
                vmem((QUADS, PAIR, cw), F32),
                vmem((2, len(EARLY), SENDS, PAIR, cw), BF16),
                vmem((KEYS, n), F32), vmem((KEYS, n), F32),
                vmem((KEYS, n), BF16), vmem((KEYS, n), BF16),
                vmem((HD, n), F32),
                vmem((PAIR, PAIR), F32),
                vmem((n, HD), BF16),
                dma((5,)), dma((sum(SND.values()),)), dma((sum(RCV.values()),)), dma((6,)), dma((2,)), dma((3, 2)),
                pltpu.SemaphoreType.REGULAR((2,)),
            ],
            compiler_params=pltpu.CompilerParams(
                collective_id=0, has_side_effects=True, vmem_limit_bytes=58 << 20),
        )(x_loc, ln_gain.reshape(1, width), wq_loc.reshape(nb, PAIR, PAIR), w_kv.reshape(wkv_shape), wo_loc, positions.reshape(1, tokens))
        y, k, v = pl.pallas_call(
            finish,
            name="outputs",
            out_shape=tuple(jax.ShapeDtypeStruct(s, BF16) for s in ((rows, width), kv_shape, kv_shape)),
            in_specs=[vm] * 2,
            out_specs=(hbm,) * 3,
            scratch_shapes=[dma((3,))],
            compiler_params=pltpu.CompilerParams(vmem_limit_bytes=1 << 20),
        )(pltpu.with_memory_space_constraint(y, pltpu.VMEM), pltpu.with_memory_space_constraint(kv, pltpu.VMEM))
        return y, k.reshape(tokens, HD), v.reshape(tokens, HD)

    split, whole = P("model", None), P(None, None)
    return jax.shard_map(
        local_step,
        mesh=mesh,
        in_specs=(split, P(), P(None, "model"), whole, split, P()),
        out_specs=(split, whole, whole),
        check_vma=False,
    )
```

```python
import functools

import jax
import jax.numpy as jnp
from jax import lax
from jax.experimental import pallas as pl
from jax.experimental.pallas import tpu as pltpu
from jax.sharding import PartitionSpec as P

NORM_EPS = 1e-6
LOG2E = 1.4426950408889634
MESH = pl.DeviceIdType.MESH
BF16, F32, I32 = jnp.bfloat16, jnp.float32, jnp.int32
SUB, ROWS = 8, 16
HD = 128
PAIR = 2 * HD
KEYS = SUB * HD
QUADS = 4
CHUNKS = 16
LASTS = CHUNKS - 2
AHEAD = 2
MASKED = -1e30
BOTH, THREE = range(2), range(3)
NEARER = (1, 2)
HANDED_ON = (4, 5)

TILES = ((0, 0, 0), (0, 1, 0), (1, 0, 0), (1, 1, 0), (0, 2, 0), (1, 2, 0), (2, 0, 0), (2, 1, 0), (2, 2, 0), (3, 0, 1),
         (1, 3, 0), (2, 3, 0), (3, 2, 1), (3, 0, 2), (3, 2, 2), (0, 3, 0))
LATE = (1, 2, 4, 6, 9, 10, 13)
FAR = 14
EARLY = (FAR - 2, FAR - 2, FAR - 1)
LAST = TILES[-1]
NEXT = [TILES[0] if i in LATE else t for i, t in enumerate(TILES)][1:]


def digits(values):
    return sum((v % 4) << (2 * i) for i, v in enumerate(values))


SPARE = (0, 3, 0)
TABLES = [digits(t[c] - LAST[c] for t in TILES) for c in THREE] + [digits(t[c] - SPARE[c] for t in NEXT) for c in THREE]

SENDS, RECVS = 3, 5
RING, Y_RING = 4, 8

KINDS = ("kvz", "kvp", "kvd", "h", "hd", "wx", "wy", "pre", "wod", "wox", "woy", "ox", "y", "yd")
SND = dict.fromkeys(KINDS, 1)
RCV = dict.fromkeys(KINDS, 1) | dict(kvz=3, kvp=3, hd=10, wx=6, wy=6, pre=9, wox=2 * RING, woy=2 * RING, ox=3, y=RECVS * Y_RING)


def odd(v):
    return lax.rem(v, 2)


def offsets(counts):
    out = {}
    for name in counts:
        out[name] = sum(counts[k] for k in out)
    return out


SND_AT, RCV_AT = offsets(SND), offsets(RCV)


def kernel(x_in, gain_in, wq_in, wkv_in, wo_in, pos_in, y_out, kv, wo_land,
           hbuf, gain, pos, wq, v_t, posk, obuf, wbuf, acc, early, sc0, sc1, pr0, pr1, out_t, qacc, qbuf,
           loc, snd, rcv, hf_r, hb_r, ld, ready):
    me = lax.axis_index("model")
    core = odd(me)
    quad = lax.rem(me // 2, QUADS)
    z = me // 8
    width = hbuf.shape[3]
    half = width // 2
    cw = half // CHUNKS
    upper = z // 2
    away = 1 - 2 * upper

    def zof(d):
        return d + upper * (3 - 2 * d)

    e = zof(z)
    end, mid = e == 0, e == 1
    base = me - 8 * z
    dx = 2 - 4 * odd(quad)
    dy = 4 - 8 * (quad // 2)
    sib, xn, yn, dg = me + 1 - 2 * core, me + dx, me + dy, me + dx + dy
    fwd = base + 8 * (z + away)
    bwd = base + 8 * (z - away * e)
    zpeers = [base + 8 * lax.rem(z + i, QUADS) for i in (1, 2, 3)]
    bufs = ((sc0, pr0), (sc1, pr1))

    def put(src, dst, ssem, rsem, dev):
        return pltpu.make_async_remote_copy(src, dst, ssem, rsem, device_id=(dev,), device_id_type=MESH)

    def send(kind, src, dst, dev, i=0):
        return put(src, dst, snd.at[SND_AT[kind]], rcv.at[RCV_AT[kind] + i], dev)

    def sent(kind, like):
        send(kind, like, like, sib).wait_send()

    def got(kind, like, i=0):
        send(kind, like, like, sib, i).wait_recv()

    def kv_z(i):
        blk = kv.at[z, :, core]
        return send("kvz", blk, blk, zpeers[i], i)

    def kv_p(i):
        blk = kv.at[z, quad, core]
        return send("kvp", blk, blk, (xn, yn, dg)[i], i)

    def kv_d():
        blk = kv.at[:, :, core]
        return send("kvd", blk, blk, sib)

    hh = HD // 2

    def hrows(zz, cc, i):
        return hbuf.at[zz, cc, pl.ds(hh * i, hh), :]

    def h_put(n, zz, i, rsem, dev):
        return put(hrows(zz, 0, i), hrows(zz, 0, i), snd.at[SND_AT["h"]], rsem, dev)

    def h_own(i, rsems):
        return h_put(i, z, i, rsems.at[i], fwd)

    def h_own_b(i):
        return h_put(2 + i, z, i, hf_r.at[i], bwd)

    def h_f2b(i):
        return h_put(4 + i, zof(e + 1 + i // 2), i % 2, hf_r.at[2 + i], bwd)

    def h_b2f(i):
        return h_put(8 + i, zof(e - 1), i, hf_r.at[2 + i], fwd)

    def h_d(i):
        zz = z if i < 2 else (zof(e + i // 2) if i < 8 else zof(e - 1))
        return send("hd", hrows(zz, 0, i % 2), hrows(zz, 1, i % 2), sib, i)

    def f_half(i):
        zz = zof(e + 1 + i // 2)
        h_put(0, zz, i % 2, hf_r.at[i], fwd).wait_recv()
        h_d(2 + i).start()
        if i < 4:
            @pl.when(mid)
            def _():
                h_f2b(i).start()

    def b_half(i):
        @pl.when(mid)
        def _():
            h_put(0, zof(e - 1), i, hb_r.at[i], bwd).wait_recv()
            h_d(8 + i).start()
            h_b2f(i).start()

    def h_block_wait(b):
        for i in BOTH:
            h_d(2 * b + i).wait_recv()

    def half_block_wait(c):
        pl.when(end)(lambda: h_d(6 + c).wait_recv())
        pl.when(mid)(lambda: h_d(4 + c).wait_recv())

    nb = wq.shape[1]
    hb = nb // 2

    def w_piece(dev, i):
        y = int(dev is yn)
        lower, upper = slice(hb), slice(hb, nb)
        halves = (lower, upper) if y else (upper, lower)
        if i < 4:
            rows = (slice(4), slice(4, nb), *halves)[i]
            h = i // 2
            src = wq_in.at[rows, :, pl.ds(HD * h, HD)]
            dst = wq.at[1 + h, rows, :, pl.ds(HD * y, HD)]
        else:
            h = i - 4
            rows = halves[1]
            src = wq.at[1 + h, rows, :, pl.ds(HD - HD * y, HD)]
            dst = wq.at[3, rows, :, pl.ds(HD * h, HD)]
        return send("wy" if y else "wx", src, dst, dev, i)

    def w_start(*pieces):
        for i in pieces:
            w_piece(xn, i).start()
            w_piece(yn, i).start()

    def w_got(*pieces):
        for i in pieces:
            w_piece(xn, i).wait_recv()
            w_piece(yn, i).wait_recv()

    def wo_sib():
        src = wo_in.at[:, pl.ds(pl.multiple_of((1 - core) * half, half), half)]
        return send("wod", src, wo_land.at[1, 0], sib)

    def cols(ch):
        return pl.ds(pl.multiple_of(ch * cw, cw), cw)

    def own_cols(ch):
        return pl.ds(pl.multiple_of(core * half + ch * cw, cw), cw)

    def wo_piece(dev, i, ch, near=False):
        y = int(dev is yn)
        part = (0, 1, y)[i]
        src = (wo_in.at[:, own_cols(ch)], wo_land.at[1, 0, :, cols(ch)], wo_land.at[y, 2 - y, :, cols(ch)])[i]
        dst = wbuf.at[(*divmod(ch, 2), part, 3)] if near else wo_land.at[part, 3 if i == 2 else 1 + y, :, cols(ch)]
        return send("woy" if y else "wox", src, dst, dev, 2 * lax.rem(ch, RING) + i // 2)

    wo_x, wo_y = (functools.partial(wo_piece, dev) for dev in (xn, yn))

    def wo_own(ch):
        for i in BOTH:
            wo_x(i, ch).start()
            wo_y(i, ch).start()

    def wo_pass(ch, *more):
        got("wox", wo_land.at[:, 1, :, cols(ch)], 2 * lax.rem(ch, RING))
        got("woy", wo_land.at[:, 2, :, cols(ch)], 2 * lax.rem(ch, RING))

        def hand_on(near):
            wo_x(2, ch, near).start()
            wo_y(2, ch, near).start()

        if isinstance(ch, int) and ch < len(EARLY):
            pl.when(mid)(lambda: hand_on(False))

            @pl.when(end)
            def _():
                hand_on(True)
                for c in near_loads(ch):
                    c.start()
        else:
            hand_on(False)
        for nxt in more:
            @pl.when(nxt < CHUNKS)
            def _():
                wo_own(nxt)

    def wo_arrive(ch):
        wo_x(2, ch).wait_recv()
        wo_y(2, ch).wait_recv()

    def load(g, slot, src, dst):
        return pltpu.make_async_copy(src, dst, ld.at[g, slot])

    def loads(g, ch, slot):
        w = wbuf.at[g, slot]
        rest = slice(1, QUADS)
        return (load(g, slot, wo_in.at[:, own_cols(ch)], w.at[0, 0]),
                load(g, slot, wo_land.at[0, rest, :, cols(ch)], w.at[0, rest]),
                load(g, slot, wo_land.at[1, :, :, cols(ch)], w.at[1]))

    def near_loads(c):
        g, slot = divmod(c, 2)
        w, most = wbuf.at[g, slot], slice(1, 3)
        return (load(g, slot, wo_in.at[:, own_cols(c)], w.at[0, 0]),
                load(g, slot, wo_land.at[0, most, :, cols(c)], w.at[0, most]),
                load(g, slot, wo_land.at[1, :3, :, cols(c)], w.at[1, :3]))

    def near_loaded(c):
        g, slot = divmod(c, 2)
        load(g, slot, wo_land.at[:, :3, :, cols(c)], wbuf.at[g, slot, :, :3]).wait()

    def kept(c):
        return pltpu.make_async_copy(wbuf.at[(*divmod(c, 2), slice(None), 3)], wo_land.at[:, 3, :, cols(c)], loc.at[c])

    lags = (e, 2, 4 - e)

    def loaded(g, ch, slot):
        load(g, slot, wo_land.at[:, :, :, cols(ch)], wbuf.at[g, slot]).wait()

    skip = (1 - e) * len(EARLY)

    def start_loads(g, ch, slot):
        for c in loads(g, ch, slot):
            c.start()

    def each_load(step, act):
        for g, (lag, lowest, past) in enumerate(zip(lags, (skip, 0, 0), (CHUNKS, e * LASTS, CHUNKS))):
            ch = step - lag

            @pl.when((ch >= lowest) & (ch < past))
            def _():
                act(g, ch, odd(ch))

    def kof(k):
        return zof(k + e * (lax.rem(k + 1, 3) + 2 * (k // 3) - k))

    def o_x(k, cc):
        lo = obuf.shape[3] // 2
        zz = kof(k)
        group = (1, 0, 0, 2)[k]
        return send("ox", obuf.at[zz, cc, :, :lo], obuf.at[zz, 1 - cc, :, lo:], sib, group)

    def o_got(group):
        rows = slice(1 if group else 2)
        got("ox", obuf.at[rows, :, :, :obuf.shape[3] // 2], group)

    x_copy, gain_copy, wkv_copy, wq_copy, pos_copy = first = [
        pltpu.make_async_copy(src, dst, loc.at[i])
        for i, (src, dst) in enumerate(((x_in, hbuf.at[z, 0]), (gain_in, gain), (wkv_in, wbuf.at[:2]), (wq_in, wq.at[0]), (pos_in, pos)))]
    for c in first:
        c.start()
    barrier = pltpu.get_barrier_semaphore()
    peers = zpeers + [xn, yn, dg, sib]
    for dev in peers:
        pl.semaphore_signal(barrier, device_id=(dev,), device_id_type=MESH)
    pl.semaphore_wait(barrier, len(peers))
    w_start(0)
    x_copy.wait()
    gain_copy.wait()

    @pl.loop(0, SUB)
    def _(i):
        rows = pl.ds(pl.multiple_of(i * ROWS, ROWS), ROWS)
        x = hbuf[z, 0, rows, :].astype(F32)
        cent = x - jnp.mean(x, axis=-1, keepdims=True)
        var = jnp.mean(cent * cent, axis=-1, keepdims=True)
        hbuf[z, 0, rows, :] = (cent * lax.rsqrt(var + NORM_EPS) * gain[:]).astype(BF16)

    wkv_copy.wait()
    kv[z, quad, core] = jnp.dot(hbuf[z, 0], wbuf[:2].reshape(width, PAIR), preferred_element_type=F32).astype(BF16)
    for i in THREE:
        kv_p(i).start()
    w_start(1, 2, 3)
    for i in BOTH:
        h_d(i).start()
    wo_sib().start()
    def own_rows(i):
        @pl.when(end)
        def _():
            h_own(i, hb_r).start()

        @pl.when(mid)
        def _():
            h_own_b(i).start()
            h_own(i, hf_r).start()

    own_rows(0)
    for i in THREE:
        kv_p(i).wait_recv()
    for i in THREE:
        kv_z(i).start()
    own_rows(1)

    pos_copy.wait()

    @pl.loop(0, posk.shape[0] // HD)
    def _(i):
        blk = pl.ds(pl.multiple_of(i * HD, HD), HD)
        posk[blk, :] = jnp.broadcast_to(pos[:, blk], (HD, HD)).T

    def rows_of(ref, zz):
        return ref[zz].reshape(PAIR, ref.shape[3])

    def keep_q():
        q = qacc[:].astype(BF16)
        qbuf[:PAIR] = q[:, :HD]
        qbuf[PAIR:] = q[:, HD:]

    def parts(part):
        split = (part + 1) // 2
        return [[(g + split * (i - g), i + split * (part - 1 - i)) for i in BOTH] for g in BOTH]

    def head_pair(p, part, g):
        return p + g * ((part + 1) // 2)

    def q_dot(unit, js, ws):
        zz, p, part = unit
        for g in BOTH:
            rows = [hbuf[zz, cc, pl.ds(pl.multiple_of(r * hh, hh), hh), js] for cc, r in parts(part)[g]]
            w = wq[head_pair(p, part, g), ws].reshape(-1, PAIR)
            yield g, jnp.dot(jnp.concatenate(rows, axis=0), w, preferred_element_type=F32)

    def whole_q(unit):
        for g, part in q_dot(unit, slice(None), slice(None)):
            qacc[g * HD:(g + 1) * HD] = part
        keep_q()

    def unit_of(codes, last):
        k, p, part = (lax.rem(c + v, QUADS) for c, v in zip(codes, last))
        return kof(k), p, part

    wq_copy.wait()
    h_block_wait(0)
    whole_q((z, 0, 0))
    for i in THREE:
        kv_z(i).wait_recv()
    kv_d().start()
    kv_d().wait_recv()
    for j in range(QUADS):
        v_t[:, j * KEYS:(j + 1) * KEYS] = kv[j].reshape(KEYS, PAIR)[:, HD:].T

    blocks = [(k, cc) for k in range(QUADS) for cc in BOTH]
    places = nb

    def place(i):
        return wq.at[i // places, lax.rem(i, places)]

    def y_send(i, ch, off, dev):
        return send("y", place(RECVS * CHUNKS + ch * SENDS + i), place(ch * RECVS + off), dev, RECVS * lax.rem(ch, Y_RING) + off)

    def y_recv(ch, off):
        blk = place(ch * RECVS + off)
        got("y", blk, RECVS * lax.rem(ch, Y_RING) + off)
        return blk[:].astype(F32)

    def y_sib(ch):
        return send("yd", hbuf.at[0, 1, :, cols(ch)], y_out.at[:, own_cols(ch)], sib)

    def weights(g, ch):
        return wbuf[g, odd(ch)].reshape(obuf.shape[3], cw)

    def go_on(j, ch, i, off, dev):
        place(RECVS * CHUNKS + ch * SENDS + i)[:] = acc[j].astype(BF16)
        y_send(i, ch, off, dev).start()

    o_parts = ((EARLY[0] - 1, blocks[2:6]), (FAR + 1, blocks[:2]), (FAR, blocks[6:]))

    def early_send(c, i):
        return send("pre", early.at[1, c, i], early.at[0, c, i], fwd, SENDS * c + i)

    def y_early(c):
        near_loaded(c)
        kept(c).start()
        for i in NEARER:
            early_sum(c, i)

    def early_sum(c, i):
        early[1, c, i] = jnp.dot(rows_of(obuf, zof(3 - i)), weights(c // 2, c), preferred_element_type=F32).astype(BF16)
        early_send(c, i).start()

    def y_recv_early(n, ch, off):
        @pl.when(ch < len(EARLY))
        def _():
            blk = early.at[0, ch, off]
            got("pre", blk, SENDS * ch + off)
            acc[n] += blk[:].astype(F32)

        @pl.when(ch >= len(EARLY))
        def _():
            acc[n] += y_recv(ch, off)

    def pairs_0():
        w_got(*BOTH)
        f_half(0)
        b_half(0)

    def rows_1():
        f_half(1)
        b_half(1)
        h_block_wait(1)
        w_got(2)
        w_start(*HANDED_ON)
        wo_sib().wait_recv()
        wo_own(0)
        wo_own(1)

    def pairs_1():
        w_got(3)
        f_half(2)

    def rows_2():
        f_half(3)
        pl.when(end)(lambda: h_block_wait(2))
        pl.when(mid)(lambda: h_block_wait(4))

    def rows_3():
        pl.when(end)(lambda: f_half(4))
        half_block_wait(0)

    late = dict(zip(LATE, (pairs_0, rows_1, pairs_1, rows_2, rows_3, lambda: w_got(*HANDED_ON), lambda: half_block_wait(1))))

    w_bytes = wq.at[:3, :hb]

    def tell(sem, dev):
        pl.semaphore_signal(sem, device_id=(dev,), device_id_type=MESH)

    def get_ready():
        sent("wx", w_bytes)
        sent("wy", w_bytes)
        tell(ready.at[1 - e], fwd)
        pl.when(mid)(lambda: tell(ready.at[0], bwd))

    def before(i):
        if i == EARLY[0] - 1:
            yield lambda: wo_pass(0)
        if i == EARLY[0]:
            yield lambda: wo_pass(1, 2)
        if i == FAR + 1:
            yield lambda: wo_pass(4, 6)

    def after(i):
        for at, some in o_parts:
            if at == i:
                for b in some:
                    yield lambda b=b: o_x(*b).start()
        for c, at in enumerate(EARLY):
            if at == i:
                if c == 0:
                    yield lambda: o_got(0)
                if c == 1:
                    yield lambda: pl.when(end)(lambda: f_half(5))
                yield lambda c=c: wo_arrive(c)
                yield lambda c=c: pl.when(end)(lambda: y_early(c))
        if i == EARLY[1]:
            yield lambda: wo_pass(2, 3, 4)
        if i == FAR:
            yield get_ready
            yield lambda: wo_pass(3, 5)
            yield lambda: o_got(2)
            for c in THREE:
                yield lambda c=c: pl.when(end)(lambda: early_sum(c, 0))
        if i + 1 in late:
            yield late[i + 1]

    def by_tile(s, due, lo=0, hi=len(TILES)):
        if not any(True for i in range(lo, hi) for _ in due(i)):
            return
        if hi - lo == 1:
            for act in due(lo):
                act()
            return
        half_way = (lo + hi) // 2
        pl.when(s < half_way)(lambda: by_tile(s, due, lo, half_way))
        pl.when(s >= half_way)(lambda: by_tile(s, due, half_way, hi))

    scale = HD ** -0.5 * LOG2E
    n = 2 * PAIR
    kq = width // QUADS

    def tile(s, carry):
        codes, ahead = carry[:3], carry[3:]
        zz, p, part = unit_of(codes, LAST)
        following = unit_of(ahead, SPARE)
        carry = tuple(c // QUADS for c in carry)

        by_tile(s, before)
        q = qbuf[:]
        tok = (zz * QUADS + quad) * 2
        pq = [pos[:, pl.ds(pl.multiple_of((tok + c) * HD, HD), HD)] for c in (core, 1 - core)]
        pq = [[v[:, :hh], v[:, hh:]] for v in pq]
        split, second = (part + 1) // 2, part // 2
        of_core = [v[0] + second * (v[1] - v[0]) for v in pq]
        pq = [pq[g][i] + split * (of_core[i] - pq[g][i]) for g in BOTH for i in BOTH]
        pq = jnp.broadcast_to(jnp.concatenate(pq + pq, axis=1), (SUB, n))

        def scores(j):
            keys = kv[j].reshape(KEYS, PAIR)[:, :HD]
            sc = lax.dot_general(keys, q, (((1,), (1,)), ((), ())), preferred_element_type=F32)
            pk = posk[j * KEYS:(j + 1) * KEYS, :]
            pk = jnp.concatenate([pk] * (n // HD), axis=1).reshape(KEYS // SUB, SUB, n)
            sc = jnp.where(pk <= pq, sc.reshape(KEYS // SUB, SUB, n), MASKED)
            bufs[j % 2][0][:] = sc.reshape(KEYS, n)
            return jnp.max(jnp.max(sc, axis=0), axis=0, keepdims=True)

        def weigh(j, m):
            pr = jnp.exp2((bufs[j % 2][0][:].reshape(KEYS // SUB, SUB, n) - jnp.broadcast_to(m, (SUB, n))) * scale)
            bufs[j % 2][1][:] = pr.reshape(KEYS, n).astype(BF16)
            return jnp.sum(pr, axis=0)

        def add_values(j, alpha):
            got = jnp.dot(v_t[:, j * KEYS:(j + 1) * KEYS], bufs[j % 2][1][:], preferred_element_type=F32)
            out_t[:] = got if alpha is None else out_t[:] * alpha + got

        m = scores(0)
        alpha = den = None
        for j in range(QUADS):
            if j + 1 < QUADS:
                mn = jnp.maximum(m, scores(j + 1))
            for g, got in q_dot(following, slice(j * kq, (j + 1) * kq), slice(j * nb // QUADS, (j + 1) * nb // QUADS)):
                rows = slice(g * HD, (g + 1) * HD)
                qacc[rows] = got if j == 0 else qacc[rows] + got
            ps = weigh(j, m)
            if j > 0:
                add_values(j - 1, alpha if j > 1 else None)
            den = ps if j == 0 else den * now + ps
            if j > 0:
                alpha = now
            if j < QUADS - 1:
                now = jnp.exp2((m - mn) * scale)
                m = mn
        add_values(QUADS - 1, alpha)
        out = (out_t[:] / jnp.sum(den, axis=0, keepdims=True)).T.astype(BF16)
        for g in BOTH:
            hp = head_pair(p, part, g)
            for j, c in enumerate((2 * hp - hp // 2 + hp // 3, 2 * hp + 1 + (hp + 1) // 2 - hp // 2 - hp // 3)):
                for i, (cc, r) in enumerate(parts(part)[g]):
                    row = (2 * j + g) * HD + i * hh
                    obuf[zz, cc, pl.ds(pl.multiple_of(r * hh, hh), hh), pl.ds(pl.multiple_of(c * HD, HD), HD)] = out[row:row + hh]
        keep_q()

        by_tile(s, after)
        is_late = s == LATE[0] - 1
        for i in LATE[1:]:
            is_late = is_late | (s == i - 1)

        @pl.when(is_late)
        def _():
            whole_q(unit_of(carry[:3], LAST))

        return carry

    lax.fori_loop(0, len(TILES), tile, tuple(jnp.int32(t) for t in TABLES))

    @pl.when(end)
    def _():
        for c in THREE:
            kept(c).wait()
    pl.when(end)(lambda: sent("h", wq.at[0, :hb]))
    pl.when(mid)(lambda: sent("h", wq.at[:, :hb + 4]))
    sent("hd", hbuf.at[:, 0])
    pl.when(mid)(lambda: pl.semaphore_wait(ready.at[1]))
    pl.semaphore_wait(ready.at[0])

    def y_step(t, _):
        each_load(t, loaded)
        ch_a, ch_b, ch_c = (t - lag for lag in lags)

        def farther(i, ch, off):
            acc[i] = jnp.dot(rows_of(obuf, zof(3 - i)), weights(0, ch), preferred_element_type=F32)
            if off:
                y_recv_early(i, ch, i)
            go_on(i, ch, i, i + off, fwd)

        def nearest(g, ch):
            acc[2] = jnp.dot(rows_of(obuf, zof(0)), weights(g, ch), preferred_element_type=F32)
            acc[2] += y_recv(ch, 3)
            go_on(2, ch, 2, 3, bwd)

        @pl.when(end & (ch_a >= skip) & (ch_a < CHUNKS))
        def _():
            farther(0, ch_a, 0)

            @pl.when(ch_a < LASTS)
            def _():
                farther(1, ch_a, 0)
                farther(2, ch_a, 0)

            @pl.when(ch_a > LASTS)
            def _():
                for i in NEARER:
                    for ch in range(LASTS, CHUNKS):
                        farther(i, ch, 0)

        @pl.when(mid & (ch_a >= 0) & (ch_a < CHUNKS))
        def _():
            farther(0, ch_a, 3)

            @pl.when(ch_a < LASTS)
            def _():
                farther(1, ch_a, 3)

            @pl.when(ch_a > LASTS)
            def _():
                for ch in range(LASTS, CHUNKS):
                    nearest(0, ch)
                    farther(1, ch, 3)

        @pl.when(mid & (ch_b >= 0) & (ch_b < LASTS))
        def _():
            nearest(1, ch_b)

        passing = t + AHEAD

        @pl.when((passing > 4) & (passing < CHUNKS))
        def _():
            wo_pass(passing, passing + AHEAD)

        nxt = t + 1

        @pl.when((nxt >= len(EARLY)) & (nxt < CHUNKS))
        def _():
            wo_arrive(nxt)

        each_load(nxt, start_loads)

        @pl.when(ch_c == 0)
        def _():
            o_got(1)

        @pl.when((ch_c >= 0) & (ch_c < CHUNKS))
        def _():
            acc[3] = jnp.dot(rows_of(obuf, z), weights(2, ch_c), preferred_element_type=F32)

            @pl.when(end)
            def _():
                acc[3] += y_recv(ch_c, 3)

            @pl.when(mid)
            def _():
                y_recv_early(3, ch_c, 2)
                acc[3] += y_recv(ch_c, 4)
            y_out[:, own_cols(ch_c)] = acc[3, :HD].astype(BF16)
            hbuf[0, 1, :, cols(ch_c)] = acc[3, HD:].astype(BF16)
            y_sib(ch_c).start()
        return 0

    lax.fori_loop(0, CHUNKS + 4, y_step, 0)

    sent("wox", w_bytes)
    sent("woy", w_bytes)
    whole = slice(half)
    sent("yd", hbuf.at[0, 1, :, whole])
    got("yd", hbuf.at[0, 1, :, whole])
    sent("ox", obuf.at[:, :, :, :obuf.shape[3] // 2])

    @pl.when(end)
    def _():
        sent("y", wq.at[:SENDS, :CHUNKS - len(EARLY)])
        sent("pre", early.at[1])

    @pl.when(mid)
    def _():
        sent("y", wq.at[:SENDS, :CHUNKS])
    sent("kvz", kv.at[:3, :, 0])
    sent("kvp", kv.at[0, :3, 0])
    kv_d().wait_send()
    wo_sib().wait_send()


def finish(y, kv, y_out, k_out, v_out, sems):
    copies = [pltpu.make_async_copy(src, dst, sems.at[i]) for i, (src, dst) in enumerate((
        (y, y_out), (kv.at[:, :, :, :, :HD], k_out), (kv.at[:, :, :, :, HD:], v_out)))]
    for c in copies:
        c.start()
    for c in copies:
        c.wait()


def solution(mesh):
    def local_step(x_loc, ln_gain, wq_loc, w_kv, wo_loc, positions):
        rows, width = x_loc.shape
        tokens = positions.shape[0]
        dma, vmem = pltpu.SemaphoreType.DMA, pltpu.VMEM
        hbm = pl.BlockSpec(memory_space=pl.ANY)
        half = width // 2
        cw = half // CHUNKS
        nb, n = width // PAIR, 2 * PAIR
        kv_shape = (QUADS, QUADS, 2, rows, HD)
        wkv_shape = (2, 2, 2, QUADS, PAIR, cw)
        vm = pl.BlockSpec(memory_space=pltpu.VMEM)
        kv_all = (QUADS, QUADS, 2, rows, PAIR)
        y, kv, _ = pl.pallas_call(
            kernel,
            name="mqa_layer",
            out_shape=(vmem((rows, width), BF16), vmem(kv_all, BF16), jax.ShapeDtypeStruct((2, QUADS, PAIR, half), BF16)),
            in_specs=[hbm] * 6,
            out_specs=(vm, vm, hbm),
            scratch_shapes=[
                vmem((QUADS, 2, rows, width), BF16),
                vmem((1, width), F32), vmem((1, tokens), I32),
                vmem((QUADS, nb, PAIR, PAIR), BF16),
                vmem((HD, tokens), BF16),
                vmem((tokens, HD), I32),
                vmem((QUADS, 2, rows, 2 * KEYS), BF16),
                vmem((3,) + wkv_shape[1:], BF16),
                vmem((QUADS, PAIR, cw), F32),
                vmem((2, len(EARLY), SENDS, PAIR, cw), BF16),
                vmem((KEYS, n), F32), vmem((KEYS, n), F32),
                vmem((KEYS, n), BF16), vmem((KEYS, n), BF16),
                vmem((HD, n), F32),
                vmem((PAIR, PAIR), F32),
                vmem((n, HD), BF16),
                dma((5,)), dma((sum(SND.values()),)), dma((sum(RCV.values()),)), dma((6,)), dma((2,)), dma((3, 2)),
                pltpu.SemaphoreType.REGULAR((2,)),
            ],
            compiler_params=pltpu.CompilerParams(
                collective_id=0, has_side_effects=True, vmem_limit_bytes=58 << 20),
        )(x_loc, ln_gain.reshape(1, width), wq_loc.reshape(nb, PAIR, PAIR), w_kv.reshape(wkv_shape), wo_loc, positions.reshape(1, tokens))
        y, k, v = pl.pallas_call(
            finish,
            name="outputs",
            out_shape=tuple(jax.ShapeDtypeStruct(s, BF16) for s in ((rows, width), kv_shape, kv_shape)),
            in_specs=[vm] * 2,
            out_specs=(hbm,) * 3,
            scratch_shapes=[dma((3,))],
            compiler_params=pltpu.CompilerParams(vmem_limit_bytes=1 << 20),
        )(pltpu.with_memory_space_constraint(y, pltpu.VMEM), pltpu.with_memory_space_constraint(kv, pltpu.VMEM))
        return y, k.reshape(tokens, HD), v.reshape(tokens, HD)

    split, whole = P("model", None), P(None, None)
    return jax.shard_map(
        local_step,
        mesh=mesh,
        in_specs=(split, P(), P(None, "model"), whole, split, P()),
        out_specs=(split, whole, whole),
        check_vma=False,
    )
```
